128 devices in a mesh: grid: 32 (over x, z, core), orb: 4 (over y).
Axes of the slice: x: 4, y: 4, z: 4, core: 2. Of those that a mesh axis runs over, the one named last changes fastest.
Arguments:
- orbitals: bfloat16 [1800, 262144], P('orb', 'grid'), may hold values from -0.5 to 1.5
- pivots: int32 [3, 96], replicated, may hold values from 0 to 262143, as said below
Outputs:
- cholesky_factor: float32 [262144, 288], P(('grid', 'orb'))
- residual_diagonal: float32 [262144], P(('grid', 'orb'))
- diagonal_peaks: float32 [3], replicated
The draws below stay inside these ranges and needn't reach their ends.
Inputs may be any that keep to these rules, and one draw needn't show every extreme that they name: `pivots`: all 3 x 96 pivot indices are distinct grid points.
All inputs are finite; a program needn't handle non-finite values.
Results may differ from the reference program's by a relative error of at most 0.0003.
Values may be sent and summed in bfloat16 or wider, within the bound.
A program may use at most 64 MiB of HBM per device.

```python
import jax
import jax.numpy as jnp
from jax import lax

ORB = 1800
PIV = 96
STEPS = 3
GRID_POINTS = 262144


def draw_pivots(key, part):
    order = jax.random.permutation(jax.random.fold_in(key, 11), GRID_POINTS)
    return order[:STEPS * PIV].reshape(STEPS, PIV).astype(jnp.int32)


def levels(stream_key, shape, pieces, smallest, largest):
    def one(axis_at, parts):
        draws = jax.random.uniform(jax.random.fold_in(jax.random.fold_in(stream_key, 6), axis_at), (parts,), jnp.float32, smallest / len(pieces), largest / len(pieces))
        return jnp.repeat(jnp.exp(draws), shape[axis_at] // parts).reshape((-1,) + (1,) * (len(shape) - axis_at - 1))

    loudness = one(*pieces[0])
    for cut in pieces[1:]:
        loudness = loudness * one(*cut)
    return loudness


def setup_inputs(seed: int = 0) -> dict:
    keys = jax.random.split(jax.random.key(seed), 3)
    orbitals = jnp.clip(-0.5 + 2.0 * jax.random.uniform(keys[0], (ORB, GRID_POINTS), jnp.float32) ** levels(keys[0], (ORB, GRID_POINTS), ((0, 4), (1, 32)), -0.2, 0.2), -0.5, 1.5).astype(jnp.bfloat16)
    pivots = draw_pivots(jax.random.fold_in(keys[2], 71), 0)
    return dict(orbitals=orbitals, pivots=pivots)


def reference(orbitals, pivots):
    grid_count = orbitals.shape[1]
    squares = jnp.sum(jnp.square(orbitals.astype(jnp.float32)), axis=0)
    diagonal = jnp.square(squares / ORB)
    factor = jnp.zeros((grid_count, STEPS * PIV), jnp.float32)
    peaks = []
    for section in range(STEPS):
        chosen = pivots[section]
        sampled = jnp.take(orbitals, chosen, axis=1)
        known = jnp.take(factor, chosen, axis=0)
        pair = lax.dot_general(sampled.astype(jnp.float32), sampled.astype(jnp.float32), (((0,), (0,)), ((), ())), preferred_element_type=jnp.float32)
        block = jnp.square(pair / ORB) - jnp.dot(known, known.T, precision=lax.Precision.HIGHEST)
        inner = lax.dot_general(orbitals.astype(jnp.float32), sampled.astype(jnp.float32), (((0,), (0,)), ((), ())), preferred_element_type=jnp.float32)
        columns = jnp.square(inner / ORB) - jnp.dot(factor, known.T, precision=lax.Precision.HIGHEST)
        lower = jnp.linalg.cholesky(block)
        fresh = jax.scipy.linalg.solve_triangular(lower, columns.T, lower=True).T
        factor = factor.at[:, section * PIV:(section + 1) * PIV].set(fresh)
        diagonal = diagonal - jnp.sum(fresh * fresh, axis=1)
        peaks.append(jnp.max(diagonal))
    return (factor, diagonal, jnp.stack(peaks))
```

```python
import functools

import jax
import jax.numpy as jnp
from jax import lax
from jax.experimental import pallas as pl
from jax.experimental.pallas import tpu as pltpu
from jax.sharding import Mesh
from jax.sharding import PartitionSpec as P

ORB = 1800
GRID = ("grid_0", "grid_1", "grid_2")
GRID_ORB = ("grid_0", "grid_1", "grid_2", "orb")
MESH = pl.DeviceIdType.MESH
HIGHEST = lax.Precision.HIGHEST

STEPS = 3
PIV = 96
RANK = STEPS * PIV
HALF = PIV // 2
DEPTH = 450
WIDE = 512
ROWS = 8192
SHARE = 2048
PART = 1024
PIECE = 256
PIECES = PART // PIECE
SUMS = RANK + 8

CORE_A, X_A, Z_A, Y_A, Z_B, X_B, CORE_B = 0, 1, 4, 7, 10, 13, 16
FAR, NEAR, SUM = 17, 19, 21
PEAK_CORE, PEAK_Z, PEAK_X, PEAK_Y = 29, 30, 33, 36
SLOTS = 39


def nt(left, right, precision=None):
    return lax.dot_general(
        left, right, (((1,), (1,)), ((), ())), precision=precision,
        preferred_element_type=jnp.float32,
    )


def nn(left, right, precision=None):
    return lax.dot_general(
        left, right, (((1,), (0,)), ((), ())), precision=precision,
        preferred_element_type=jnp.float32,
    )


def inverse_factor(block):
    lanes = lax.broadcasted_iota(jnp.int32, (8, PIV), 1)
    subs = lax.broadcasted_iota(jnp.int32, (8, PIV), 0)
    groups = PIV // 8
    left = [block[8 * g : 8 * g + 8, :] for g in range(groups)]
    right = [jnp.where(lanes == subs + 8 * g, 1.0, 0.0) for g in range(groups)]
    sub_column = lax.broadcasted_iota(jnp.int32, (8, 1), 0)
    for k in range(PIV):
        home, r = divmod(k, 8)
        row_left = left[home][r : r + 1, :]
        row_right = right[home][r : r + 1, :]
        inverse = 1.0 / row_left[:, k : k + 1]
        row_left = row_left * inverse
        row_right = row_right * inverse
        for g in range(home, groups):
            column = left[g][:, k : k + 1]
            if g == home:
                if r == 7:
                    continue
                column = jnp.where(sub_column > r, column, 0.0)
            left[g] = left[g] - column * row_left
            right[g] = right[g] - column * row_right
    out = []
    for g in range(groups):
        pivot = jnp.sum(jnp.where(lanes == subs + 8 * g, left[g], 0.0), axis=1, keepdims=True)
        out.append(right[g] * (1.0 / jnp.sqrt(pivot)))
    return jnp.concatenate(out, axis=0)


def kernel(
    orb_hbm, piv_ref, factor_ref, diag_ref, peak_ref,
    orb, gathered, pv, a0, r0, r1, a2, r2, picked, far, near, sums_out, sums_in,
    gram, low, inv, peak_buf, local_sem, send_sem, recv_sem,
):
    x = lax.axis_index("grid_0")
    z = lax.axis_index("grid_1")
    core = lax.axis_index("grid_2")
    me = lax.axis_index("orb")
    right, left, across = lax.rem(me + 1, 4), lax.rem(me + 3, 4), lax.rem(me + 2, 4)
    other = 1 - core

    barrier = pltpu.get_barrier_semaphore()
    pl.semaphore_signal(barrier, inc=1, device_id={"grid_2": other}, device_id_type=MESH)
    for d in (1, 2, 3):
        pl.semaphore_signal(barrier, inc=1, device_id={"grid_0": lax.rem(x + d, 4)}, device_id_type=MESH)
        pl.semaphore_signal(barrier, inc=1, device_id={"grid_1": lax.rem(z + d, 4)}, device_id_type=MESH)
        pl.semaphore_signal(barrier, inc=1, device_id={"orb": lax.rem(me + d, 4)}, device_id_type=MESH)

    def load(part):
        return pltpu.make_async_copy(
            orb_hbm.at[:, pl.ds(pl.multiple_of(part * PART, PART), PART)], orb.at[part], local_sem.at[part]
        )

    order = []
    for owner in (across, left, right, me):
        order += [2 * owner, 2 * owner + 1]
    for part in order:
        load(part).start()

    def remote(src, dst, slot, where):
        return pltpu.make_async_remote_copy(
            src_ref=src, dst_ref=dst, send_sem=send_sem.at[slot], recv_sem=recv_sem.at[slot],
            device_id=where, device_id_type=MESH,
        )

    started = []

    def go(src, dst, slot, where):
        copy = remote(src, dst, slot, where)
        copy.start()
        started.append(copy)
        return copy

    pl.semaphore_wait(barrier, 10)
    load(order[0]).wait()
    load(order[1]).wait()
    far_a = go(orb.at[2 * across], far.at[0], FAR, {"orb": left})
    far_b = go(orb.at[2 * across + 1], far.at[1], FAR + 1, {"orb": right})
    for part in order[2:]:
        load(part).wait()
    near_b = go(orb.at[2 * left + 1], near.at[1], NEAR + 1, {"orb": left})
    near_a = go(orb.at[2 * right], near.at[0], NEAR, {"orb": right})

    base = ((x * 4 + z) * 2 + core) * ROWS
    gathered[...] = jnp.zeros_like(gathered)
    here = piv_ref[...] - base

    def extract(part, carry):
        spots = lax.broadcasted_iota(jnp.int32, (RANK, PART), 1) + part * PART
        chosen = jnp.where(spots == here, 1.0, 0.0).astype(jnp.bfloat16)
        gathered[:, 0:DEPTH] += nt(chosen, orb[part])
        return carry

    lax.fori_loop(0, ROWS // PART, extract, 0)
    for h in range(2):
        for lane in range(4):
            for s in range(STEPS):
                a0[h, lane, s] = gathered[
                    s * PIV + h * HALF : s * PIV + (h + 1) * HALF, lane * 128 : (lane + 1) * 128
                ].astype(jnp.bfloat16)

    go(a0.at[other], r0, CORE_A, {"grid_2": other}).wait_recv()
    r0[...] = (r0[...].astype(jnp.float32) + a0[core].astype(jnp.float32)).astype(jnp.bfloat16)
    copies = []
    for d in (1, 2, 3):
        there = lax.rem(x + d, 4)
        copies.append(go(r0.at[there], r1.at[d - 1], X_A + d - 1, {"grid_0": there}))
    for copy in copies:
        copy.wait_recv()
    total = r0[x].astype(jnp.float32)
    for d in range(3):
        total += r1[d].astype(jnp.float32)
    a2[0:STEPS] = total.astype(jnp.bfloat16)
    a2[STEPS] = jnp.zeros((HALF, 128), jnp.bfloat16)
    copies = []
    for d in (1, 2, 3):
        there = lax.rem(z + d, 4)
        copies.append(go(a2.at[there], r2.at[d - 1], Z_A + d - 1, {"grid_1": there}))
    for copy in copies:
        copy.wait_recv()
    total = a2[z].astype(jnp.float32)
    for d in range(3):
        total += r2[d].astype(jnp.float32)
    pv[core, x, z, me] = total.astype(jnp.bfloat16)
    mine = pv.at[core, x, z, me]
    copies = [go(mine, mine, Y_A + d - 1, {"orb": lax.rem(me + d, 4)}) for d in (1, 2, 3)]
    for copy in copies:
        copy.wait_recv()
    mine = pv.at[core, x, z]
    copies = [go(mine, mine, Z_B + d - 1, {"grid_1": lax.rem(z + d, 4)}) for d in (1, 2, 3)]
    for copy in copies:
        copy.wait_recv()
    mine = pv.at[core, x, 0:STEPS]
    copies = [go(mine, mine, X_B + d - 1, {"grid_0": lax.rem(x + d, 4)}) for d in (1, 2, 3)]
    for copy in copies:
        copy.wait_recv()
    mine = pv.at[core, :, 0:STEPS]
    go(mine, mine, CORE_B, {"grid_2": other}).wait_recv()
    for h in range(2):
        for lane in range(4):
            for s in range(STEPS):
                for y in range(4):
                    picked[y, s * PIV + h * HALF : s * PIV + (h + 1) * HALF, lane * 128 : (lane + 1) * 128] = (
                        pv[h, lane, s, y]
                    )

    def squares(values):
        wide = values.astype(jnp.float32)
        return jnp.sum(wide * wide, axis=0, keepdims=True)

    far_a.wait_recv()
    far_b.wait_recv()

    def send_sums(t):
        return [
            remote(sums_out.at[0, t], sums_in.at[0, t], SUM + 2 * t, {"orb": left}),
            remote(sums_out.at[1, t], sums_in.at[1, t], SUM + 2 * t + 1, {"orb": right}),
        ]

    def middle(t, carry):
        span = pl.ds(pl.multiple_of(t * PIECE, PIECE), PIECE)
        for h, (own, source) in enumerate(((2 * left, right), (2 * right + 1, left))):
            a = orb[own, :, span]
            b = far[h, :, span]
            sums_out[h, t, 0:RANK] = nn(picked[me, :, 0:DEPTH], a) + nn(picked[source, :, 0:DEPTH], b)
            sums_out[h, t, RANK:SUMS] = jnp.broadcast_to(squares(a) + squares(b), (8, PIECE))
        for copy in send_sums(t):
            copy.start()
        return carry

    lax.fori_loop(0, PIECES, middle, 0)

    pairs = nt(picked[0], picked[0])
    for y in range(1, 4):
        pairs += nt(picked[y], picked[y])
    block = jnp.square(pairs * (1.0 / ORB))
    for i in range(STEPS):
        for j in range(i + 1):
            gram[3 * i + j] = block[i * PIV : (i + 1) * PIV, j * PIV : (j + 1) * PIV]

    def diagonal_inverse(i, carry):
        def update(k, carry):
            gram[4 * i] -= nt(low[3 * i + k], low[3 * i + k], HIGHEST)
            return carry

        lax.fori_loop(0, i, update, 0)
        inv[4 * i] = inverse_factor(gram[4 * i])

        def panel(j, carry):
            def update(k, carry):
                gram[3 * j + i] -= nt(low[3 * j + k], low[3 * i + k], HIGHEST)
                return carry

            lax.fori_loop(0, i, update, 0)
            low[3 * j + i] = nt(gram[3 * j + i], inv[4 * i], HIGHEST)
            return carry

        lax.fori_loop(i + 1, STEPS, panel, 0)
        return carry

    lax.fori_loop(0, STEPS, diagonal_inverse, 0)
    inv[3] = -nn(inv[4], nn(low[3], inv[0], HIGHEST), HIGHEST)
    inv[7] = -nn(inv[8], nn(low[7], inv[4], HIGHEST), HIGHEST)
    inv[6] = -nn(inv[8], nn(low[6], inv[0], HIGHEST) + nn(low[7], inv[3], HIGHEST), HIGHEST)

    near_a.wait_recv()
    near_b.wait_recv()

    def finish(t, best):
        for copy in send_sums(t):
            copy.wait_recv()
        best = list(best)
        for h, source in enumerate((left, right)):
            span = pl.ds(pl.multiple_of(t * PIECE, PIECE), PIECE)
            a = orb[2 * me + h, :, span]
            b = near[h, :, span]
            inner = sums_in[h, t, 0:RANK] + nn(picked[me, :, 0:DEPTH], a) + nn(picked[source, :, 0:DEPTH], b)
            columns = jnp.square(inner * (1.0 / ORB))
            rest = jnp.square((sums_in[h, t, RANK : RANK + 1] + squares(a) + squares(b)) * (1.0 / ORB))
            out = pl.ds(pl.multiple_of(h * PART + t * PIECE, PIECE), PIECE)
            for i in range(STEPS):
                fresh = nn(inv[3 * i], columns[0:PIV], HIGHEST)
                for j in range(1, i + 1):
                    fresh += nn(inv[3 * i + j], columns[j * PIV : (j + 1) * PIV], HIGHEST)
                factor_ref[i * PIV : (i + 1) * PIV, out] = fresh
                rest -= jnp.sum(fresh * fresh, axis=0, keepdims=True)
                best[i] = jnp.maximum(best[i], rest)
            diag_ref[:, out] = rest
        return tuple(best)

    low_start = jnp.full((1, PIECE), -jnp.inf, jnp.float32)
    best = lax.fori_loop(0, PIECES, finish, (low_start,) * STEPS)
    rows = lax.broadcasted_iota(jnp.int32, (8, 128), 0)
    peak = jnp.full((8, 128), -jnp.inf, jnp.float32)
    for i in range(STEPS):
        peak = jnp.where(rows == i, jnp.max(best[i]), peak)

    def spread(peak, at, slot, axis, count, index):
        peak_buf[at] = peak
        copies = [
            go(peak_buf.at[at], peak_buf.at[at + d], slot + d - 1, {axis: lax.rem(index + d, count)})
            for d in range(1, count)
        ]
        for d, copy in enumerate(copies, 1):
            copy.wait_recv()
            peak = jnp.maximum(peak, peak_buf[at + d])
        return peak

    peak = spread(peak, 0, PEAK_CORE, "grid_2", 2, core)
    peak = spread(peak, 2, PEAK_Z, "grid_1", 4, z)
    peak = spread(peak, 6, PEAK_X, "grid_0", 4, x)
    peak = spread(peak, 10, PEAK_Y, "orb", 4, me)
    peak_ref[...] = peak

    for copy in started:
        copy.wait_send()
    for t in range(PIECES):
        for copy in send_sums(t):
            copy.wait_send()


def on_device(orbitals, pivots):
    pivot_column = pivots.reshape(RANK, 1)
    f32, bf16 = jnp.float32, jnp.bfloat16
    vmem = pl.BlockSpec(memory_space=pltpu.VMEM)
    factor, diagonal, peaks = pl.pallas_call(
        kernel,
        out_shape=(
            jax.ShapeDtypeStruct((RANK, SHARE), f32),
            jax.ShapeDtypeStruct((1, SHARE), f32),
            jax.ShapeDtypeStruct((8, 128), f32),
        ),
        in_specs=[pl.BlockSpec(memory_space=pl.ANY), vmem],
        out_specs=(vmem, vmem, vmem),
        scratch_shapes=[
            pltpu.VMEM((ROWS // PART, DEPTH, PART), bf16),
            pltpu.VMEM((RANK, WIDE), f32),
            pltpu.VMEM((2, 4, 4, 4, HALF, 128), bf16),
            pltpu.VMEM((2, 4, STEPS, HALF, 128), bf16),
            pltpu.VMEM((4, STEPS, HALF, 128), bf16),
            pltpu.VMEM((3, STEPS, HALF, 128), bf16),
            pltpu.VMEM((4, HALF, 128), bf16),
            pltpu.VMEM((3, HALF, 128), bf16),
            pltpu.VMEM((4, RANK, WIDE), bf16),
            pltpu.VMEM((2, DEPTH, PART), bf16),
            pltpu.VMEM((2, DEPTH, PART), bf16),
            pltpu.VMEM((2, PIECES, SUMS, PIECE), f32),
            pltpu.VMEM((2, PIECES, SUMS, PIECE), f32),
            pltpu.VMEM((9, PIV, PIV), f32),
            pltpu.VMEM((9, PIV, PIV), f32),
            pltpu.VMEM((9, PIV, PIV), f32),
            pltpu.VMEM((14, 8, 128), f32),
            pltpu.SemaphoreType.DMA((ROWS // PART,)),
            pltpu.SemaphoreType.DMA((SLOTS,)),
            pltpu.SemaphoreType.DMA((SLOTS,)),
        ],
        compiler_params=pltpu.CompilerParams(
            collective_id=0, has_side_effects=True, vmem_limit_bytes=50 * 1024 * 1024
        ),
    )(orbitals, pivot_column)
    return factor.T, diagonal.reshape(SHARE), peaks[:STEPS, 0]


def solution(mesh):
    split = Mesh(
        mesh.devices.reshape(4, 4, 2, mesh.shape["orb"]), ("grid_0", "grid_1", "grid_2", "orb")
    )
    return jax.shard_map(
        on_device,
        mesh=split,
        in_specs=(P("orb", GRID), P()),
        out_specs=(P(GRID_ORB, None), P(GRID_ORB), P()),
        check_vma=False,
    )
```

```python
import functools

import jax
import jax.numpy as jnp
from jax import lax
from jax.experimental import pallas as pl
from jax.experimental.pallas import tpu as pltpu
from jax.sharding import Mesh
from jax.sharding import PartitionSpec as P

ORB = 1800
GRID = ("grid_0", "grid_1", "grid_2")
GRID_ORB = ("grid_0", "grid_1", "grid_2", "orb")
MESH = pl.DeviceIdType.MESH
HIGHEST = lax.Precision.HIGHEST

STEPS = 3
PIV = 96
RANK = STEPS * PIV
HALF = PIV // 2
DEPTH = 450
WIDE = 512
ROWS = 8192
SHARE = 2048
PART = 1024
PIECE = 256
PIECES = PART // PIECE
SUMS = RANK + 8

FIRST = 768

CORE_A, X_A, Z_A, Y_A, X_B, Z_B, X_C, Z_C, CORE_B = 0, 1, 4, 7, 10, 13, 16, 19, 22
FAR, FAR_REST, NEAR, SUM = 23, 25, 27, 29
PEAK_CORE, PEAK_Z, PEAK_X, PEAK_Y = 37, 38, 41, 44
SLOTS = 47


def nt(left, right, precision=None):
    return lax.dot_general(
        left, right, (((1,), (1,)), ((), ())), precision=precision,
        preferred_element_type=jnp.float32,
    )


def nn(left, right, precision=None):
    return lax.dot_general(
        left, right, (((1,), (0,)), ((), ())), precision=precision,
        preferred_element_type=jnp.float32,
    )


def inverse_factor(block):
    lanes = lax.broadcasted_iota(jnp.int32, (8, PIV), 1)
    subs = lax.broadcasted_iota(jnp.int32, (8, PIV), 0)
    groups = PIV // 8
    left = [block[8 * g : 8 * g + 8, :] for g in range(groups)]
    right = [jnp.where(lanes == subs + 8 * g, 1.0, 0.0) for g in range(groups)]

    def row(values, r):
        return jnp.broadcast_to(values[r : r + 1, :], (8, PIV))

    out = []
    for home in range(groups):
        column = {
            (g, j): jnp.broadcast_to(left[g][:, 8 * home + j : 8 * home + j + 1], (8, PIV))
            for g in range(home, groups)
            for j in range(8)
        }
        kept = right[home]
        for r in range(8):
            scale = lax.rsqrt(row(column[home, r], r))
            spread = [row(column[home, r], j) * scale for j in range(r + 1, 8)]
            row_left = row(left[home], r) * scale
            row_right = row(right[home], r) * scale
            kept = jnp.where(subs == r, row_right, kept)
            for g in range(home, groups):
                times = column[g, r] * scale
                if g == home:
                    times = jnp.where(subs > r, times, 0.0)
                left[g] = left[g] - times * row_left
                right[g] = right[g] - times * row_right
                for j in range(r + 1, 8):
                    column[g, j] = column[g, j] - times * spread[j - r - 1]
        out.append(kept)
    return jnp.concatenate(out, axis=0)


def kernel(
    orb_hbm, piv_ref, factor_ref, diag_ref, peak_ref,
    orb, gathered, pv, a0, r0, r1, a2, r2, picked, far, near, sums_out, sums_in, own,
    gram, low, inv, peak_buf, local_sem, send_sem, recv_sem,
):
    x = lax.axis_index("grid_0")
    z = lax.axis_index("grid_1")
    core = lax.axis_index("grid_2")
    me = lax.axis_index("orb")
    right, left, across = lax.rem(me + 1, 4), lax.rem(me + 3, 4), lax.rem(me + 2, 4)
    other = 1 - core

    barrier = pltpu.get_barrier_semaphore()
    pl.semaphore_signal(barrier, inc=1, device_id={"grid_2": other}, device_id_type=MESH)
    for d in (1, 2, 3):
        pl.semaphore_signal(barrier, inc=1, device_id={"grid_0": lax.rem(x + d, 4)}, device_id_type=MESH)
        pl.semaphore_signal(barrier, inc=1, device_id={"grid_1": lax.rem(z + d, 4)}, device_id_type=MESH)
        pl.semaphore_signal(barrier, inc=1, device_id={"orb": lax.rem(me + d, 4)}, device_id_type=MESH)

    def load(part):
        return pltpu.make_async_copy(
            orb_hbm.at[:, pl.ds(pl.multiple_of(part * PART, PART), PART)], orb.at[part], local_sem.at[part]
        )

    def part_at(i):
        return 2 * lax.rem(me + 2 + lax.div(i, 2), 4) + lax.rem(i, 2)

    for i in range(ROWS // PART):
        load(part_at(i)).start()

    def remote(src, dst, slot, where):
        return pltpu.make_async_remote_copy(
            src_ref=src, dst_ref=dst, send_sem=send_sem.at[slot], recv_sem=recv_sem.at[slot],
            device_id=where, device_id_type=MESH,
        )

    started = []

    def go(src, dst, slot, where):
        copy = remote(src, dst, slot, where)
        copy.start()
        started.append(copy)
        return copy

    base = ((x * 4 + z) * 2 + core) * ROWS
    gathered[...] = jnp.zeros_like(gathered)
    here = piv_ref[...] - base

    def extract(i, carry):
        part = part_at(i)
        load(part).wait()
        spots = lax.broadcasted_iota(jnp.int32, (RANK, PART), 1) + part * PART
        chosen = jnp.where(spots == here, 1.0, 0.0).astype(jnp.bfloat16)
        gathered[:, 0:DEPTH] += nt(chosen, orb[part])
        return carry

    lax.fori_loop(0, 2, extract, 0)
    pl.semaphore_wait(barrier, 10)

    def far_copies(low, high, slot):
        span = slice(low, high)
        return [
            go(orb.at[2 * across, :, span], far.at[0, :, span], slot, {"orb": left}),
            go(orb.at[2 * across + 1, :, span], far.at[1, :, span], slot + 1, {"orb": right}),
        ]

    far_all = far_copies(0, FIRST, FAR)
    lax.fori_loop(2, ROWS // PART, extract, 0)
    for h in range(2):
        for lane in range(4):
            for s in range(STEPS):
                a0[h, lane, s] = gathered[
                    s * PIV + h * HALF : s * PIV + (h + 1) * HALF, lane * 128 : (lane + 1) * 128
                ].astype(jnp.bfloat16)

    go(a0.at[other], r0, CORE_A, {"grid_2": other}).wait_recv()
    r0[...] = (r0[...].astype(jnp.float32) + a0[core].astype(jnp.float32)).astype(jnp.bfloat16)
    copies = []
    for d in (1, 2, 3):
        there = lax.rem(x + d, 4)
        copies.append(go(r0.at[there], r1.at[d - 1], X_A + d - 1, {"grid_0": there}))
    for copy in copies:
        copy.wait_recv()
    total = r0[x].astype(jnp.float32)
    for d in range(3):
        total += r1[d].astype(jnp.float32)
    a2[0:STEPS] = total.astype(jnp.bfloat16)
    a2[STEPS] = jnp.zeros((HALF, 128), jnp.bfloat16)
    copies = []
    for d in (1, 2, 3):
        there = lax.rem(z + d, 4)
        copies.append(go(a2.at[there], r2.at[d - 1], Z_A + d - 1, {"grid_1": there}))
    for copy in copies:
        copy.wait_recv()
    total = a2[z].astype(jnp.float32)
    for d in range(3):
        total += r2[d].astype(jnp.float32)
    pv[core, x, z, me] = total.astype(jnp.bfloat16)
    mine = pv.at[core, x, z, me]
    copies = [go(mine, mine, Y_A + d - 1, {"orb": lax.rem(me + d, 4)}) for d in (1, 2, 3)]
    far_all += far_copies(FIRST, PART, FAR_REST)
    near_all = [
        go(orb.at[2 * left + 1], near.at[1], NEAR + 1, {"orb": left}),
        go(orb.at[2 * right], near.at[0], NEAR, {"orb": right}),
    ]
    for copy in copies:
        copy.wait_recv()
    copies = []
    for d in (1, 2, 3):
        mine = pv.at[core, x, z, 0:2]
        copies.append(go(mine, mine, X_B + d - 1, {"grid_0": lax.rem(x + d, 4)}))
        mine = pv.at[core, x, z, 2:4]
        copies.append(go(mine, mine, Z_B + d - 1, {"grid_1": lax.rem(z + d, 4)}))
    for copy in copies:
        copy.wait_recv()
    copies = []
    for d in (1, 2, 3):
        mine = pv.at[core, :, z, 0:2]
        copies.append(go(mine, mine, Z_C + d - 1, {"grid_1": lax.rem(z + d, 4)}))
        mine = pv.at[core, x, 0:STEPS, 2:4]
        copies.append(go(mine, mine, X_C + d - 1, {"grid_0": lax.rem(x + d, 4)}))
    for copy in copies:
        copy.wait_recv()
    mine = pv.at[core, :, 0:STEPS]
    go(mine, mine, CORE_B, {"grid_2": other}).wait_recv()
    for h in range(2):
        for lane in range(4):
            for s in range(STEPS):
                for y in range(4):
                    picked[y, s * PIV + h * HALF : s * PIV + (h + 1) * HALF, lane * 128 : (lane + 1) * 128] = (
                        pv[h, lane, s, y]
                    )

    def squares(values):
        wide = values.astype(jnp.float32)
        return jnp.sum(wide * wide, axis=0, keepdims=True)

    for copy in far_all:
        copy.wait_recv()

    def send_sums(t):
        return [
            remote(sums_out.at[0, t], sums_in.at[0, t], SUM + 2 * t, {"orb": left}),
            remote(sums_out.at[1, t], sums_in.at[1, t], SUM + 2 * t + 1, {"orb": right}),
        ]

    def middle(t, carry):
        span = pl.ds(pl.multiple_of(t * PIECE, PIECE), PIECE)
        for h, (own, source) in enumerate(((2 * left, right), (2 * right + 1, left))):
            a = orb[own, :, span]
            b = far[h, :, span]
            sums_out[h, t, 0:RANK] = nn(picked[me, :, 0:DEPTH], a) + nn(picked[source, :, 0:DEPTH], b)
            sums_out[h, t, RANK:SUMS] = jnp.broadcast_to(squares(a) + squares(b), (8, PIECE))
        for copy in send_sums(t):
            copy.start()
        return carry

    lax.fori_loop(0, PIECES, middle, 0)

    pairs = nt(picked[0], picked[0])
    for y in range(1, 4):
        pairs += nt(picked[y], picked[y])
    block = jnp.square(pairs * (1.0 / ORB))
    for i in range(STEPS):
        for j in range(i + 1):
            gram[3 * i + j] = block[i * PIV : (i + 1) * PIV, j * PIV : (j + 1) * PIV]

    def diagonal_inverse(i, carry):
        def update(k, carry):
            gram[4 * i] -= nt(low[3 * i + k], low[3 * i + k], HIGHEST)
            return carry

        lax.fori_loop(0, i, update, 0)
        inv[4 * i] = inverse_factor(gram[4 * i])

        def panel(j, carry):
            def update(k, carry):
                gram[3 * j + i] -= nt(low[3 * j + k], low[3 * i + k], HIGHEST)
                return carry

            lax.fori_loop(0, i, update, 0)
            low[3 * j + i] = nt(gram[3 * j + i], inv[4 * i], HIGHEST)
            return carry

        lax.fori_loop(i + 1, STEPS, panel, 0)
        return carry

    lax.fori_loop(0, STEPS, diagonal_inverse, 0)
    inv[3] = -nn(inv[4], nn(low[3], inv[0], HIGHEST), HIGHEST)
    inv[7] = -nn(inv[8], nn(low[7], inv[4], HIGHEST), HIGHEST)
    inv[6] = -nn(inv[8], nn(low[6], inv[0], HIGHEST) + nn(low[7], inv[3], HIGHEST), HIGHEST)

    for copy in near_all:
        copy.wait_recv()

    def own_products(t, carry):
        span = pl.ds(pl.multiple_of(t * PIECE, PIECE), PIECE)
        for h, source in enumerate((left, right)):
            a = orb[2 * me + h, :, span]
            b = near[h, :, span]
            own[h, t, 0:RANK] = nn(picked[me, :, 0:DEPTH], a) + nn(picked[source, :, 0:DEPTH], b)
            own[h, t, RANK:SUMS] = jnp.broadcast_to(squares(a) + squares(b), (8, PIECE))
        return carry

    lax.fori_loop(0, PIECES, own_products, 0)

    def finish(t, best):
        for copy in send_sums(t):
            copy.wait_recv()
        best = list(best)
        for h in range(2):
            columns = jnp.square((sums_in[h, t, 0:RANK] + own[h, t, 0:RANK]) * (1.0 / ORB))
            rest = jnp.square((sums_in[h, t, RANK : RANK + 1] + own[h, t, RANK : RANK + 1]) * (1.0 / ORB))
            out = pl.ds(pl.multiple_of(h * PART + t * PIECE, PIECE), PIECE)
            for i in range(STEPS):
                fresh = nn(inv[3 * i], columns[0:PIV], HIGHEST)
                for j in range(1, i + 1):
                    fresh += nn(inv[3 * i + j], columns[j * PIV : (j + 1) * PIV], HIGHEST)
                factor_ref[i * PIV : (i + 1) * PIV, out] = fresh
                rest -= jnp.sum(fresh * fresh, axis=0, keepdims=True)
                best[i] = jnp.maximum(best[i], rest)
            diag_ref[:, out] = rest
        return tuple(best)

    low_start = jnp.full((1, PIECE), -jnp.inf, jnp.float32)
    best = lax.fori_loop(0, PIECES, finish, (low_start,) * STEPS)
    rows = lax.broadcasted_iota(jnp.int32, (8, 128), 0)
    peak = jnp.full((8, 128), -jnp.inf, jnp.float32)
    for i in range(STEPS):
        peak = jnp.where(rows == i, jnp.max(best[i]), peak)

    def spread(peak, at, slot, axis, count, index):
        peak_buf[at] = peak
        copies = [
            go(peak_buf.at[at], peak_buf.at[at + d], slot + d - 1, {axis: lax.rem(index + d, count)})
            for d in range(1, count)
        ]
        for d, copy in enumerate(copies, 1):
            copy.wait_recv()
            peak = jnp.maximum(peak, peak_buf[at + d])
        return peak

    peak = spread(peak, 0, PEAK_CORE, "grid_2", 2, core)
    peak = spread(peak, 2, PEAK_Z, "grid_1", 4, z)
    peak = spread(peak, 6, PEAK_X, "grid_0", 4, x)
    peak = spread(peak, 10, PEAK_Y, "orb", 4, me)
    peak_ref[...] = peak

    for copy in started:
        copy.wait_send()
    for t in range(PIECES):
        for copy in send_sums(t):
            copy.wait_send()


def on_device(orbitals, pivots):
    pivot_column = pivots.reshape(RANK, 1)
    f32, bf16 = jnp.float32, jnp.bfloat16
    vmem = pl.BlockSpec(memory_space=pltpu.VMEM)
    factor, diagonal, peaks = pl.pallas_call(
        kernel,
        out_shape=(
            jax.ShapeDtypeStruct((RANK, SHARE), f32),
            jax.ShapeDtypeStruct((1, SHARE), f32),
            jax.ShapeDtypeStruct((8, 128), f32),
        ),
        in_specs=[pl.BlockSpec(memory_space=pl.ANY), vmem],
        out_specs=(vmem, vmem, vmem),
        scratch_shapes=[
            pltpu.VMEM((ROWS // PART, DEPTH, PART), bf16),
            pltpu.VMEM((RANK, WIDE), f32),
            pltpu.VMEM((2, 4, 4, 4, HALF, 128), bf16),
            pltpu.VMEM((2, 4, STEPS, HALF, 128), bf16),
            pltpu.VMEM((4, STEPS, HALF, 128), bf16),
            pltpu.VMEM((3, STEPS, HALF, 128), bf16),
            pltpu.VMEM((4, HALF, 128), bf16),
            pltpu.VMEM((3, HALF, 128), bf16),
            pltpu.VMEM((4, RANK, WIDE), bf16),
            pltpu.VMEM((2, DEPTH, PART), bf16),
            pltpu.VMEM((2, DEPTH, PART), bf16),
            pltpu.VMEM((2, PIECES, SUMS, PIECE), f32),
            pltpu.VMEM((2, PIECES, SUMS, PIECE), f32),
            pltpu.VMEM((2, PIECES, SUMS, PIECE), f32),
            pltpu.VMEM((9, PIV, PIV), f32),
            pltpu.VMEM((9, PIV, PIV), f32),
            pltpu.VMEM((9, PIV, PIV), f32),
            pltpu.VMEM((14, 8, 128), f32),
            pltpu.SemaphoreType.DMA((ROWS // PART,)),
            pltpu.SemaphoreType.DMA((SLOTS,)),
            pltpu.SemaphoreType.DMA((SLOTS,)),
        ],
        compiler_params=pltpu.CompilerParams(
            collective_id=0, has_side_effects=True, vmem_limit_bytes=50 * 1024 * 1024
        ),
    )(orbitals, pivot_column)
    return factor.T, diagonal.reshape(SHARE), peaks[:STEPS, 0]


def solution(mesh):
    split = Mesh(
        mesh.devices.reshape(4, 4, 2, mesh.shape["orb"]), ("grid_0", "grid_1", "grid_2", "orb")
    )
    return jax.shard_map(
        on_device,
        mesh=split,
        in_specs=(P("orb", GRID), P()),
        out_specs=(P(GRID_ORB, None), P(GRID_ORB), P()),
        check_vma=False,
    )
```

```python
import functools

import jax
import jax.numpy as jnp
from jax import lax
from jax.experimental import pallas as pl
from jax.experimental.pallas import tpu as pltpu
from jax.sharding import Mesh
from jax.sharding import PartitionSpec as P

ORB = 1800
GRID = ("grid_0", "grid_1", "grid_2")
GRID_ORB = ("grid_0", "grid_1", "grid_2", "orb")
MESH = pl.DeviceIdType.MESH
HIGHEST = lax.Precision.HIGHEST

STEPS = 3
PIV = 96
RANK = STEPS * PIV
HALF = PIV // 2
DEPTH = 450
WIDE = 512
ROWS = 8192
SHARE = 2048
PART = 1024
PIECE = 256
PIECES = PART // PIECE
WORDS = 2 * PIV
FIELD = 21
SCALE = float(2 ** (FIELD - 1) - 64)
TINY = 1e-30

CORE_A, X_A, Z_A, Y_A, X_B, Z_B, X_C, Z_C, CORE_B = 0, 1, 4, 7, 10, 13, 16, 19, 22
FAR, NEAR, NORM, SUM = 23, 25, 27, 29
PEAK_A, PEAK_B = 37, 44
SLOTS = 59


def nt(left, right, precision=None):
    return lax.dot_general(
        left, right, (((1,), (1,)), ((), ())), precision=precision,
        preferred_element_type=jnp.float32,
    )


def nn(left, right, precision=None):
    return lax.dot_general(
        left, right, (((1,), (0,)), ((), ())), precision=precision,
        preferred_element_type=jnp.float32,
    )


def inverse_factor(block):
    lanes = lax.broadcasted_iota(jnp.int32, (8, PIV), 1)
    subs = lax.broadcasted_iota(jnp.int32, (8, PIV), 0)
    groups = PIV // 8
    left = [block[8 * g : 8 * g + 8, :] for g in range(groups)]
    right = [jnp.where(lanes == subs + 8 * g, 1.0, 0.0) for g in range(groups)]

    def row(values, r):
        return jnp.broadcast_to(values[r : r + 1, :], (8, PIV))

    out = []
    for home in range(groups):
        column = {
            (g, j): jnp.broadcast_to(left[g][:, 8 * home + j : 8 * home + j + 1], (8, PIV))
            for g in range(home, groups)
            for j in range(8)
        }
        kept = right[home]
        for r in range(8):
            scale = lax.rsqrt(row(column[home, r], r))
            spread = [row(column[home, r], j) * scale for j in range(r + 1, 8)]
            row_left = row(left[home], r) * scale
            row_right = row(right[home], r) * scale
            kept = jnp.where(subs == r, row_right, kept)
            for g in range(home, groups):
                times = column[g, r] * scale
                if g == home:
                    times = jnp.where(subs > r, times, 0.0)
                left[g] = left[g] - times * row_left
                right[g] = right[g] - times * row_right
                for j in range(r + 1, 8):
                    column[g, j] = column[g, j] - times * spread[j - r - 1]
        out.append(kept)
    return jnp.concatenate(out, axis=0)


def kernel(
    orb_hbm, piv_hbm, factor_ref, diag_ref, peak_ref,
    pivots, orb, gathered, pv, a0, r0, r1, a2, r2, picked, far, near, sums_out, sums_in, own,
    norm_out, norm_in, own_squares, norm_own, pack, unpack, gram, low, inv, peak_buf, local_sem, send_sem, recv_sem,
):
    x = lax.axis_index("grid_0")
    z = lax.axis_index("grid_1")
    core = lax.axis_index("grid_2")
    me = lax.axis_index("orb")
    right, left, across = lax.rem(me + 1, 4), lax.rem(me + 3, 4), lax.rem(me + 2, 4)
    other = 1 - core

    barrier = pltpu.get_barrier_semaphore()
    pl.semaphore_signal(barrier, inc=1, device_id={"grid_2": other}, device_id_type=MESH)
    for d in (1, 2, 3):
        pl.semaphore_signal(barrier, inc=1, device_id={"grid_0": lax.rem(x + d, 4)}, device_id_type=MESH)
        pl.semaphore_signal(barrier, inc=1, device_id={"grid_1": lax.rem(z + d, 4)}, device_id_type=MESH)
        pl.semaphore_signal(barrier, inc=1, device_id={"orb": lax.rem(me + d, 4)}, device_id_type=MESH)

    def load(part):
        return pltpu.make_async_copy(
            orb_hbm.at[:, pl.ds(pl.multiple_of(part * PART, PART), PART)], orb.at[part], local_sem.at[part]
        )

    def part_at(i):
        return 2 * lax.rem(me + 2 + lax.div(i, 2), 4) + lax.rem(i, 2)

    load_pivots = pltpu.make_async_copy(piv_hbm, pivots, local_sem.at[ROWS // PART])
    load_pivots.start()
    for i in range(ROWS // PART):
        load(part_at(i)).start()

    def remote(src, dst, slot, where):
        return pltpu.make_async_remote_copy(
            src_ref=src, dst_ref=dst, send_sem=send_sem.at[slot], recv_sem=recv_sem.at[slot],
            device_id=where, device_id_type=MESH,
        )

    started = []

    def go(src, dst, slot, where):
        copy = remote(src, dst, slot, where)
        copy.start()
        started.append(copy)
        return copy

    base = ((x * 4 + z) * 2 + core) * ROWS
    gathered[...] = jnp.zeros_like(gathered)
    load_pivots.wait()
    square = (PIV, PIV)
    eye = lax.broadcasted_iota(jnp.int32, square, 0) == lax.broadcasted_iota(jnp.int32, square, 1)
    here = jnp.concatenate(
        [
            jnp.sum(
                jnp.where(eye, jnp.broadcast_to(pivots[s : s + 1].astype(jnp.float32), square), 0.0),
                axis=1, keepdims=True,
            )
            for s in range(STEPS)
        ],
        axis=0,
    ).astype(jnp.int32) - base

    def extract(i, carry):
        part = part_at(i)
        load(part).wait()
        spots = lax.broadcasted_iota(jnp.int32, (RANK, PART), 1) + part * PART
        chosen = jnp.where(spots == here, 1.0, 0.0).astype(jnp.bfloat16)
        gathered[:, 0:DEPTH] += nt(chosen, orb[part])
        return carry

    lax.fori_loop(0, 2, extract, 0)
    pl.semaphore_wait(barrier, 10)

    far_all = [
        go(orb.at[2 * across], far.at[0], FAR, {"orb": left}),
        go(orb.at[2 * across + 1], far.at[1], FAR + 1, {"orb": right}),
    ]
    lax.fori_loop(2, ROWS // PART, extract, 0)
    for h in range(2):
        for lane in range(4):
            for s in range(STEPS):
                a0[h, lane, s] = gathered[
                    s * PIV + h * HALF : s * PIV + (h + 1) * HALF, lane * 128 : (lane + 1) * 128
                ].astype(jnp.bfloat16)

    go(a0.at[other], r0, CORE_A, {"grid_2": other}).wait_recv()
    r0[...] = (r0[...].astype(jnp.float32) + a0[core].astype(jnp.float32)).astype(jnp.bfloat16)
    copies = []
    for d in (1, 2, 3):
        there = lax.rem(x + d, 4)
        copies.append(go(r0.at[there], r1.at[d - 1], X_A + d - 1, {"grid_0": there}))
    for copy in copies:
        copy.wait_recv()
    total = r0[x].astype(jnp.float32)
    for d in range(3):
        total += r1[d].astype(jnp.float32)
    a2[0:STEPS] = total.astype(jnp.bfloat16)
    a2[STEPS] = jnp.zeros((HALF, 128), jnp.bfloat16)
    copies = []
    for d in (1, 2, 3):
        there = lax.rem(z + d, 4)
        copies.append(go(a2.at[there], r2.at[d - 1], Z_A + d - 1, {"grid_1": there}))
    for copy in copies:
        copy.wait_recv()
    total = a2[z].astype(jnp.float32)
    for d in range(3):
        total += r2[d].astype(jnp.float32)
    pv[core, x, z, me] = total.astype(jnp.bfloat16)
    mine = pv.at[core, x, z, me]
    copies = [go(mine, mine, Y_A + d - 1, {"orb": lax.rem(me + d, 4)}) for d in (1, 2, 3)]
    near_all = [
        go(orb.at[2 * left + 1], near.at[1], NEAR + 1, {"orb": left}),
        go(orb.at[2 * right], near.at[0], NEAR, {"orb": right}),
    ]
    for copy in copies:
        copy.wait_recv()
    copies = []
    for d in (1, 2, 3):
        mine = pv.at[core, x, z, 0:2]
        copies.append(go(mine, mine, X_B + d - 1, {"grid_0": lax.rem(x + d, 4)}))
        mine = pv.at[core, x, z, 2:4]
        copies.append(go(mine, mine, Z_B + d - 1, {"grid_1": lax.rem(z + d, 4)}))
    for copy in copies:
        copy.wait_recv()
    copies = []
    for d in (1, 2, 3):
        mine = pv.at[core, :, z, 0:2]
        copies.append(go(mine, mine, Z_C + d - 1, {"grid_1": lax.rem(z + d, 4)}))
        mine = pv.at[core, x, 0:STEPS, 2:4]
        copies.append(go(mine, mine, X_C + d - 1, {"grid_0": lax.rem(x + d, 4)}))

    def squares(values):
        wide = values.astype(jnp.float32)
        return jnp.sum(wide * wide, axis=0, keepdims=True)

    for copy in far_all:
        copy.wait_recv()

    def norms(t, carry):
        span = pl.ds(pl.multiple_of(t * PIECE, PIECE), PIECE)
        for h, owned in enumerate((2 * left, 2 * right + 1)):
            norm_out[h, :, span] = squares(orb[owned, :, span]) + squares(far[h, :, span])
        return carry

    lax.fori_loop(0, PIECES, norms, 0)
    norm_copies = [
        go(norm_out.at[0], norm_in.at[0], NORM, {"orb": left}),
        go(norm_out.at[1], norm_in.at[1], NORM + 1, {"orb": right}),
    ]
    for copy in copies:
        copy.wait_recv()
    mine = pv.at[core, :, 0:STEPS]
    go(mine, mine, CORE_B, {"grid_2": other}).wait_recv()
    for h in range(2):
        for lane in range(4):
            for s in range(STEPS):
                for y in range(4):
                    picked[y, s * PIV + h * HALF : s * PIV + (h + 1) * HALF, lane * 128 : (lane + 1) * 128] = (
                        pv[h, lane, s, y]
                    )

    for y in range(4):
        wide = picked[y].astype(jnp.float32)
        norm_own[y] = jnp.broadcast_to(jnp.sum(wide * wide, axis=1, keepdims=True), (RANK, PIECE))
    for h, (beside, beyond) in enumerate(((right, across), (left, across))):
        pack[h] = lax.rsqrt(jnp.maximum(norm_own[me] + norm_own[beside], TINY)) * SCALE
        far_norm = jnp.maximum(norm_own[beside] + norm_own[beyond], TINY)
        unpack[h] = far_norm * lax.rsqrt(far_norm) * (1.0 / SCALE)

    def send_sums(t):
        return [
            remote(sums_out.at[0, t], sums_in.at[0, t], SUM + 2 * t, {"orb": left}),
            remote(sums_out.at[1, t], sums_in.at[1, t], SUM + 2 * t + 1, {"orb": right}),
        ]

    def middle(t, carry):
        span = pl.ds(pl.multiple_of(t * PIECE, PIECE), PIECE)
        for h, (own, source) in enumerate(((2 * left, right), (2 * right + 1, left))):
            a = orb[own, :, span]
            b = far[h, :, span]
            product = nn(picked[me, :, 0:DEPTH], a) + nn(picked[source, :, 0:DEPTH], b)
            over = lax.rsqrt(jnp.maximum(norm_out[h, :, span], TINY))
            whole = jnp.round(product * pack[h] * over).astype(jnp.int32)
            last = whole[2 * PIV : RANK]
            mask = (1 << FIELD) - 1
            sums_out[h, t, 0:PIV] = (whole[0:PIV] & mask) | (last << FIELD)
            sums_out[h, t, PIV:WORDS] = (whole[PIV : 2 * PIV] & mask) | ((last >> (32 - FIELD)) << FIELD)
        for copy in send_sums(t):
            copy.start()
        return carry

    lax.fori_loop(0, PIECES, middle, 0)

    pairs = nt(picked[0], picked[0])
    for y in range(1, 4):
        pairs += nt(picked[y], picked[y])
    block = jnp.square(pairs * (1.0 / ORB))
    for i in range(STEPS):
        for j in range(i + 1):
            gram[3 * i + j] = block[i * PIV : (i + 1) * PIV, j * PIV : (j + 1) * PIV]

    def diagonal_inverse(i, carry):
        def update(k, carry):
            gram[4 * i] -= nt(low[3 * i + k], low[3 * i + k], HIGHEST)
            return carry

        lax.fori_loop(0, i, update, 0)
        inv[4 * i] = inverse_factor(gram[4 * i])

        def panel(j, carry):
            def update(k, carry):
                gram[3 * j + i] -= nt(low[3 * j + k], low[3 * i + k], HIGHEST)
                return carry

            lax.fori_loop(0, i, update, 0)
            low[3 * j + i] = nt(gram[3 * j + i], inv[4 * i], HIGHEST)
            return carry

        lax.fori_loop(i + 1, STEPS, panel, 0)
        return carry

    lax.fori_loop(0, STEPS, diagonal_inverse, 0)
    inv[3] = -nn(inv[4], nn(low[3], inv[0], HIGHEST), HIGHEST)
    inv[7] = -nn(inv[8], nn(low[7], inv[4], HIGHEST), HIGHEST)
    inv[6] = -nn(inv[8], nn(low[6], inv[0], HIGHEST) + nn(low[7], inv[3], HIGHEST), HIGHEST)

    for copy in near_all + norm_copies:
        copy.wait_recv()

    def own_products(t, carry):
        span = pl.ds(pl.multiple_of(t * PIECE, PIECE), PIECE)
        for h, source in enumerate((left, right)):
            a = orb[2 * me + h, :, span]
            b = near[h, :, span]
            own[h, t] = nn(picked[me, :, 0:DEPTH], a) + nn(picked[source, :, 0:DEPTH], b)
            own_squares[h, :, span] = squares(a) + squares(b)
        return carry

    lax.fori_loop(0, PIECES, own_products, 0)

    def finish(t, best):
        for copy in send_sums(t):
            copy.wait_recv()
        best = list(best)
        for h in range(2):
            span = pl.ds(pl.multiple_of(t * PIECE, PIECE), PIECE)
            first, second = sums_in[h, t, 0:PIV], sums_in[h, t, PIV:WORDS]
            spare = 32 - FIELD
            whole = jnp.concatenate(
                [
                    (first << spare) >> spare,
                    (second << spare) >> spare,
                    ((second >> FIELD) << spare) | lax.shift_right_logical(first, FIELD),
                ],
                axis=0,
            ).astype(jnp.float32)
            norm = norm_in[h, :, span]
            bounded = jnp.maximum(norm, TINY)
            arrived = whole * unpack[h] * (bounded * lax.rsqrt(bounded))
            columns = jnp.square((arrived + own[h, t]) * (1.0 / ORB))
            rest = jnp.square((norm + own_squares[h, :, span]) * (1.0 / ORB))
            out = pl.ds(pl.multiple_of(h * PART + t * PIECE, PIECE), PIECE)
            for i in range(STEPS):
                fresh = nn(inv[3 * i], columns[0:PIV], HIGHEST)
                for j in range(1, i + 1):
                    fresh += nn(inv[3 * i + j], columns[j * PIV : (j + 1) * PIV], HIGHEST)
                factor_ref[i * PIV : (i + 1) * PIV, out] = fresh
                rest -= jnp.sum(fresh * fresh, axis=0, keepdims=True)
                best[i] = jnp.maximum(best[i], rest)
            diag_ref[:, out] = rest
        return tuple(best)

    low_start = jnp.full((1, PIECE), -jnp.inf, jnp.float32)
    best = lax.fori_loop(0, PIECES, finish, (low_start,) * STEPS)
    lanes = lax.broadcasted_iota(jnp.int32, (1, 128), 1)
    peak = jnp.full((1, 128), -jnp.inf, jnp.float32)
    for i in range(STEPS):
        peak = jnp.where(lanes == i, jnp.max(best[i], axis=1, keepdims=True), peak)

    def spread(peak, at, slot, one, other):
        (one_axis, one_count, one_index), (other_axis, other_count, other_index) = one, other
        peak_buf[at] = peak
        copies = []
        for d in range(1, one_count * other_count):
            there = {
                one_axis: lax.rem(one_index + d // other_count, one_count),
                other_axis: lax.rem(other_index + d % other_count, other_count),
            }
            copies.append(go(peak_buf.at[at], peak_buf.at[at + d], slot + d - 1, there))
        for copy in copies:
            copy.wait_recv()
        for d in range(1, one_count * other_count):
            peak = jnp.maximum(peak, peak_buf[at + d])
        return peak

    peak = spread(peak, 0, PEAK_A, ("orb", 4, me), ("grid_2", 2, core))
    peak = spread(peak, 8, PEAK_B, ("grid_0", 4, x), ("grid_1", 4, z))
    peak_ref[...] = peak

    for copy in started:
        copy.wait_send()
    for t in range(PIECES):
        for copy in send_sums(t):
            copy.wait_send()


def on_device(orbitals, pivots):
    f32, bf16 = jnp.float32, jnp.bfloat16
    vmem = pl.BlockSpec(memory_space=pltpu.VMEM)
    factor, diagonal, peaks = pl.pallas_call(
        kernel,
        out_shape=(
            jax.ShapeDtypeStruct((RANK, SHARE), f32),
            jax.ShapeDtypeStruct((1, SHARE), f32),
            jax.ShapeDtypeStruct((1, 128), f32),
        ),
        in_specs=[pl.BlockSpec(memory_space=pl.ANY)] * 2,
        out_specs=(vmem, vmem, vmem),
        scratch_shapes=[
            pltpu.VMEM((STEPS, PIV), jnp.int32),
            pltpu.VMEM((ROWS // PART, DEPTH, PART), bf16),
            pltpu.VMEM((RANK, WIDE), f32),
            pltpu.VMEM((2, 4, 4, 4, HALF, 128), bf16),
            pltpu.VMEM((2, 4, STEPS, HALF, 128), bf16),
            pltpu.VMEM((4, STEPS, HALF, 128), bf16),
            pltpu.VMEM((3, STEPS, HALF, 128), bf16),
            pltpu.VMEM((4, HALF, 128), bf16),
            pltpu.VMEM((3, HALF, 128), bf16),
            pltpu.VMEM((4, RANK, WIDE), bf16),
            pltpu.VMEM((2, DEPTH, PART), bf16),
            pltpu.VMEM((2, DEPTH, PART), bf16),
            pltpu.VMEM((2, PIECES, WORDS, PIECE), jnp.int32),
            pltpu.VMEM((2, PIECES, WORDS, PIECE), jnp.int32),
            pltpu.VMEM((2, PIECES, RANK, PIECE), f32),
            pltpu.VMEM((2, 1, PART), f32),
            pltpu.VMEM((2, 1, PART), f32),
            pltpu.VMEM((2, 1, PART), f32),
            pltpu.VMEM((4, RANK, PIECE), f32),
            pltpu.VMEM((2, RANK, PIECE), f32),
            pltpu.VMEM((2, RANK, PIECE), f32),
            pltpu.VMEM((9, PIV, PIV), f32),
            pltpu.VMEM((9, PIV, PIV), f32),
            pltpu.VMEM((9, PIV, PIV), f32),
            pltpu.VMEM((24, 1, 128), f32),
            pltpu.SemaphoreType.DMA((ROWS // PART + 1,)),
            pltpu.SemaphoreType.DMA((SLOTS,)),
            pltpu.SemaphoreType.DMA((SLOTS,)),
        ],
        compiler_params=pltpu.CompilerParams(
            collective_id=0, has_side_effects=True, vmem_limit_bytes=50 * 1024 * 1024
        ),
    )(orbitals, pivots)
    return factor.T, diagonal.reshape(SHARE), peaks[0, :STEPS]


def solution(mesh):
    split = Mesh(
        mesh.devices.reshape(4, 4, 2, mesh.shape["orb"]), ("grid_0", "grid_1", "grid_2", "orb")
    )
    return jax.shard_map(
        on_device,
        mesh=split,
        in_specs=(P("orb", GRID), P()),
        out_specs=(P(GRID_ORB, None), P(GRID_ORB), P()),
        check_vma=False,
    )
```

```python
import functools

import jax
import jax.numpy as jnp
from jax import lax
from jax.experimental import pallas as pl
from jax.experimental.pallas import tpu as pltpu
from jax.sharding import Mesh
from jax.sharding import PartitionSpec as P

ORB = 1800
GRID = ("grid_0", "grid_1", "grid_2")
GRID_ORB = ("grid_0", "grid_1", "grid_2", "orb")
MESH = pl.DeviceIdType.MESH
HIGHEST = lax.Precision.HIGHEST

STEPS = 3
PIV = 96
RANK = STEPS * PIV
HALF = PIV // 2
DEPTH = 450
WIDE = 512
ROWS = 8192
SHARE = 2048
PART = 1024
PIECE = 256
PIECES = PART // PIECE
WORDS = 2 * PIV
FIELD = 21
SCALE = float(2 ** (FIELD - 1) - 64)
TINY = 1e-30

FIRST = 896

CORE_A, X_A, Z_A, Y_A, B, X_C, Z_C, CORE_B, FAR, NEAR, NORM, SUM = range(12)
LAST = SUM + PIECES - 1
PEAK_A, PEAK_B = LAST + 2, LAST + 3
SLOTS = LAST + 4


def nt(left, right, precision=None):
    return lax.dot_general(
        left, right, (((1,), (1,)), ((), ())), precision=precision,
        preferred_element_type=jnp.float32,
    )


def nn(left, right, precision=None):
    return lax.dot_general(
        left, right, (((1,), (0,)), ((), ())), precision=precision,
        preferred_element_type=jnp.float32,
    )


def inverse_factor(block):
    lanes = lax.broadcasted_iota(jnp.int32, (8, PIV), 1)
    subs = lax.broadcasted_iota(jnp.int32, (8, PIV), 0)
    groups = PIV // 8
    left = [block[8 * g : 8 * g + 8, :] for g in range(groups)]
    right = [jnp.where(lanes == subs + 8 * g, 1.0, 0.0) for g in range(groups)]

    def row(values, r):
        return jnp.broadcast_to(values[r : r + 1, :], (8, PIV))

    out = []
    for home in range(groups):
        column = {
            (g, j): jnp.broadcast_to(left[g][:, 8 * home + j : 8 * home + j + 1], (8, PIV))
            for g in range(home, groups)
            for j in range(8)
        }
        kept = right[home]
        for r in range(8):
            scale = lax.rsqrt(row(column[home, r], r))
            spread = [row(column[home, r], j) * scale for j in range(r + 1, 8)]
            row_left = row(left[home], r) * scale
            row_right = row(right[home], r) * scale
            kept = jnp.where(subs == r, row_right, kept)
            for g in range(home, groups):
                times = column[g, r] * scale
                if g == home:
                    times = jnp.where(subs > r, times, 0.0)
                left[g] = left[g] - times * row_left
                right[g] = right[g] - times * row_right
                for j in range(r + 1, 8):
                    column[g, j] = column[g, j] - times * spread[j - r - 1]
        out.append(kept)
    return jnp.concatenate(out, axis=0)


def kernel(
    orb_hbm, piv_hbm, factor_ref, diag_ref, peak_ref,
    pivots, orb, gathered, pv, a0, r0, r1, a2, r2, picked, far, near, sums_out, sums_in, own,
    norm_out, norm_in, own_squares, norm_own, pack, unpack, gram, low, inv, peak_buf, local_sem, send_sem, recv_sem,
):
    x = lax.axis_index("grid_0")
    z = lax.axis_index("grid_1")
    core = lax.axis_index("grid_2")
    me = lax.axis_index("orb")
    right, left, across = lax.rem(me + 1, 4), lax.rem(me + 3, 4), lax.rem(me + 2, 4)
    other = 1 - core

    barrier = pltpu.get_barrier_semaphore()
    pl.semaphore_signal(barrier, inc=1, device_id={"grid_2": other}, device_id_type=MESH)
    for d in (1, 2, 3):
        pl.semaphore_signal(barrier, inc=1, device_id={"grid_0": lax.rem(x + d, 4)}, device_id_type=MESH)
        pl.semaphore_signal(barrier, inc=1, device_id={"grid_1": lax.rem(z + d, 4)}, device_id_type=MESH)
        pl.semaphore_signal(barrier, inc=1, device_id={"orb": lax.rem(me + d, 4)}, device_id_type=MESH)

    def owner_at(i):
        return lax.rem(me + 2 + i, 4)

    def load(part):
        return pltpu.make_async_copy(
            orb_hbm.at[:, pl.ds(pl.multiple_of(part * PART, PART), PART)], orb.at[part], local_sem.at[lax.div(part, 2)]
        )

    def loaded(owner):
        pair = orb.at[pl.ds(2 * owner, 2)]
        pltpu.make_async_copy(pair, pair, local_sem.at[owner]).wait()

    load_pivots = pltpu.make_async_copy(piv_hbm, pivots, local_sem.at[4])
    load_pivots.start()
    for i in range(4):
        load(2 * owner_at(i)).start()
        load(2 * owner_at(i) + 1).start()

    def remote(src, dst, slot, where):
        return pltpu.make_async_remote_copy(
            src_ref=src, dst_ref=dst, send_sem=send_sem.at[slot], recv_sem=recv_sem.at[slot],
            device_id=where, device_id_type=MESH,
        )

    def go(src, dst, slot, where):
        remote(src, dst, slot, where).start()

    unsent = []

    def arrived(slot, size):
        pltpu.make_async_copy(size, size, recv_sem.at[slot]).wait()
        unsent.append((slot, size))

    def sent():
        for slot, size in unsent:
            pltpu.make_async_copy(size, size, send_sem.at[slot]).wait()
        unsent.clear()

    base = ((x * 4 + z) * 2 + core) * ROWS
    gathered[...] = jnp.zeros_like(gathered)
    load_pivots.wait()
    square = (PIV, PIV)
    eye = lax.broadcasted_iota(jnp.int32, square, 0) == lax.broadcasted_iota(jnp.int32, square, 1)
    here = jnp.concatenate(
        [
            jnp.sum(
                jnp.where(eye, jnp.broadcast_to(pivots[s : s + 1].astype(jnp.float32), square), 0.0),
                axis=1, keepdims=True,
            )
            for s in range(STEPS)
        ],
        axis=0,
    ).astype(jnp.int32) - base

    pl.semaphore_wait(barrier, 10)

    def far_copies(low, high):
        start = pl.multiple_of(across * SHARE, SHARE)
        span = slice(low, high)
        go(orb_hbm.at[:, pl.ds(start + low, high - low)], far.at[0, :, span], FAR, {"orb": left})
        go(orb_hbm.at[:, pl.ds(start + PART + low, high - low)], far.at[1, :, span], FAR, {"orb": right})

    far_copies(0, FIRST)

    def extract(i, carry):
        owner = owner_at(i)
        loaded(owner)
        for part in (2 * owner, 2 * owner + 1):
            spots = lax.broadcasted_iota(jnp.int32, (RANK, PART), 1) + part * PART
            chosen = jnp.where(spots == here, 1.0, 0.0).astype(jnp.bfloat16)
            gathered[:, 0:DEPTH] += nt(chosen, orb[part])
        return carry

    lax.fori_loop(0, 4, extract, 0)
    for h in range(2):
        for lane in range(4):
            for s in range(STEPS):
                a0[h, lane, s] = gathered[
                    s * PIV + h * HALF : s * PIV + (h + 1) * HALF, lane * 128 : (lane + 1) * 128
                ].astype(jnp.bfloat16)

    go(a0.at[other], r0, CORE_A, {"grid_2": other})
    arrived(CORE_A, r0)
    r0[...] = (r0[...].astype(jnp.float32) + a0[core].astype(jnp.float32)).astype(jnp.bfloat16)
    for d in (1, 2, 3):
        there = lax.rem(x + d, 4)
        go(r0.at[there], r1.at[d - 1], X_A, {"grid_0": there})
    arrived(X_A, r1)
    total = r0[x].astype(jnp.float32)
    for d in range(3):
        total += r1[d].astype(jnp.float32)
    a2[0:STEPS] = total.astype(jnp.bfloat16)
    a2[STEPS] = jnp.zeros((HALF, 128), jnp.bfloat16)
    for d in (1, 2, 3):
        there = lax.rem(z + d, 4)
        go(a2.at[there], r2.at[d - 1], Z_A, {"grid_1": there})
    arrived(Z_A, r2)
    total = a2[z].astype(jnp.float32)
    for d in range(3):
        total += r2[d].astype(jnp.float32)
    pv[core, x, z, me] = total.astype(jnp.bfloat16)
    mine = pv.at[core, x, z, me]
    for d in (1, 2, 3):
        go(mine, mine, Y_A, {"orb": lax.rem(me + d, 4)})
    far_copies(FIRST, PART)
    go(orb.at[2 * left + 1], near.at[1], NEAR, {"orb": left})
    go(orb.at[2 * right], near.at[0], NEAR, {"orb": right})
    arrived(Y_A, r2)
    for d in (1, 2, 3):
        mine = pv.at[core, x, z, 0:2]
        go(mine, mine, B, {"grid_0": lax.rem(x + d, 4)})
        mine = pv.at[core, x, z, 2:4]
        go(mine, mine, B, {"grid_1": lax.rem(z + d, 4)})
    arrived(B, a0.at[0])
    for d in (1, 2, 3):
        mine = pv.at[core, :, z, 0:2]
        go(mine, mine, Z_C, {"grid_1": lax.rem(z + d, 4)})
        mine = pv.at[core, x, 0:STEPS, 2:4]
        go(mine, mine, X_C, {"grid_0": lax.rem(x + d, 4)})

    def squares(values):
        wide = values.astype(jnp.float32)
        return jnp.sum(wide * wide, axis=0, keepdims=True)

    arrived(FAR, far)

    def norms(t, carry):
        span = pl.ds(pl.multiple_of(t * PIECE, PIECE), PIECE)
        for h, owned in enumerate((2 * left, 2 * right + 1)):
            norm_out[h, :, span] = squares(orb[owned, :, span]) + squares(far[h, :, span])
        return carry

    lax.fori_loop(0, PIECES, norms, 0)
    go(norm_out.at[0], norm_in.at[0], NORM, {"orb": left})
    go(norm_out.at[1], norm_in.at[1], NORM, {"orb": right})
    arrived(Z_C, a0)
    arrived(X_C, pv.at[0, 0:3, 0:3, 0:2])
    mine = pv.at[core, :, 0:STEPS]
    go(mine, mine, CORE_B, {"grid_2": other})
    arrived(CORE_B, pv.at[0, :, 0:STEPS])
    for h in range(2):
        for lane in range(4):
            for s in range(STEPS):
                for y in range(4):
                    picked[y, s * PIV + h * HALF : s * PIV + (h + 1) * HALF, lane * 128 : (lane + 1) * 128] = (
                        pv[h, lane, s, y]
                    )

    for y in range(4):
        wide = picked[y].astype(jnp.float32)
        norm_own[y] = jnp.broadcast_to(jnp.sum(wide * wide, axis=1, keepdims=True), (RANK, PIECE))
    for h, (beside, beyond) in enumerate(((right, across), (left, across))):
        pack[h] = lax.rsqrt(jnp.maximum(norm_own[me] + norm_own[beside], TINY)) * SCALE
        far_norm = jnp.maximum(norm_own[beside] + norm_own[beyond], TINY)
        unpack[h] = far_norm * lax.rsqrt(far_norm) * (1.0 / SCALE)

    def send_sums(t, span, slot):
        for h, where in enumerate((left, right)):
            go(sums_out.at[h, t, :, span], sums_in.at[h, t, :, span], slot, {"orb": where})

    halves = (slice(0, 128), slice(128, 256))

    def middle(t, carry):
        span = pl.ds(pl.multiple_of(t * PIECE, PIECE), PIECE)
        for h, (own, source) in enumerate(((2 * left, right), (2 * right + 1, left))):
            a = orb[own, :, span]
            b = far[h, :, span]
            product = nn(picked[me, :, 0:DEPTH], a) + nn(picked[source, :, 0:DEPTH], b)
            over = lax.rsqrt(jnp.maximum(norm_out[h, :, span], TINY))
            whole = jnp.round(product * pack[h] * over).astype(jnp.int32)
            last = whole[2 * PIV : RANK]
            mask = (1 << FIELD) - 1
            sums_out[h, t, 0:PIV] = (whole[0:PIV] & mask) | (last << FIELD)
            sums_out[h, t, PIV:WORDS] = (whole[PIV : 2 * PIV] & mask) | ((last >> (32 - FIELD)) << FIELD)

        @pl.when(t < PIECES - 1)
        def _():
            send_sums(t, slice(0, PIECE), SUM + t)

        return carry

    lax.fori_loop(0, PIECES, middle, 0)
    for half in range(2):
        send_sums(PIECES - 1, halves[half], LAST + half)

    pairs = nt(picked[0], picked[0])
    for y in range(1, 4):
        pairs += nt(picked[y], picked[y])
    block = jnp.square(pairs * (1.0 / ORB))
    for i in range(STEPS):
        for j in range(i + 1):
            gram[3 * i + j] = block[i * PIV : (i + 1) * PIV, j * PIV : (j + 1) * PIV]

    def diagonal_inverse(i, carry):
        def update(k, carry):
            gram[4 * i] -= nt(low[3 * i + k], low[3 * i + k], HIGHEST)
            return carry

        lax.fori_loop(0, i, update, 0)
        inv[4 * i] = inverse_factor(gram[4 * i])

        def panel(j, carry):
            def update(k, carry):
                gram[3 * j + i] -= nt(low[3 * j + k], low[3 * i + k], HIGHEST)
                return carry

            lax.fori_loop(0, i, update, 0)
            low[3 * j + i] = nt(gram[3 * j + i], inv[4 * i], HIGHEST)
            return carry

        lax.fori_loop(i + 1, STEPS, panel, 0)
        return carry

    lax.fori_loop(0, STEPS, diagonal_inverse, 0)
    inv[3] = -nn(inv[4], nn(low[3], inv[0], HIGHEST), HIGHEST)
    inv[7] = -nn(inv[8], nn(low[7], inv[4], HIGHEST), HIGHEST)
    inv[6] = -nn(inv[8], nn(low[6], inv[0], HIGHEST) + nn(low[7], inv[3], HIGHEST), HIGHEST)

    arrived(NEAR, near)
    arrived(NORM, norm_in)

    def own_products(t, carry):
        span = pl.ds(pl.multiple_of(t * PIECE, PIECE), PIECE)
        for h, source in enumerate((left, right)):
            a = orb[2 * me + h, :, span]
            b = near[h, :, span]
            own[h, t] = nn(picked[me, :, 0:DEPTH], a) + nn(picked[source, :, 0:DEPTH], b)
            own_squares[h, :, span] = squares(a) + squares(b)
        return carry

    lax.fori_loop(0, PIECES, own_products, 0)

    def finish(t, low, width, best):
        best = list(best)
        for h in range(2):
            start = t * PIECE + low
            span = pl.ds(pl.multiple_of(start, 128), width)
            out = pl.ds(pl.multiple_of(h * PART + start, 128), width)
            inside = slice(low, low + width)
            first, second = sums_in[h, t, 0:PIV, inside], sums_in[h, t, PIV:WORDS, inside]
            spare = 32 - FIELD
            whole = jnp.concatenate(
                [
                    (first << spare) >> spare,
                    (second << spare) >> spare,
                    ((second >> FIELD) << spare) | lax.shift_right_logical(first, FIELD),
                ],
                axis=0,
            ).astype(jnp.float32)
            norm = norm_in[h, :, span]
            bounded = jnp.maximum(norm, TINY)
            received = whole * unpack[h, :, 0:width] * (bounded * lax.rsqrt(bounded))
            columns = jnp.square((received + own[h, t, :, inside]) * (1.0 / ORB))
            rest = jnp.square((norm + own_squares[h, :, span]) * (1.0 / ORB))
            for i in range(STEPS):
                fresh = nn(inv[3 * i], columns[0:PIV], HIGHEST)
                for j in range(1, i + 1):
                    fresh += nn(inv[3 * i + j], columns[j * PIV : (j + 1) * PIV], HIGHEST)
                factor_ref[i * PIV : (i + 1) * PIV, out] = fresh
                rest -= jnp.sum(fresh * fresh, axis=0, keepdims=True)
                for at in range(0, width, 128):
                    best[i] = jnp.maximum(best[i], rest[:, at : at + 128])
            diag_ref[:, out] = rest
        return tuple(best)

    def whole_piece(t, best):
        size = sums_in.at[:, t]
        pltpu.make_async_copy(size, size, recv_sem.at[SUM + t]).wait()
        return finish(t, 0, PIECE, best)

    best = (jnp.full((1, 128), -jnp.inf, jnp.float32),) * STEPS
    best = lax.fori_loop(0, PIECES - 1, whole_piece, best)
    for half in range(2):
        arrived(LAST + half, sums_in.at[:, PIECES - 1, :, halves[half]])
        best = finish(PIECES - 1, half * 128, 128, best)
    lanes = lax.broadcasted_iota(jnp.int32, (1, 128), 1)
    peak = jnp.full((1, 128), -jnp.inf, jnp.float32)
    for i in range(STEPS):
        peak = jnp.where(lanes == i, jnp.max(best[i], axis=1, keepdims=True), peak)

    unsent.extend((SUM + t, sums_in.at[:, t]) for t in range(PIECES - 1))

    def spread(peak, at, slot, one, other):
        (one_axis, one_count, one_index), (other_axis, other_count, other_index) = one, other
        count = one_count * other_count
        peak_buf[at] = peak
        for d in reversed(range(1, count)):
            there = {
                one_axis: lax.rem(one_index + d // other_count, one_count),
                other_axis: lax.rem(other_index + d % other_count, other_count),
            }
            go(peak_buf.at[at], peak_buf.at[at + d], slot, there)
        sent()
        arrived(slot, peak_buf.at[at + 1 : at + count])
        for d in range(1, count):
            peak = jnp.maximum(peak, peak_buf[at + d])
        return peak

    peak = spread(peak, 0, PEAK_A, ("orb", 4, me), ("grid_2", 2, core))
    peak = spread(peak, 8, PEAK_B, ("grid_0", 4, x), ("grid_1", 4, z))
    sent()
    peak_ref[...] = peak


def hand_over(factor, diagonal, peaks, factor_out, diagonal_out, peaks_out, diagonal_flat, peaks_flat, sem):
    copies = [
        pltpu.make_async_copy(src, dst, sem.at[i])
        for i, (src, dst) in enumerate(
            ((factor, factor_out), (diagonal_flat, diagonal_out), (peaks_flat, peaks_out))
        )
    ]
    copies[0].start()
    diagonal_flat[...] = diagonal[...].reshape(SHARE)
    copies[1].start()
    peaks_flat[...] = peaks[0, 0:STEPS]
    copies[2].start()
    for copy in copies:
        copy.wait()


def on_device(orbitals, pivots):
    f32, bf16 = jnp.float32, jnp.bfloat16
    vmem = pl.BlockSpec(memory_space=pltpu.VMEM)
    factor, diagonal, peaks = pl.pallas_call(
        kernel,
        out_shape=(
            jax.ShapeDtypeStruct((RANK, SHARE), f32),
            jax.ShapeDtypeStruct((1, SHARE), f32),
            jax.ShapeDtypeStruct((1, 128), f32),
        ),
        in_specs=[pl.BlockSpec(memory_space=pltpu.HBM)] * 2,
        out_specs=(vmem, vmem, vmem),
        scratch_shapes=[
            pltpu.VMEM((STEPS, PIV), jnp.int32),
            pltpu.VMEM((ROWS // PART, DEPTH, PART), bf16),
            pltpu.VMEM((RANK, WIDE), f32),
            pltpu.VMEM((2, 4, 4, 4, HALF, 128), bf16),
            pltpu.VMEM((2, 4, STEPS, HALF, 128), bf16),
            pltpu.VMEM((4, STEPS, HALF, 128), bf16),
            pltpu.VMEM((3, STEPS, HALF, 128), bf16),
            pltpu.VMEM((4, HALF, 128), bf16),
            pltpu.VMEM((3, HALF, 128), bf16),
            pltpu.VMEM((4, RANK, WIDE), bf16),
            pltpu.VMEM((2, DEPTH, PART), bf16),
            pltpu.VMEM((2, DEPTH, PART), bf16),
            pltpu.VMEM((2, PIECES, WORDS, PIECE), jnp.int32),
            pltpu.VMEM((2, PIECES, WORDS, PIECE), jnp.int32),
            pltpu.VMEM((2, PIECES, RANK, PIECE), f32),
            pltpu.VMEM((2, 1, PART), f32),
            pltpu.VMEM((2, 1, PART), f32),
            pltpu.VMEM((2, 1, PART), f32),
            pltpu.VMEM((4, RANK, PIECE), f32),
            pltpu.VMEM((2, RANK, PIECE), f32),
            pltpu.VMEM((2, RANK, PIECE), f32),
            pltpu.VMEM((9, PIV, PIV), f32),
            pltpu.VMEM((9, PIV, PIV), f32),
            pltpu.VMEM((9, PIV, PIV), f32),
            pltpu.VMEM((24, 1, 128), f32),
            pltpu.SemaphoreType.DMA((5,)),
            pltpu.SemaphoreType.DMA((SLOTS,)),
            pltpu.SemaphoreType.DMA((SLOTS,)),
        ],
        compiler_params=pltpu.CompilerParams(
            collective_id=0, has_side_effects=True, vmem_limit_bytes=50 * 1024 * 1024
        ),
    )(orbitals, pltpu.with_memory_space_constraint(pivots, pltpu.HBM))
    factor, diagonal, peaks = pl.pallas_call(
        hand_over,
        out_shape=(
            jax.ShapeDtypeStruct((RANK, SHARE), f32),
            jax.ShapeDtypeStruct((SHARE,), f32),
            jax.ShapeDtypeStruct((STEPS,), f32),
        ),
        in_specs=[vmem] * 3,
        out_specs=(pl.BlockSpec(memory_space=pltpu.HBM),) * 3,
        scratch_shapes=[pltpu.VMEM((SHARE,), f32), pltpu.VMEM((STEPS,), f32), pltpu.SemaphoreType.DMA((3,))],
        compiler_params=pltpu.CompilerParams(vmem_limit_bytes=4 * 1024 * 1024),
    )(factor, diagonal, peaks)
    return factor.T, diagonal, peaks


def solution(mesh):
    split = Mesh(
        mesh.devices.reshape(4, 4, 2, mesh.shape["orb"]), ("grid_0", "grid_1", "grid_2", "orb")
    )
    return jax.shard_map(
        on_device,
        mesh=split,
        in_specs=(P("orb", GRID), P()),
        out_specs=(P(GRID_ORB, None), P(GRID_ORB), P()),
        check_vma=False,
    )
```

```python
import functools

import jax
import jax.numpy as jnp
from jax import lax
from jax.experimental import pallas as pl
from jax.experimental.pallas import tpu as pltpu
from jax.sharding import Mesh
from jax.sharding import PartitionSpec as P

ORB = 1800
GRID = ("grid_0", "grid_1", "grid_2")
GRID_ORB = ("grid_0", "grid_1", "grid_2", "orb")
MESH = pl.DeviceIdType.MESH
HIGHEST = lax.Precision.HIGHEST

STEPS = 3
PIV = 96
RANK = STEPS * PIV
HALF = PIV // 2
DEPTH = 450
WIDE = 512
ROWS = 8192
SHARE = 2048
PART = 1024
PIECE = 256
PIECES = PART // PIECE
WORDS = 2 * PIV
STRIPS = 4
FIELD = 21
SCALE = float(2 ** (FIELD - 1) - 64)
TINY = 1e-30

FIRST = 896

CORE_A, X_A, Z_A, Y_A, B, X_C, Z_C, CORE_B, FAR, NEAR, NORM, SUM = range(12)
LAST = SUM + PIECES - 1
PEAK_A = LAST + 2
SLOTS = LAST + 3


def nt(left, right, precision=None):
    return lax.dot_general(
        left, right, (((1,), (1,)), ((), ())), precision=precision,
        preferred_element_type=jnp.float32,
    )


def nn(left, right, precision=None):
    return lax.dot_general(
        left, right, (((1,), (0,)), ((), ())), precision=precision,
        preferred_element_type=jnp.float32,
    )


def inverse_factor(block):
    lanes = lax.broadcasted_iota(jnp.int32, (8, PIV), 1)
    subs = lax.broadcasted_iota(jnp.int32, (8, PIV), 0)
    groups = PIV // 8
    left = [block[8 * g : 8 * g + 8, :] for g in range(groups)]
    right = [jnp.where(lanes == subs + 8 * g, 1.0, 0.0) for g in range(groups)]

    def row(values, r):
        return jnp.broadcast_to(values[r : r + 1, :], (8, PIV))

    out = []
    for home in range(groups):
        column = {
            (g, j): jnp.broadcast_to(left[g][:, 8 * home + j : 8 * home + j + 1], (8, PIV))
            for g in range(home, groups)
            for j in range(8)
        }
        kept = right[home]
        for r in range(8):
            scale = lax.rsqrt(row(column[home, r], r))
            spread = [row(column[home, r], j) * scale for j in range(r + 1, 8)]
            row_left = row(left[home], r) * scale
            row_right = row(right[home], r) * scale
            kept = jnp.where(subs == r, row_right, kept)
            for g in range(home, groups):
                times = column[g, r] * scale
                if g == home:
                    times = jnp.where(subs > r, times, 0.0)
                left[g] = left[g] - times * row_left
                right[g] = right[g] - times * row_right
                for j in range(r + 1, 8):
                    column[g, j] = column[g, j] - times * spread[j - r - 1]
        out.append(kept)
    return jnp.concatenate(out, axis=0)


def kernel(
    orb_hbm, piv_hbm, factor_ref, diag_ref, peak_ref,
    pivots, orb, gathered, pv, a0, r0, r1, a2, r2, picked, far, near, sums_out, sums_in, own,
    norm_out, norm_in, own_squares, norm_own, pack, unpack, gram, low, inv, peak_buf, local_sem, send_sem, recv_sem,
):
    x = lax.axis_index("grid_0")
    z = lax.axis_index("grid_1")
    core = lax.axis_index("grid_2")
    me = lax.axis_index("orb")
    right, left, across = lax.rem(me + 1, 4), lax.rem(me + 3, 4), lax.rem(me + 2, 4)
    other = 1 - core

    barrier = pltpu.get_barrier_semaphore()
    for axis, count, index in (("orb", 4, me), ("grid_0", 4, x), ("grid_1", 4, z), ("grid_2", 2, core)):
        for d in range(1, count):
            there = {axis: lax.rem(index + d, count)}
            pl.semaphore_signal(barrier, inc=1, device_id=there, device_id_type=MESH)

    def owner_at(i):
        return lax.rem(me + 2 + i, 4)

    def load(part):
        return pltpu.make_async_copy(
            orb_hbm.at[:, pl.ds(pl.multiple_of(part * PART, PART), PART)], orb.at[part], local_sem.at[lax.div(part, 2)]
        )

    def loaded(owner):
        pair = orb.at[pl.ds(2 * owner, 2)]
        pltpu.make_async_copy(pair, pair, local_sem.at[owner]).wait()

    load_pivots = pltpu.make_async_copy(piv_hbm, pivots, local_sem.at[4])
    load_pivots.start()
    for i in range(4):
        load(2 * owner_at(i)).start()
        load(2 * owner_at(i) + 1).start()

    def remote(src, dst, slot, where):
        return pltpu.make_async_remote_copy(
            src_ref=src, dst_ref=dst, send_sem=send_sem.at[slot], recv_sem=recv_sem.at[slot],
            device_id=where, device_id_type=MESH,
        )

    def go(src, dst, slot, where):
        remote(src, dst, slot, where).start()

    unsent = []

    def arrived(slot, size):
        pltpu.make_async_copy(size, size, recv_sem.at[slot]).wait()
        unsent.append((slot, size))

    def sent():
        for slot, size in unsent:
            pltpu.make_async_copy(size, size, send_sem.at[slot]).wait()
        unsent.clear()

    pl.semaphore_wait(barrier, 10)

    def far_copies(low, high):
        start = pl.multiple_of(across * SHARE, SHARE)
        span = slice(low, high)
        go(orb_hbm.at[:, pl.ds(start + low, high - low)], far.at[0, :, span], FAR, {"orb": left})
        go(orb_hbm.at[:, pl.ds(start + PART + low, high - low)], far.at[1, :, span], FAR, {"orb": right})

    far_copies(0, FIRST)

    base = ((x * 4 + z) * 2 + core) * ROWS
    gathered[...] = jnp.zeros_like(gathered)
    load_pivots.wait()
    square = (PIV, PIV)
    eye = lax.broadcasted_iota(jnp.int32, square, 0) == lax.broadcasted_iota(jnp.int32, square, 1)
    here = jnp.concatenate(
        [
            jnp.sum(
                jnp.where(eye, jnp.broadcast_to(pivots[s : s + 1].astype(jnp.float32), square), 0.0),
                axis=1, keepdims=True,
            )
            for s in range(STEPS)
        ],
        axis=0,
    ).astype(jnp.int32) - base

    def extract(i, carry):
        owner = owner_at(i)
        loaded(owner)
        for part in (2 * owner, 2 * owner + 1):
            spots = lax.broadcasted_iota(jnp.int32, (RANK, PART), 1) + part * PART
            chosen = jnp.where(spots == here, 1.0, 0.0).astype(jnp.bfloat16)
            gathered[:, 0:DEPTH] += nt(chosen, orb[part])
        return carry

    lax.fori_loop(0, 4, extract, 0)
    for h in range(2):
        for lane in range(4):
            for s in range(STEPS):
                a0[h, lane, s] = gathered[
                    s * PIV + h * HALF : s * PIV + (h + 1) * HALF, lane * 128 : (lane + 1) * 128
                ].astype(jnp.bfloat16)

    go(a0.at[other], r0, CORE_A, {"grid_2": other})
    arrived(CORE_A, r0)
    r0[...] = (r0[...].astype(jnp.float32) + a0[core].astype(jnp.float32)).astype(jnp.bfloat16)
    for d in (1, 2, 3):
        there = lax.rem(x + d, 4)
        go(r0.at[there], r1.at[d - 1], X_A, {"grid_0": there})
    arrived(X_A, r1)
    total = r0[x].astype(jnp.float32)
    for d in range(3):
        total += r1[d].astype(jnp.float32)
    a2[0:STEPS] = total.astype(jnp.bfloat16)
    a2[STEPS] = jnp.zeros((HALF, 128), jnp.bfloat16)
    for d in (1, 2, 3):
        there = lax.rem(z + d, 4)
        go(a2.at[there], r2.at[d - 1], Z_A, {"grid_1": there})
    arrived(Z_A, r2)
    total = a2[z].astype(jnp.float32)
    for d in range(3):
        total += r2[d].astype(jnp.float32)
    pv[core, x, z, me] = total.astype(jnp.bfloat16)
    mine = pv.at[core, x, z, me]
    for d in (1, 2, 3):
        go(mine, mine, Y_A, {"orb": lax.rem(me + d, 4)})
    far_copies(FIRST, PART)
    go(orb.at[2 * left + 1], near.at[1], NEAR, {"orb": left})
    go(orb.at[2 * right], near.at[0], NEAR, {"orb": right})
    arrived(Y_A, r2)
    for d in (1, 2, 3):
        mine = pv.at[core, x, z, 0:2]
        go(mine, mine, B, {"grid_0": lax.rem(x + d, 4)})
        mine = pv.at[core, x, z, 2:4]
        go(mine, mine, B, {"grid_1": lax.rem(z + d, 4)})
    arrived(B, a0.at[0])
    for d in (1, 2, 3):
        mine = pv.at[core, :, z, 0:2]
        go(mine, mine, Z_C, {"grid_1": lax.rem(z + d, 4)})
        mine = pv.at[core, x, 0:STEPS, 2:4]
        go(mine, mine, X_C, {"grid_0": lax.rem(x + d, 4)})

    def squares(values):
        wide = values.astype(jnp.float32)
        return jnp.sum(wide * wide, axis=0, keepdims=True)

    arrived(FAR, far)

    def norms(t, carry):
        span = pl.ds(pl.multiple_of(t * PIECE, PIECE), PIECE)
        for h, owned in enumerate((2 * left, 2 * right + 1)):
            norm_out[h, :, span] = squares(orb[owned, :, span]) + squares(far[h, :, span])
        return carry

    lax.fori_loop(0, PIECES, norms, 0)
    go(norm_out.at[0], norm_in.at[0], NORM, {"orb": left})
    go(norm_out.at[1], norm_in.at[1], NORM, {"orb": right})
    arrived(Z_C, a0)
    arrived(X_C, pv.at[0, 0:3, 0:3, 0:2])
    mine = pv.at[core, :, 0:STEPS]
    go(mine, mine, CORE_B, {"grid_2": other})
    arrived(CORE_B, pv.at[0, :, 0:STEPS])
    for h in range(2):
        for lane in range(4):
            for s in range(STEPS):
                for y in range(4):
                    picked[y, s * PIV + h * HALF : s * PIV + (h + 1) * HALF, lane * 128 : (lane + 1) * 128] = (
                        pv[h, lane, s, y]
                    )

    for y in range(4):
        wide = picked[y].astype(jnp.float32)
        norm_own[y] = jnp.broadcast_to(jnp.sum(wide * wide, axis=1, keepdims=True), (RANK, PIECE))
    for h, (beside, beyond) in enumerate(((right, across), (left, across))):
        pack[h] = lax.rsqrt(jnp.maximum(norm_own[me] + norm_own[beside], TINY)) * SCALE
        far_norm = jnp.maximum(norm_own[beside] + norm_own[beyond], TINY)
        unpack[h] = far_norm * lax.rsqrt(far_norm) * (1.0 / SCALE)

    def send_sums(t, span, slot):
        for h, where in enumerate((left, right)):
            go(sums_out.at[h, t, :, span], sums_in.at[h, t, :, span], slot, {"orb": where})

    halves = (slice(0, 128), slice(128, 256))

    def middle(t, carry):
        span = pl.ds(pl.multiple_of(t * PIECE, PIECE), PIECE)
        for h, (own, source) in enumerate(((2 * left, right), (2 * right + 1, left))):
            a = orb[own, :, span]
            b = far[h, :, span]
            product = nn(picked[me, :, 0:DEPTH], a) + nn(picked[source, :, 0:DEPTH], b)
            over = lax.rsqrt(jnp.maximum(norm_out[h, :, span], TINY))
            whole = jnp.round(product * pack[h] * over).astype(jnp.int32)
            last = whole[2 * PIV : RANK]
            mask = (1 << FIELD) - 1
            sums_out[h, t, 0:PIV] = (whole[0:PIV] & mask) | (last << FIELD)
            sums_out[h, t, PIV:WORDS] = (whole[PIV : 2 * PIV] & mask) | ((last >> (32 - FIELD)) << FIELD)

        @pl.when(t < PIECES - 1)
        def _():
            send_sums(t, slice(0, PIECE), SUM + t)

        return carry

    lax.fori_loop(0, PIECES, middle, 0)
    for half in range(2):
        send_sums(PIECES - 1, halves[half], LAST + half)

    pairs = nt(picked[0], picked[0])
    for y in range(1, 4):
        pairs += nt(picked[y], picked[y])
    block = jnp.square(pairs * (1.0 / ORB))
    for i in range(STEPS):
        for j in range(i + 1):
            gram[3 * i + j] = block[i * PIV : (i + 1) * PIV, j * PIV : (j + 1) * PIV]

    def diagonal_inverse(i, carry):
        def update(k, carry):
            gram[4 * i] -= nt(low[3 * i + k], low[3 * i + k], HIGHEST)
            return carry

        lax.fori_loop(0, i, update, 0)
        inv[4 * i] = inverse_factor(gram[4 * i])

        def panel(j, carry):
            def update(k, carry):
                gram[3 * j + i] -= nt(low[3 * j + k], low[3 * i + k], HIGHEST)
                return carry

            lax.fori_loop(0, i, update, 0)
            low[3 * j + i] = nt(gram[3 * j + i], inv[4 * i], HIGHEST)
            return carry

        lax.fori_loop(i + 1, STEPS, panel, 0)
        return carry

    lax.fori_loop(0, STEPS, diagonal_inverse, 0)
    inv[3] = -nn(inv[4], nn(low[3], inv[0], HIGHEST), HIGHEST)
    inv[7] = -nn(inv[8], nn(low[7], inv[4], HIGHEST), HIGHEST)
    inv[6] = -nn(inv[8], nn(low[6], inv[0], HIGHEST) + nn(low[7], inv[3], HIGHEST), HIGHEST)

    arrived(NEAR, near)
    arrived(NORM, norm_in)

    def own_products(t, carry):
        span = pl.ds(pl.multiple_of(t * PIECE, PIECE), PIECE)
        for h, source in enumerate((left, right)):
            a = orb[2 * me + h, :, span]
            b = near[h, :, span]
            own[h, t] = nn(picked[me, :, 0:DEPTH], a) + nn(picked[source, :, 0:DEPTH], b)
            own_squares[h, :, span] = squares(a) + squares(b)
        return carry

    lax.fori_loop(0, PIECES, own_products, 0)

    def finish(t, low, width, best):
        best = list(best)
        for h in range(2):
            start = t * PIECE + low
            span = pl.ds(pl.multiple_of(start, 128), width)
            out = pl.ds(pl.multiple_of(h * PART + start, 128), width)
            inside = slice(low, low + width)
            first, second = sums_in[h, t, 0:PIV, inside], sums_in[h, t, PIV:WORDS, inside]
            spare = 32 - FIELD
            whole = jnp.concatenate(
                [
                    (first << spare) >> spare,
                    (second << spare) >> spare,
                    ((second >> FIELD) << spare) | lax.shift_right_logical(first, FIELD),
                ],
                axis=0,
            ).astype(jnp.float32)
            norm = norm_in[h, :, span]
            bounded = jnp.maximum(norm, TINY)
            received = whole * unpack[h, :, 0:width] * (bounded * lax.rsqrt(bounded))
            columns = jnp.square((received + own[h, t, :, inside]) * (1.0 / ORB))
            rest = jnp.square((norm + own_squares[h, :, span]) * (1.0 / ORB))
            for i in range(STEPS):
                fresh = nn(inv[3 * i], columns[0:PIV], HIGHEST)
                for j in range(1, i + 1):
                    fresh += nn(inv[3 * i + j], columns[j * PIV : (j + 1) * PIV], HIGHEST)
                factor_ref[i * PIV : (i + 1) * PIV, out] = fresh
                rest -= jnp.sum(fresh * fresh, axis=0, keepdims=True)
                for at in range(0, width, 128):
                    best[i] = jnp.maximum(best[i], rest[:, at : at + 128])
            diag_ref[:, out] = rest
        return tuple(best)

    def whole_piece(t, best):
        size = sums_in.at[:, t]
        pltpu.make_async_copy(size, size, recv_sem.at[SUM + t]).wait()
        return finish(t, 0, PIECE, best)

    best = (jnp.full((1, 128), -jnp.inf, jnp.float32),) * STEPS
    best = lax.fori_loop(0, PIECES - 1, whole_piece, best)
    for half in range(2):
        arrived(LAST + half, sums_in.at[:, PIECES - 1, :, halves[half]])
        best = finish(PIECES - 1, half * 128, 128, best)
    lanes = lax.broadcasted_iota(jnp.int32, (1, 128), 1)
    peak = jnp.full((1, 128), -jnp.inf, jnp.float32)
    for i in range(STEPS):
        peak = jnp.where(lanes == i, jnp.max(best[i], axis=1, keepdims=True), peak)

    unsent.extend((SUM + t, sums_in.at[:, t]) for t in range(PIECES - 1))

    peak_buf[0] = peak
    shifts = [(dx, dz, dy, dc) for dx in range(4) for dz in range(4) for dy in range(4) for dc in range(2)]
    shifts.sort(key=lambda shift: -sum(min(step, 4 - step) for step in shift[:3]))
    for shift in shifts:
        if not any(shift):
            continue
        slot = ((shift[0] * 4 + shift[1]) * 4 + shift[2]) * 2 + shift[3]
        there = {
            "grid_0": lax.rem(x + shift[0], 4),
            "grid_1": lax.rem(z + shift[1], 4),
            "orb": lax.rem(me + shift[2], 4),
            "grid_2": lax.rem(core + shift[3], 2),
        }
        go(peak_buf.at[0], peak_buf.at[slot], PEAK_A, there)
    sent()
    arrived(PEAK_A, peak_buf.at[1:128])
    sent()
    peak_ref[...] = jnp.max(peak_buf[...], axis=0)


def hand_over(factor, diagonal, peaks, factor_out, diagonal_out, peaks_out, diagonal_flat, peaks_flat, sem):
    strip = RANK // STRIPS
    copies = []
    for i in range(STRIPS):
        rows = slice(i * strip, (i + 1) * strip)
        copies.append(pltpu.make_async_copy(factor.at[rows], factor_out.at[rows], sem.at[i]))
        copies[-1].start()
    diagonal_flat[...] = diagonal[...].reshape(SHARE)
    peaks_flat[...] = peaks[0, 0:STEPS]
    for src, dst in ((diagonal_flat, diagonal_out), (peaks_flat, peaks_out)):
        copies.append(pltpu.make_async_copy(src, dst, sem.at[len(copies)]))
        copies[-1].start()
    for copy in copies:
        copy.wait()


def on_device(orbitals, pivots):
    f32, bf16 = jnp.float32, jnp.bfloat16
    vmem = pl.BlockSpec(memory_space=pltpu.VMEM)
    factor, diagonal, peaks = pl.pallas_call(
        kernel,
        out_shape=(
            jax.ShapeDtypeStruct((RANK, SHARE), f32),
            jax.ShapeDtypeStruct((1, SHARE), f32),
            jax.ShapeDtypeStruct((1, 128), f32),
        ),
        in_specs=[pl.BlockSpec(memory_space=pltpu.HBM)] * 2,
        out_specs=(vmem, vmem, vmem),
        scratch_shapes=[
            pltpu.VMEM((STEPS, PIV), jnp.int32),
            pltpu.VMEM((ROWS // PART, DEPTH, PART), bf16),
            pltpu.VMEM((RANK, WIDE), f32),
            pltpu.VMEM((2, 4, 4, 4, HALF, 128), bf16),
            pltpu.VMEM((2, 4, STEPS, HALF, 128), bf16),
            pltpu.VMEM((4, STEPS, HALF, 128), bf16),
            pltpu.VMEM((3, STEPS, HALF, 128), bf16),
            pltpu.VMEM((4, HALF, 128), bf16),
            pltpu.VMEM((3, HALF, 128), bf16),
            pltpu.VMEM((4, RANK, WIDE), bf16),
            pltpu.VMEM((2, DEPTH, PART), bf16),
            pltpu.VMEM((2, DEPTH, PART), bf16),
            pltpu.VMEM((2, PIECES, WORDS, PIECE), jnp.int32),
            pltpu.VMEM((2, PIECES, WORDS, PIECE), jnp.int32),
            pltpu.VMEM((2, PIECES, RANK, PIECE), f32),
            pltpu.VMEM((2, 1, PART), f32),
            pltpu.VMEM((2, 1, PART), f32),
            pltpu.VMEM((2, 1, PART), f32),
            pltpu.VMEM((4, RANK, PIECE), f32),
            pltpu.VMEM((2, RANK, PIECE), f32),
            pltpu.VMEM((2, RANK, PIECE), f32),
            pltpu.VMEM((9, PIV, PIV), f32),
            pltpu.VMEM((9, PIV, PIV), f32),
            pltpu.VMEM((9, PIV, PIV), f32),
            pltpu.VMEM((128, 1, 128), f32),
            pltpu.SemaphoreType.DMA((5,)),
            pltpu.SemaphoreType.DMA((SLOTS,)),
            pltpu.SemaphoreType.DMA((SLOTS,)),
        ],
        compiler_params=pltpu.CompilerParams(
            collective_id=0, has_side_effects=True, vmem_limit_bytes=50 * 1024 * 1024
        ),
    )(orbitals, pltpu.with_memory_space_constraint(pivots, pltpu.HBM))
    factor, diagonal, peaks = pl.pallas_call(
        hand_over,
        out_shape=(
            jax.ShapeDtypeStruct((RANK, SHARE), f32),
            jax.ShapeDtypeStruct((SHARE,), f32),
            jax.ShapeDtypeStruct((STEPS,), f32),
        ),
        in_specs=[vmem] * 3,
        out_specs=(pl.BlockSpec(memory_space=pltpu.HBM),) * 3,
        scratch_shapes=[pltpu.VMEM((SHARE,), f32), pltpu.VMEM((STEPS,), f32), pltpu.SemaphoreType.DMA((STRIPS + 2,))],
        compiler_params=pltpu.CompilerParams(vmem_limit_bytes=4 * 1024 * 1024),
    )(factor, diagonal, peaks)
    return factor.T, diagonal, peaks


def solution(mesh):
    split = Mesh(
        mesh.devices.reshape(4, 4, 2, mesh.shape["orb"]), ("grid_0", "grid_1", "grid_2", "orb")
    )
    return jax.shard_map(
        on_device,
        mesh=split,
        in_specs=(P("orb", GRID), P()),
        out_specs=(P(GRID_ORB, None), P(GRID_ORB), P()),
        check_vma=False,
    )
```

```python
import functools

import jax
import jax.numpy as jnp
from jax import lax
from jax.experimental import pallas as pl
from jax.experimental.pallas import tpu as pltpu
from jax.sharding import Mesh
from jax.sharding import PartitionSpec as P

ORB = 1800
GRID = ("grid_0", "grid_1", "grid_2")
GRID_ORB = ("grid_0", "grid_1", "grid_2", "orb")
MESH = pl.DeviceIdType.MESH
HIGHEST = lax.Precision.HIGHEST

STEPS = 3
PIV = 96
RANK = STEPS * PIV
HALF = PIV // 2
DEPTH = 450
WIDE = 512
ROWS = 8192
SHARE = 2048
PART = 1024
PIECE = 256
PIECES = PART // PIECE
WORDS = 2 * PIV
STRIPS = 4
FIELD = 21
SCALE = float(2 ** (FIELD - 1) - 64)
TINY = 1e-30

FIRST = 768
RAW = 256
RAW_PIECES = RAW // PIECE

CORE_A, X_A, Z_A, Y_A, X_O, Z_O, CORE_O, B, X_C, Z_C, CORE_B, FAR, NEAR, NEAR_CODED, NORM, SUM = range(16)
LAST = SUM + PIECES - 1
PEAK_A = LAST + 2
SLOTS = LAST + 3


def nt(left, right, precision=None):
    return lax.dot_general(
        left, right, (((1,), (1,)), ((), ())), precision=precision,
        preferred_element_type=jnp.float32,
    )


def nn(left, right, precision=None):
    return lax.dot_general(
        left, right, (((1,), (0,)), ((), ())), precision=precision,
        preferred_element_type=jnp.float32,
    )


def inverse_factor(block):
    lanes = lax.broadcasted_iota(jnp.int32, (8, PIV), 1)
    subs = lax.broadcasted_iota(jnp.int32, (8, PIV), 0)
    groups = PIV // 8
    left = [block[8 * g : 8 * g + 8, :] for g in range(groups)]
    right = [jnp.where(lanes == subs + 8 * g, 1.0, 0.0) for g in range(groups)]

    def row(values, r):
        return jnp.broadcast_to(values[r : r + 1, :], (8, PIV))

    out = []
    for home in range(groups):
        column = {
            (g, j): jnp.broadcast_to(left[g][:, 8 * home + j : 8 * home + j + 1], (8, PIV))
            for g in range(home, groups)
            for j in range(8)
        }
        kept = right[home]
        for r in range(8):
            scale = lax.rsqrt(row(column[home, r], r))
            spread = [row(column[home, r], j) * scale for j in range(r + 1, 8)]
            row_left = row(left[home], r) * scale
            row_right = row(right[home], r) * scale
            kept = jnp.where(subs == r, row_right, kept)
            for g in range(home, groups):
                times = column[g, r] * scale
                if g == home:
                    times = jnp.where(subs > r, times, 0.0)
                left[g] = left[g] - times * row_left
                right[g] = right[g] - times * row_right
                for j in range(r + 1, 8):
                    column[g, j] = column[g, j] - times * spread[j - r - 1]
        out.append(kept)
    return jnp.concatenate(out, axis=0)


def kernel(
    orb_hbm, piv_hbm, factor_ref, diag_ref, peak_ref,
    pivots, orb, gathered, pv, a0, r0, r1, a2, r2, picked, far, near, sums_out, sums_in, words_out, words_in, own,
    norm_out, norm_in, own_squares, norm_own, pack, unpack, gram, low, inv, peak_buf, local_sem, send_sem, recv_sem,
):
    x = lax.axis_index("grid_0")
    z = lax.axis_index("grid_1")
    core = lax.axis_index("grid_2")
    me = lax.axis_index("orb")
    right, left, across = lax.rem(me + 1, 4), lax.rem(me + 3, 4), lax.rem(me + 2, 4)
    other = 1 - core

    barrier = pltpu.get_barrier_semaphore()
    for axis, count, index in (("orb", 4, me), ("grid_0", 4, x), ("grid_1", 4, z), ("grid_2", 2, core)):
        for d in range(1, count):
            there = {axis: lax.rem(index + d, count)}
            pl.semaphore_signal(barrier, inc=1, device_id=there, device_id_type=MESH)

    def owner_at(i):
        return lax.rem(me + 2 + i, 4)

    def load(part):
        return pltpu.make_async_copy(
            orb_hbm.at[:, pl.ds(pl.multiple_of(part * PART, PART), PART)], orb.at[part], local_sem.at[lax.div(part, 2)]
        )

    def loaded(owner):
        pair = orb.at[pl.ds(2 * owner, 2)]
        pltpu.make_async_copy(pair, pair, local_sem.at[owner]).wait()

    load_pivots = pltpu.make_async_copy(piv_hbm, pivots, local_sem.at[4])
    load_pivots.start()
    for i in range(4):
        load(2 * owner_at(i)).start()
        load(2 * owner_at(i) + 1).start()

    def remote(src, dst, slot, where):
        return pltpu.make_async_remote_copy(
            src_ref=src, dst_ref=dst, send_sem=send_sem.at[slot], recv_sem=recv_sem.at[slot],
            device_id=where, device_id_type=MESH,
        )

    def go(src, dst, slot, where):
        remote(src, dst, slot, where).start()

    unsent = []

    def arrived(slot, size):
        pltpu.make_async_copy(size, size, recv_sem.at[slot]).wait()
        unsent.append((slot, size))

    def sent():
        for slot, size in unsent:
            pltpu.make_async_copy(size, size, send_sem.at[slot]).wait()
        unsent.clear()

    base = ((x * 4 + z) * 2 + core) * ROWS
    gathered[...] = jnp.zeros_like(gathered)
    load_pivots.wait()
    square = (PIV, PIV)
    eye = lax.broadcasted_iota(jnp.int32, square, 0) == lax.broadcasted_iota(jnp.int32, square, 1)
    here = jnp.concatenate(
        [
            jnp.sum(
                jnp.where(eye, jnp.broadcast_to(pivots[s : s + 1].astype(jnp.float32), square), 0.0),
                axis=1, keepdims=True,
            )
            for s in range(STEPS)
        ],
        axis=0,
    ).astype(jnp.int32) - base

    def extract(i, carry):
        owner = owner_at(i)
        loaded(owner)
        for part in (2 * owner, 2 * owner + 1):
            spots = lax.broadcasted_iota(jnp.int32, (RANK, PART), 1) + part * PART
            chosen = jnp.where(spots == here, 1.0, 0.0).astype(jnp.bfloat16)
            gathered[:, 0:DEPTH] += nt(chosen, orb[part])
        return carry

    extract(0, 0)
    pl.semaphore_wait(barrier, 10)

    def far_copies(low, high):
        start = pl.multiple_of(across * SHARE, SHARE)
        span = slice(low, high)
        go(orb_hbm.at[:, pl.ds(start + low, high - low)], far.at[0, :, span], FAR, {"orb": left})
        go(orb_hbm.at[:, pl.ds(start + PART + low, high - low)], far.at[1, :, span], FAR, {"orb": right})

    far_copies(0, FIRST)
    lax.fori_loop(1, 4, extract, 0)
    for h in range(2):
        for lane in range(4):
            for s in range(STEPS):
                a0[h, lane, s] = gathered[
                    s * PIV + h * HALF : s * PIV + (h + 1) * HALF, lane * 128 : (lane + 1) * 128
                ].astype(jnp.bfloat16)

    go(a0.at[other], r0, CORE_A, {"grid_2": other})
    arrived(CORE_A, r0)
    r0[...] = (r0[...].astype(jnp.float32) + a0[core].astype(jnp.float32)).astype(jnp.bfloat16)
    for d in (1, 2, 3):
        there = lax.rem(x + d, 4)
        go(r0.at[there], r1.at[d - 1], X_A, {"grid_0": there})
    arrived(X_A, r1)
    total = r0[x].astype(jnp.float32)
    for d in range(3):
        total += r1[d].astype(jnp.float32)
    a2[0:STEPS] = total.astype(jnp.bfloat16)
    a2[STEPS] = jnp.zeros((HALF, 128), jnp.bfloat16)
    for d in (1, 2, 3):
        there = lax.rem(z + d, 4)
        go(a2.at[there], r2.at[d - 1], Z_A, {"grid_1": there})
    arrived(Z_A, r2)
    total = a2[z].astype(jnp.float32)
    for d in range(3):
        total += r2[d].astype(jnp.float32)
    pv[core, x, z, 0] = total.astype(jnp.bfloat16)
    mine = pv.at[core, x, z, 0]
    for d in (1, 2, 3):
        go(mine, pv.at[core, x, z, 4 - d], Y_A, {"orb": lax.rem(me + d, 4)})
    far_copies(FIRST, PART)
    go(orb.at[2 * left + 1, :, 0:RAW], near.at[1], NEAR, {"orb": left})
    go(orb.at[2 * right, :, 0:RAW], near.at[0], NEAR, {"orb": right})

    for d in (1, 2, 3):
        go(mine, mine, X_O, {"grid_0": lax.rem(x + d, 4)})

    def squares(values):
        wide = values.astype(jnp.float32)
        return jnp.sum(wide * wide, axis=0, keepdims=True)

    def near_norms(t, carry):
        span = pl.ds(pl.multiple_of(t * PIECE, PIECE), PIECE)
        after = pl.ds(pl.multiple_of(PART - RAW + t * PIECE, PIECE), PIECE)
        for h, owned in enumerate((2 * left + 1, 2 * right)):
            norm_out[h, :, after] = squares(orb[owned, :, span])
        return carry

    lax.fori_loop(RAW_PIECES, PIECES, near_norms, 0)
    arrived(X_O, r2)
    mine = pv.at[core, :, z, 0]
    for d in (1, 2, 3):
        go(mine, mine, Z_O, {"grid_1": lax.rem(z + d, 4)})
    arrived(Z_O, a0.at[0])
    mine = pv.at[core, :, 0:STEPS, 0]
    go(mine, mine, CORE_O, {"grid_2": other})
    arrived(CORE_O, pv.at[0, :, 0:STEPS, 0])

    def pick(y):
        for h in range(2):
            for lane in range(4):
                for s in range(STEPS):
                    picked[y, s * PIV + h * HALF : s * PIV + (h + 1) * HALF, lane * 128 : (lane + 1) * 128] = (
                        pv[h, lane, s, y]
                    )
        wide = picked[y].astype(jnp.float32)
        norm_own[y] = jnp.broadcast_to(jnp.sum(wide * wide, axis=1, keepdims=True), (RANK, PIECE))

    pick(0)
    pack[2] = lax.rsqrt(jnp.maximum(norm_own[0], TINY)) * SCALE

    def encode(product, scale, squared):
        whole = jnp.round(product * scale * lax.rsqrt(jnp.maximum(squared, TINY))).astype(jnp.int32)
        last = whole[2 * PIV : RANK]
        mask = (1 << FIELD) - 1
        return (
            (whole[0:PIV] & mask) | (last << FIELD),
            (whole[PIV : 2 * PIV] & mask) | ((last >> (32 - FIELD)) << FIELD),
        )

    def near_products(t, carry):
        span = pl.ds(pl.multiple_of(t * PIECE, PIECE), PIECE)
        after = pl.ds(pl.multiple_of(PART - RAW + t * PIECE, PIECE), PIECE)
        u = t - RAW_PIECES
        for h, (owned, where) in enumerate(((2 * left + 1, left), (2 * right, right))):
            product = nn(picked[0, :, 0:DEPTH], orb[owned, :, span])
            first, second = encode(product, pack[2], norm_out[h, :, after])
            words_out[h, u, 0:PIV] = first
            words_out[h, u, PIV:WORDS] = second
            go(words_out.at[h, u], words_in.at[h, u], NEAR_CODED, {"orb": where})
        return carry

    lax.fori_loop(RAW_PIECES, PIECES, near_products, 0)

    arrived(Y_A, r2)
    for d in (1, 2, 3):
        mine = pv.at[core, x, z, 1:2]
        go(mine, mine, B, {"grid_0": lax.rem(x + d, 4)})
        mine = pv.at[core, x, z, 2:4]
        go(mine, mine, B, {"grid_1": lax.rem(z + d, 4)})
    arrived(B, a0.at[0, 0:3])
    for d in (1, 2, 3):
        mine = pv.at[core, :, z, 1:2]
        go(mine, mine, Z_C, {"grid_1": lax.rem(z + d, 4)})
        mine = pv.at[core, x, 0:STEPS, 2:4]
        go(mine, mine, X_C, {"grid_0": lax.rem(x + d, 4)})

    arrived(FAR, far)

    def norms(t, carry):
        span = pl.ds(pl.multiple_of(t * PIECE, PIECE), PIECE)
        for h, owned in enumerate((2 * left, 2 * right + 1)):
            norm_out[h, :, span] = squares(orb[owned, :, span]) + squares(far[h, :, span])
        return carry

    lax.fori_loop(0, PIECES, norms, 0)
    go(norm_out.at[0], norm_in.at[0], NORM, {"orb": left})
    go(norm_out.at[1], norm_in.at[1], NORM, {"orb": right})
    arrived(Z_C, a0.at[0])
    arrived(X_C, pv.at[0, 0:3, 0:3, 0:2])
    mine = pv.at[core, :, 0:STEPS, 1:4]
    go(mine, mine, CORE_B, {"grid_2": other})
    arrived(CORE_B, pv.at[0, :, 0:STEPS, 1:4])
    for y in range(1, 4):
        pick(y)

    def size_of(squared):
        bounded = jnp.maximum(squared, TINY)
        return bounded * lax.rsqrt(bounded)

    for h, beside in enumerate((1, 3)):
        pack[h] = lax.rsqrt(jnp.maximum(norm_own[0] + norm_own[beside], TINY)) * SCALE
        unpack[h] = size_of(norm_own[beside] + norm_own[2]) * (1.0 / SCALE)
        unpack[2 + h] = size_of(norm_own[beside]) * (1.0 / SCALE)

    def decode(first, second, scale, squared):
        spare = 32 - FIELD
        whole = jnp.concatenate(
            [
                (first << spare) >> spare,
                (second << spare) >> spare,
                ((second >> FIELD) << spare) | lax.shift_right_logical(first, FIELD),
            ],
            axis=0,
        ).astype(jnp.float32)
        return whole * scale * size_of(squared)

    def send_sums(t, span, slot):
        for h, where in enumerate((left, right)):
            go(sums_out.at[h, t, :, span], sums_in.at[h, t, :, span], slot, {"orb": where})

    halves = (slice(0, 128), slice(128, 256))

    def middle(t, carry):
        span = pl.ds(pl.multiple_of(t * PIECE, PIECE), PIECE)
        for h, (own, source) in enumerate(((2 * left, 1), (2 * right + 1, 3))):
            a = orb[own, :, span]
            b = far[h, :, span]
            product = nn(picked[0, :, 0:DEPTH], a) + nn(picked[source, :, 0:DEPTH], b)
            first, second = encode(product, pack[h], norm_out[h, :, span])
            sums_out[h, t, 0:PIV] = first
            sums_out[h, t, PIV:WORDS] = second

        @pl.when(t < PIECES - 1)
        def _():
            send_sums(t, slice(0, PIECE), SUM + t)

        return carry

    lax.fori_loop(0, PIECES, middle, 0)
    for half in range(2):
        send_sums(PIECES - 1, halves[half], LAST + half)

    pairs = nt(picked[0], picked[0])
    for y in range(1, 4):
        pairs += nt(picked[y], picked[y])
    block = jnp.square(pairs * (1.0 / ORB))
    for i in range(STEPS):
        for j in range(i + 1):
            gram[3 * i + j] = block[i * PIV : (i + 1) * PIV, j * PIV : (j + 1) * PIV]

    def diagonal_inverse(i, carry):
        def update(k, carry):
            gram[4 * i] -= nt(low[3 * i + k], low[3 * i + k], HIGHEST)
            return carry

        lax.fori_loop(0, i, update, 0)
        inv[4 * i] = inverse_factor(gram[4 * i])

        def panel(j, carry):
            def update(k, carry):
                gram[3 * j + i] -= nt(low[3 * j + k], low[3 * i + k], HIGHEST)
                return carry

            lax.fori_loop(0, i, update, 0)
            low[3 * j + i] = nt(gram[3 * j + i], inv[4 * i], HIGHEST)
            return carry

        lax.fori_loop(i + 1, STEPS, panel, 0)
        return carry

    lax.fori_loop(0, STEPS, diagonal_inverse, 0)
    inv[3] = -nn(inv[4], nn(low[3], inv[0], HIGHEST), HIGHEST)
    inv[7] = -nn(inv[8], nn(low[7], inv[4], HIGHEST), HIGHEST)
    inv[6] = -nn(inv[8], nn(low[6], inv[0], HIGHEST) + nn(low[7], inv[3], HIGHEST), HIGHEST)

    arrived(NEAR, near)
    arrived(NORM, norm_in)

    def own_products(t, carry):
        span = pl.ds(pl.multiple_of(t * PIECE, PIECE), PIECE)
        for h, source in enumerate((3, 1)):
            a = orb[2 * me + h, :, span]
            b = near[h, :, span]
            own[h, t] = nn(picked[0, :, 0:DEPTH], a) + nn(picked[source, :, 0:DEPTH], b)
            own_squares[h, :, span] = squares(a) + squares(b)
        return carry

    def own_and_coded(t, carry):
        span = pl.ds(pl.multiple_of(t * PIECE, PIECE), PIECE)
        after = pl.ds(pl.multiple_of(PART - RAW + t * PIECE, PIECE), PIECE)
        u = t - RAW_PIECES
        for h in range(2):
            a = orb[2 * me + h, :, span]
            squared = norm_in[1 - h, :, after]
            coded = decode(
                words_in[1 - h, u, 0:PIV], words_in[1 - h, u, PIV:WORDS], unpack[3 - h], squared
            )
            own[h, t] = nn(picked[0, :, 0:DEPTH], a) + coded
            own_squares[h, :, span] = squares(a) + squared
        return carry

    lax.fori_loop(0, RAW_PIECES, own_products, 0)
    arrived(NEAR_CODED, words_in)
    lax.fori_loop(RAW_PIECES, PIECES, own_and_coded, 0)

    def finish(t, low, width, best):
        best = list(best)
        for h in range(2):
            start = t * PIECE + low
            span = pl.ds(pl.multiple_of(start, 128), width)
            out = pl.ds(pl.multiple_of(h * PART + start, 128), width)
            inside = slice(low, low + width)
            norm = norm_in[h, :, span]
            received = decode(
                sums_in[h, t, 0:PIV, inside], sums_in[h, t, PIV:WORDS, inside], unpack[h, :, 0:width], norm
            )
            columns = jnp.square((received + own[h, t, :, inside]) * (1.0 / ORB))
            rest = jnp.square((norm + own_squares[h, :, span]) * (1.0 / ORB))
            for i in range(STEPS):
                fresh = nn(inv[3 * i], columns[0:PIV], HIGHEST)
                for j in range(1, i + 1):
                    fresh += nn(inv[3 * i + j], columns[j * PIV : (j + 1) * PIV], HIGHEST)
                factor_ref[i * PIV : (i + 1) * PIV, out] = fresh
                rest -= jnp.sum(fresh * fresh, axis=0, keepdims=True)
                for at in range(0, width, 128):
                    best[i] = jnp.maximum(best[i], rest[:, at : at + 128])
            diag_ref[:, out] = rest
        return tuple(best)

    def whole_piece(t, best):
        size = sums_in.at[:, t]
        pltpu.make_async_copy(size, size, recv_sem.at[SUM + t]).wait()
        return finish(t, 0, PIECE, best)

    best = (jnp.full((1, 128), -jnp.inf, jnp.float32),) * STEPS
    best = lax.fori_loop(0, PIECES - 1, whole_piece, best)
    for half in range(2):
        arrived(LAST + half, sums_in.at[:, PIECES - 1, :, halves[half]])
        best = finish(PIECES - 1, half * 128, 128, best)
    lanes = lax.broadcasted_iota(jnp.int32, (1, 128), 1)
    peak = jnp.full((1, 128), -jnp.inf, jnp.float32)
    for i in range(STEPS):
        peak = jnp.where(lanes == i, jnp.max(best[i], axis=1, keepdims=True), peak)

    unsent.extend((SUM + t, sums_in.at[:, t]) for t in range(PIECES - 1))

    peak_buf[0] = peak
    shifts = [(dx, dz, dy, dc) for dx in range(4) for dz in range(4) for dy in range(4) for dc in range(2)]
    shifts.sort(key=lambda shift: -sum(min(step, 4 - step) for step in shift[:3]))
    for shift in shifts:
        if not any(shift):
            continue
        slot = ((shift[0] * 4 + shift[1]) * 4 + shift[2]) * 2 + shift[3]
        there = {
            "grid_0": lax.rem(x + shift[0], 4),
            "grid_1": lax.rem(z + shift[1], 4),
            "orb": lax.rem(me + shift[2], 4),
            "grid_2": lax.rem(core + shift[3], 2),
        }
        go(peak_buf.at[0], peak_buf.at[slot], PEAK_A, there)
    sent()
    arrived(PEAK_A, peak_buf.at[1:128])
    sent()
    peak_ref[...] = jnp.max(peak_buf[...], axis=0)


def hand_over(factor, diagonal, peaks, factor_out, diagonal_out, peaks_out, diagonal_flat, peaks_flat, sem):
    strip = RANK // STRIPS
    copies = []
    for i in range(STRIPS):
        rows = slice(i * strip, (i + 1) * strip)
        copies.append(pltpu.make_async_copy(factor.at[rows], factor_out.at[rows], sem.at[i]))
        copies[-1].start()
    diagonal_flat[...] = diagonal[...].reshape(SHARE)
    peaks_flat[...] = peaks[0, 0:STEPS]
    for src, dst in ((diagonal_flat, diagonal_out), (peaks_flat, peaks_out)):
        copies.append(pltpu.make_async_copy(src, dst, sem.at[len(copies)]))
        copies[-1].start()
    for copy in copies:
        copy.wait()


def on_device(orbitals, pivots):
    f32, bf16 = jnp.float32, jnp.bfloat16
    vmem = pl.BlockSpec(memory_space=pltpu.VMEM)
    factor, diagonal, peaks = pl.pallas_call(
        kernel,
        out_shape=(
            jax.ShapeDtypeStruct((RANK, SHARE), f32),
            jax.ShapeDtypeStruct((1, SHARE), f32),
            jax.ShapeDtypeStruct((1, 128), f32),
        ),
        in_specs=[pl.BlockSpec(memory_space=pltpu.HBM)] * 2,
        out_specs=(vmem, vmem, vmem),
        scratch_shapes=[
            pltpu.VMEM((STEPS, PIV), jnp.int32),
            pltpu.VMEM((ROWS // PART, DEPTH, PART), bf16),
            pltpu.VMEM((RANK, WIDE), f32),
            pltpu.VMEM((2, 4, 4, 4, HALF, 128), bf16),
            pltpu.VMEM((2, 4, STEPS, HALF, 128), bf16),
            pltpu.VMEM((4, STEPS, HALF, 128), bf16),
            pltpu.VMEM((3, STEPS, HALF, 128), bf16),
            pltpu.VMEM((4, HALF, 128), bf16),
            pltpu.VMEM((3, HALF, 128), bf16),
            pltpu.VMEM((4, RANK, WIDE), bf16),
            pltpu.VMEM((2, DEPTH, PART), bf16),
            pltpu.VMEM((2, DEPTH, RAW), bf16),
            pltpu.VMEM((2, PIECES, WORDS, PIECE), jnp.int32),
            pltpu.VMEM((2, PIECES, WORDS, PIECE), jnp.int32),
            pltpu.VMEM((2, PIECES - RAW_PIECES, WORDS, PIECE), jnp.int32),
            pltpu.VMEM((2, PIECES - RAW_PIECES, WORDS, PIECE), jnp.int32),
            pltpu.VMEM((2, PIECES, RANK, PIECE), f32),
            pltpu.VMEM((2, 1, 2 * PART - RAW), f32),
            pltpu.VMEM((2, 1, 2 * PART - RAW), f32),
            pltpu.VMEM((2, 1, PART), f32),
            pltpu.VMEM((4, RANK, PIECE), f32),
            pltpu.VMEM((3, RANK, PIECE), f32),
            pltpu.VMEM((4, RANK, PIECE), f32),
            pltpu.VMEM((9, PIV, PIV), f32),
            pltpu.VMEM((9, PIV, PIV), f32),
            pltpu.VMEM((9, PIV, PIV), f32),
            pltpu.VMEM((128, 1, 128), f32),
            pltpu.SemaphoreType.DMA((5,)),
            pltpu.SemaphoreType.DMA((SLOTS,)),
            pltpu.SemaphoreType.DMA((SLOTS,)),
        ],
        compiler_params=pltpu.CompilerParams(
            collective_id=0, has_side_effects=True, vmem_limit_bytes=50 * 1024 * 1024
        ),
    )(orbitals, pltpu.with_memory_space_constraint(pivots, pltpu.HBM))
    factor, diagonal, peaks = pl.pallas_call(
        hand_over,
        out_shape=(
            jax.ShapeDtypeStruct((RANK, SHARE), f32),
            jax.ShapeDtypeStruct((SHARE,), f32),
            jax.ShapeDtypeStruct((STEPS,), f32),
        ),
        in_specs=[vmem] * 3,
        out_specs=(pl.BlockSpec(memory_space=pltpu.HBM),) * 3,
        scratch_shapes=[pltpu.VMEM((SHARE,), f32), pltpu.VMEM((STEPS,), f32), pltpu.SemaphoreType.DMA((STRIPS + 2,))],
        compiler_params=pltpu.CompilerParams(vmem_limit_bytes=4 * 1024 * 1024),
    )(factor, diagonal, peaks)
    return factor.T, diagonal, peaks


def solution(mesh):
    split = Mesh(
        mesh.devices.reshape(4, 4, 2, mesh.shape["orb"]), ("grid_0", "grid_1", "grid_2", "orb")
    )
    return jax.shard_map(
        on_device,
        mesh=split,
        in_specs=(P("orb", GRID), P()),
        out_specs=(P(GRID_ORB, None), P(GRID_ORB), P()),
        check_vma=False,
    )
```

```python
import functools

import jax
import jax.numpy as jnp
from jax import lax
from jax.experimental import pallas as pl
from jax.experimental.pallas import tpu as pltpu
from jax.sharding import Mesh
from jax.sharding import PartitionSpec as P

ORB = 1800
GRID = ("grid_0", "grid_1", "grid_2")
GRID_ORB = ("grid_0", "grid_1", "grid_2", "orb")
MESH = pl.DeviceIdType.MESH
HIGHEST = lax.Precision.HIGHEST

STEPS = 3
PIV = 96
RANK = STEPS * PIV
HALF = PIV // 2
DEPTH = 450
WIDE = 512
ROWS = 8192
SHARE = 2048
PART = 1024
PIECE = 256
PIECES = PART // PIECE
WORDS = 2 * PIV
STRIPS = 4
FIELD = 21
SCALE = float(2 ** (FIELD - 1) - 64)
TINY = 1e-30

FIRST = 768

CORE_A, X_A, Z_A, Y_A, X_O, Z_O, CORE_O, B, X_C, Z_C, CORE_B, FAR, NEAR, NORM, SUM = range(15)
LAST = SUM + PIECES - 1
PEAK_A = LAST + 2
SLOTS = LAST + 3


def nt(left, right, precision=None):
    return lax.dot_general(
        left, right, (((1,), (1,)), ((), ())), precision=precision,
        preferred_element_type=jnp.float32,
    )


def nn(left, right, precision=None):
    return lax.dot_general(
        left, right, (((1,), (0,)), ((), ())), precision=precision,
        preferred_element_type=jnp.float32,
    )


def inverse_factor(block):
    lanes = lax.broadcasted_iota(jnp.int32, (8, PIV), 1)
    subs = lax.broadcasted_iota(jnp.int32, (8, PIV), 0)
    groups = PIV // 8
    left = [block[8 * g : 8 * g + 8, :] for g in range(groups)]
    right = [jnp.where(lanes == subs + 8 * g, 1.0, 0.0) for g in range(groups)]

    def row(values, r):
        return jnp.broadcast_to(values[r : r + 1, :], (8, PIV))

    out = []
    for home in range(groups):
        column = {
            (g, j): jnp.broadcast_to(left[g][:, 8 * home + j : 8 * home + j + 1], (8, PIV))
            for g in range(home, groups)
            for j in range(8)
        }
        kept = right[home]
        for r in range(8):
            scale = lax.rsqrt(row(column[home, r], r))
            spread = [row(column[home, r], j) * scale for j in range(r + 1, 8)]
            row_left = row(left[home], r) * scale
            row_right = row(right[home], r) * scale
            kept = jnp.where(subs == r, row_right, kept)
            for g in range(home, groups):
                times = column[g, r] * scale
                if g == home:
                    times = jnp.where(subs > r, times, 0.0)
                left[g] = left[g] - times * row_left
                right[g] = right[g] - times * row_right
                for j in range(r + 1, 8):
                    column[g, j] = column[g, j] - times * spread[j - r - 1]
        out.append(kept)
    return jnp.concatenate(out, axis=0)


def kernel(
    orb_hbm, piv_hbm, factor_ref, diag_ref, peak_ref,
    pivots, orb, gathered, pv, a0, r0, r1, a2, r2, picked, far, sums_out, sums_in, words_out, words_in, own,
    norm_out, norm_in, own_squares, norm_own, pack, unpack, gram, low, inv, peak_buf, local_sem, send_sem, recv_sem,
):
    x = lax.axis_index("grid_0")
    z = lax.axis_index("grid_1")
    core = lax.axis_index("grid_2")
    me = lax.axis_index("orb")
    right, left, across = lax.rem(me + 1, 4), lax.rem(me + 3, 4), lax.rem(me + 2, 4)
    other = 1 - core

    barrier = pltpu.get_barrier_semaphore()
    for axis, count, index in (("orb", 4, me), ("grid_0", 4, x), ("grid_1", 4, z), ("grid_2", 2, core)):
        for d in range(1, count):
            there = {axis: lax.rem(index + d, count)}
            pl.semaphore_signal(barrier, inc=1, device_id=there, device_id_type=MESH)

    def owner_at(i):
        return lax.rem(me + 2 + i, 4)

    def load(part):
        return pltpu.make_async_copy(
            orb_hbm.at[:, pl.ds(pl.multiple_of(part * PART, PART), PART)], orb.at[part], local_sem.at[lax.div(part, 2)]
        )

    def loaded(owner):
        pair = orb.at[pl.ds(2 * owner, 2)]
        pltpu.make_async_copy(pair, pair, local_sem.at[owner]).wait()

    load_pivots = pltpu.make_async_copy(piv_hbm, pivots, local_sem.at[4])
    load_pivots.start()
    for i in range(4):
        load(2 * owner_at(i)).start()
        load(2 * owner_at(i) + 1).start()

    def remote(src, dst, slot, where):
        return pltpu.make_async_remote_copy(
            src_ref=src, dst_ref=dst, send_sem=send_sem.at[slot], recv_sem=recv_sem.at[slot],
            device_id=where, device_id_type=MESH,
        )

    def go(src, dst, slot, where):
        remote(src, dst, slot, where).start()

    unsent = []

    def arrived(slot, size):
        pltpu.make_async_copy(size, size, recv_sem.at[slot]).wait()
        unsent.append((slot, size))

    def sent():
        for slot, size in unsent:
            pltpu.make_async_copy(size, size, send_sem.at[slot]).wait()
        unsent.clear()

    base = ((x * 4 + z) * 2 + core) * ROWS
    gathered[...] = jnp.zeros_like(gathered)
    load_pivots.wait()
    square = (PIV, PIV)
    eye = lax.broadcasted_iota(jnp.int32, square, 0) == lax.broadcasted_iota(jnp.int32, square, 1)
    here = jnp.concatenate(
        [
            jnp.sum(
                jnp.where(eye, jnp.broadcast_to(pivots[s : s + 1].astype(jnp.float32), square), 0.0),
                axis=1, keepdims=True,
            )
            for s in range(STEPS)
        ],
        axis=0,
    ).astype(jnp.int32) - base

    def extract(i, carry):
        owner = owner_at(i)
        loaded(owner)
        for part in (2 * owner, 2 * owner + 1):
            spots = lax.broadcasted_iota(jnp.int32, (RANK, PART), 1) + part * PART
            chosen = jnp.where(spots == here, 1.0, 0.0).astype(jnp.bfloat16)
            gathered[:, 0:DEPTH] += nt(chosen, orb[part])
        return carry

    extract(0, 0)
    pl.semaphore_wait(barrier, 10)

    def far_copies(low, high):
        start = pl.multiple_of(across * SHARE, SHARE)
        span = slice(low, high)
        go(orb_hbm.at[:, pl.ds(start + low, high - low)], far.at[0, :, span], FAR, {"orb": left})
        go(orb_hbm.at[:, pl.ds(start + PART + low, high - low)], far.at[1, :, span], FAR, {"orb": right})

    far_copies(0, FIRST)
    lax.fori_loop(1, 4, extract, 0)
    for h in range(2):
        for lane in range(4):
            for s in range(STEPS):
                a0[h, lane, s] = gathered[
                    s * PIV + h * HALF : s * PIV + (h + 1) * HALF, lane * 128 : (lane + 1) * 128
                ].astype(jnp.bfloat16)

    go(a0.at[other], r0, CORE_A, {"grid_2": other})
    arrived(CORE_A, r0)
    r0[...] = (r0[...].astype(jnp.float32) + a0[core].astype(jnp.float32)).astype(jnp.bfloat16)
    for d in (1, 2, 3):
        there = lax.rem(x + d, 4)
        go(r0.at[there], r1.at[d - 1], X_A, {"grid_0": there})
    arrived(X_A, r1)
    total = r0[x].astype(jnp.float32)
    for d in range(3):
        total += r1[d].astype(jnp.float32)
    a2[0:STEPS] = total.astype(jnp.bfloat16)
    a2[STEPS] = jnp.zeros((HALF, 128), jnp.bfloat16)
    for d in (1, 2, 3):
        there = lax.rem(z + d, 4)
        go(a2.at[there], r2.at[d - 1], Z_A, {"grid_1": there})
    arrived(Z_A, r2)
    total = a2[z].astype(jnp.float32)
    for d in range(3):
        total += r2[d].astype(jnp.float32)
    pv[core, x, z, 0] = total.astype(jnp.bfloat16)
    mine = pv.at[core, x, z, 0]
    for d in (1, 2, 3):
        go(mine, pv.at[core, x, z, 4 - d], Y_A, {"orb": lax.rem(me + d, 4)})
    far_copies(FIRST, PART)

    for d in (1, 2, 3):
        go(mine, mine, X_O, {"grid_0": lax.rem(x + d, 4)})

    def squares(values):
        wide = values.astype(jnp.float32)
        return jnp.sum(wide * wide, axis=0, keepdims=True)

    def near_norms(t, carry):
        span = pl.ds(pl.multiple_of(t * PIECE, PIECE), PIECE)
        after = pl.ds(pl.multiple_of(PART + t * PIECE, PIECE), PIECE)
        for h, owned in enumerate((2 * left + 1, 2 * right)):
            norm_out[h, :, after] = squares(orb[owned, :, span])
        return carry

    lax.fori_loop(0, PIECES, near_norms, 0)
    arrived(X_O, r2)
    mine = pv.at[core, :, z, 0]
    for d in (1, 2, 3):
        go(mine, mine, Z_O, {"grid_1": lax.rem(z + d, 4)})
    arrived(Z_O, a0.at[0])
    mine = pv.at[core, :, 0:STEPS, 0]
    go(mine, mine, CORE_O, {"grid_2": other})
    arrived(CORE_O, pv.at[0, :, 0:STEPS, 0])

    def pick(y):
        for h in range(2):
            for lane in range(4):
                for s in range(STEPS):
                    picked[y, s * PIV + h * HALF : s * PIV + (h + 1) * HALF, lane * 128 : (lane + 1) * 128] = (
                        pv[h, lane, s, y]
                    )
        wide = picked[y].astype(jnp.float32)
        norm_own[y] = jnp.broadcast_to(jnp.sum(wide * wide, axis=1, keepdims=True), (RANK, PIECE))

    pick(0)
    pack[2] = lax.rsqrt(jnp.maximum(norm_own[0], TINY)) * SCALE

    def encode(product, scale, squared):
        whole = jnp.round(product * scale * lax.rsqrt(jnp.maximum(squared, TINY))).astype(jnp.int32)
        last = whole[2 * PIV : RANK]
        mask = (1 << FIELD) - 1
        return (
            (whole[0:PIV] & mask) | (last << FIELD),
            (whole[PIV : 2 * PIV] & mask) | ((last >> (32 - FIELD)) << FIELD),
        )

    def near_products(t, carry):
        span = pl.ds(pl.multiple_of(t * PIECE, PIECE), PIECE)
        after = pl.ds(pl.multiple_of(PART + t * PIECE, PIECE), PIECE)
        for h, (owned, where) in enumerate(((2 * left + 1, left), (2 * right, right))):
            product = nn(picked[0, :, 0:DEPTH], orb[owned, :, span])
            first, second = encode(product, pack[2], norm_out[h, :, after])
            words_out[h, t, 0:PIV] = first
            words_out[h, t, PIV:WORDS] = second
            go(words_out.at[h, t], words_in.at[h, t], NEAR, {"orb": where})
        return carry

    lax.fori_loop(0, PIECES, near_products, 0)

    arrived(Y_A, r2)
    for d in (1, 2, 3):
        mine = pv.at[core, x, z, 1:2]
        go(mine, mine, B, {"grid_0": lax.rem(x + d, 4)})
        mine = pv.at[core, x, z, 2:4]
        go(mine, mine, B, {"grid_1": lax.rem(z + d, 4)})
    arrived(B, a0.at[0, 0:3])
    for d in (1, 2, 3):
        mine = pv.at[core, :, z, 1:2]
        go(mine, mine, Z_C, {"grid_1": lax.rem(z + d, 4)})
        mine = pv.at[core, x, 0:STEPS, 2:4]
        go(mine, mine, X_C, {"grid_0": lax.rem(x + d, 4)})

    arrived(FAR, far)

    def norms(t, carry):
        span = pl.ds(pl.multiple_of(t * PIECE, PIECE), PIECE)
        for h, owned in enumerate((2 * left, 2 * right + 1)):
            norm_out[h, :, span] = squares(orb[owned, :, span]) + squares(far[h, :, span])
        return carry

    lax.fori_loop(0, PIECES, norms, 0)
    go(norm_out.at[0], norm_in.at[0], NORM, {"orb": left})
    go(norm_out.at[1], norm_in.at[1], NORM, {"orb": right})
    arrived(Z_C, a0.at[0])
    arrived(X_C, pv.at[0, 0:3, 0:3, 0:2])
    mine = pv.at[core, :, 0:STEPS, 1:4]
    go(mine, mine, CORE_B, {"grid_2": other})
    arrived(CORE_B, pv.at[0, :, 0:STEPS, 1:4])
    for y in range(1, 4):
        pick(y)

    def size_of(squared):
        bounded = jnp.maximum(squared, TINY)
        return bounded * lax.rsqrt(bounded)

    for h, beside in enumerate((1, 3)):
        pack[h] = lax.rsqrt(jnp.maximum(norm_own[0] + norm_own[beside], TINY)) * SCALE
        unpack[h] = size_of(norm_own[beside] + norm_own[2]) * (1.0 / SCALE)
        unpack[2 + h] = size_of(norm_own[beside]) * (1.0 / SCALE)

    def decode(first, second, scale, squared):
        spare = 32 - FIELD
        whole = jnp.concatenate(
            [
                (first << spare) >> spare,
                (second << spare) >> spare,
                ((second >> FIELD) << spare) | lax.shift_right_logical(first, FIELD),
            ],
            axis=0,
        ).astype(jnp.float32)
        return whole * scale * size_of(squared)

    def send_sums(t, span, slot):
        for h, where in enumerate((left, right)):
            go(sums_out.at[h, t, :, span], sums_in.at[h, t, :, span], slot, {"orb": where})

    halves = (slice(0, 128), slice(128, 256))

    def middle(t, carry):
        span = pl.ds(pl.multiple_of(t * PIECE, PIECE), PIECE)
        for h, (own, source) in enumerate(((2 * left, 1), (2 * right + 1, 3))):
            a = orb[own, :, span]
            b = far[h, :, span]
            product = nn(picked[0, :, 0:DEPTH], a) + nn(picked[source, :, 0:DEPTH], b)
            first, second = encode(product, pack[h], norm_out[h, :, span])
            sums_out[h, t, 0:PIV] = first
            sums_out[h, t, PIV:WORDS] = second

        @pl.when(t < PIECES - 1)
        def _():
            send_sums(t, slice(0, PIECE), SUM + t)

        return carry

    lax.fori_loop(0, PIECES, middle, 0)
    for half in range(2):
        send_sums(PIECES - 1, halves[half], LAST + half)

    pairs = nt(picked[0], picked[0])
    for y in range(1, 4):
        pairs += nt(picked[y], picked[y])
    block = jnp.square(pairs * (1.0 / ORB))
    for i in range(STEPS):
        for j in range(i + 1):
            gram[3 * i + j] = block[i * PIV : (i + 1) * PIV, j * PIV : (j + 1) * PIV]

    def diagonal_inverse(i, carry):
        def update(k, carry):
            gram[4 * i] -= nt(low[3 * i + k], low[3 * i + k], HIGHEST)
            return carry

        lax.fori_loop(0, i, update, 0)
        inv[4 * i] = inverse_factor(gram[4 * i])

        def panel(j, carry):
            def update(k, carry):
                gram[3 * j + i] -= nt(low[3 * j + k], low[3 * i + k], HIGHEST)
                return carry

            lax.fori_loop(0, i, update, 0)
            low[3 * j + i] = nt(gram[3 * j + i], inv[4 * i], HIGHEST)
            return carry

        lax.fori_loop(i + 1, STEPS, panel, 0)
        return carry

    lax.fori_loop(0, STEPS, diagonal_inverse, 0)
    inv[3] = -nn(inv[4], nn(low[3], inv[0], HIGHEST), HIGHEST)
    inv[7] = -nn(inv[8], nn(low[7], inv[4], HIGHEST), HIGHEST)
    inv[6] = -nn(inv[8], nn(low[6], inv[0], HIGHEST) + nn(low[7], inv[3], HIGHEST), HIGHEST)

    arrived(NORM, norm_in)

    def own_and_coded(t, carry):
        span = pl.ds(pl.multiple_of(t * PIECE, PIECE), PIECE)
        after = pl.ds(pl.multiple_of(PART + t * PIECE, PIECE), PIECE)
        for h in range(2):
            a = orb[2 * me + h, :, span]
            squared = norm_in[1 - h, :, after]
            coded = decode(
                words_in[1 - h, t, 0:PIV], words_in[1 - h, t, PIV:WORDS], unpack[3 - h], squared
            )
            own[h, t] = nn(picked[0, :, 0:DEPTH], a) + coded
            own_squares[h, :, span] = squares(a) + squared
        return carry

    arrived(NEAR, words_in)
    lax.fori_loop(0, PIECES, own_and_coded, 0)

    def finish(t, low, width, best):
        best = list(best)
        for h in range(2):
            start = t * PIECE + low
            span = pl.ds(pl.multiple_of(start, 128), width)
            out = pl.ds(pl.multiple_of(h * PART + start, 128), width)
            inside = slice(low, low + width)
            norm = norm_in[h, :, span]
            received = decode(
                sums_in[h, t, 0:PIV, inside], sums_in[h, t, PIV:WORDS, inside], unpack[h, :, 0:width], norm
            )
            columns = jnp.square((received + own[h, t, :, inside]) * (1.0 / ORB))
            rest = jnp.square((norm + own_squares[h, :, span]) * (1.0 / ORB))
            for i in range(STEPS):
                fresh = nn(inv[3 * i], columns[0:PIV], HIGHEST)
                for j in range(1, i + 1):
                    fresh += nn(inv[3 * i + j], columns[j * PIV : (j + 1) * PIV], HIGHEST)
                factor_ref[i * PIV : (i + 1) * PIV, out] = fresh
                rest -= jnp.sum(fresh * fresh, axis=0, keepdims=True)
                for at in range(0, width, 128):
                    best[i] = jnp.maximum(best[i], rest[:, at : at + 128])
            diag_ref[:, out] = rest
        return tuple(best)

    def whole_piece(t, best):
        size = sums_in.at[:, t]
        pltpu.make_async_copy(size, size, recv_sem.at[SUM + t]).wait()
        return finish(t, 0, PIECE, best)

    best = (jnp.full((1, 128), -jnp.inf, jnp.float32),) * STEPS
    best = lax.fori_loop(0, PIECES - 1, whole_piece, best)
    for half in range(2):
        arrived(LAST + half, sums_in.at[:, PIECES - 1, :, halves[half]])
        best = finish(PIECES - 1, half * 128, 128, best)
    lanes = lax.broadcasted_iota(jnp.int32, (1, 128), 1)
    peak = jnp.full((1, 128), -jnp.inf, jnp.float32)
    for i in range(STEPS):
        peak = jnp.where(lanes == i, jnp.max(best[i], axis=1, keepdims=True), peak)

    unsent.extend((SUM + t, sums_in.at[:, t]) for t in range(PIECES - 1))

    peak_buf[0] = peak
    shifts = [(dx, dz, dy, dc) for dx in range(4) for dz in range(4) for dy in range(4) for dc in range(2)]
    shifts.sort(key=lambda shift: -sum(min(step, 4 - step) for step in shift[:3]))
    for shift in shifts:
        if not any(shift):
            continue
        slot = ((shift[0] * 4 + shift[1]) * 4 + shift[2]) * 2 + shift[3]
        there = {
            "grid_0": lax.rem(x + shift[0], 4),
            "grid_1": lax.rem(z + shift[1], 4),
            "orb": lax.rem(me + shift[2], 4),
            "grid_2": lax.rem(core + shift[3], 2),
        }
        go(peak_buf.at[0], peak_buf.at[slot], PEAK_A, there)
    sent()
    arrived(PEAK_A, peak_buf.at[1:128])
    sent()
    peak_ref[...] = jnp.max(peak_buf[...], axis=0)


def hand_over(factor, diagonal, peaks, factor_out, diagonal_out, peaks_out, diagonal_flat, peaks_flat, sem):
    strip = RANK // STRIPS
    copies = []
    for i in range(STRIPS):
        rows = slice(i * strip, (i + 1) * strip)
        copies.append(pltpu.make_async_copy(factor.at[rows], factor_out.at[rows], sem.at[i]))
        copies[-1].start()
    diagonal_flat[...] = diagonal[...].reshape(SHARE)
    peaks_flat[...] = peaks[0, 0:STEPS]
    for src, dst in ((diagonal_flat, diagonal_out), (peaks_flat, peaks_out)):
        copies.append(pltpu.make_async_copy(src, dst, sem.at[len(copies)]))
        copies[-1].start()
    for copy in copies:
        copy.wait()


def on_device(orbitals, pivots):
    f32, bf16 = jnp.float32, jnp.bfloat16
    vmem = pl.BlockSpec(memory_space=pltpu.VMEM)
    factor, diagonal, peaks = pl.pallas_call(
        kernel,
        out_shape=(
            jax.ShapeDtypeStruct((RANK, SHARE), f32),
            jax.ShapeDtypeStruct((1, SHARE), f32),
            jax.ShapeDtypeStruct((1, 128), f32),
        ),
        in_specs=[pl.BlockSpec(memory_space=pltpu.HBM)] * 2,
        out_specs=(vmem, vmem, vmem),
        scratch_shapes=[
            pltpu.VMEM((STEPS, PIV), jnp.int32),
            pltpu.VMEM((ROWS // PART, DEPTH, PART), bf16),
            pltpu.VMEM((RANK, WIDE), f32),
            pltpu.VMEM((2, 4, 4, 4, HALF, 128), bf16),
            pltpu.VMEM((2, 4, STEPS, HALF, 128), bf16),
            pltpu.VMEM((4, STEPS, HALF, 128), bf16),
            pltpu.VMEM((3, STEPS, HALF, 128), bf16),
            pltpu.VMEM((4, HALF, 128), bf16),
            pltpu.VMEM((3, HALF, 128), bf16),
            pltpu.VMEM((4, RANK, WIDE), bf16),
            pltpu.VMEM((2, DEPTH, PART), bf16),
            pltpu.VMEM((2, PIECES, WORDS, PIECE), jnp.int32),
            pltpu.VMEM((2, PIECES, WORDS, PIECE), jnp.int32),
            pltpu.VMEM((2, PIECES, WORDS, PIECE), jnp.int32),
            pltpu.VMEM((2, PIECES, WORDS, PIECE), jnp.int32),
            pltpu.VMEM((2, PIECES, RANK, PIECE), f32),
            pltpu.VMEM((2, 1, 2 * PART), f32),
            pltpu.VMEM((2, 1, 2 * PART), f32),
            pltpu.VMEM((2, 1, PART), f32),
            pltpu.VMEM((4, RANK, PIECE), f32),
            pltpu.VMEM((3, RANK, PIECE), f32),
            pltpu.VMEM((4, RANK, PIECE), f32),
            pltpu.VMEM((9, PIV, PIV), f32),
            pltpu.VMEM((9, PIV, PIV), f32),
            pltpu.VMEM((9, PIV, PIV), f32),
            pltpu.VMEM((128, 1, 128), f32),
            pltpu.SemaphoreType.DMA((5,)),
            pltpu.SemaphoreType.DMA((SLOTS,)),
            pltpu.SemaphoreType.DMA((SLOTS,)),
        ],
        compiler_params=pltpu.CompilerParams(
            collective_id=0, has_side_effects=True, vmem_limit_bytes=50 * 1024 * 1024
        ),
    )(orbitals, pltpu.with_memory_space_constraint(pivots, pltpu.HBM))
    factor, diagonal, peaks = pl.pallas_call(
        hand_over,
        out_shape=(
            jax.ShapeDtypeStruct((RANK, SHARE), f32),
            jax.ShapeDtypeStruct((SHARE,), f32),
            jax.ShapeDtypeStruct((STEPS,), f32),
        ),
        in_specs=[vmem] * 3,
        out_specs=(pl.BlockSpec(memory_space=pltpu.HBM),) * 3,
        scratch_shapes=[pltpu.VMEM((SHARE,), f32), pltpu.VMEM((STEPS,), f32), pltpu.SemaphoreType.DMA((STRIPS + 2,))],
        compiler_params=pltpu.CompilerParams(vmem_limit_bytes=4 * 1024 * 1024),
    )(factor, diagonal, peaks)
    return factor.T, diagonal, peaks


def solution(mesh):
    split = Mesh(
        mesh.devices.reshape(4, 4, 2, mesh.shape["orb"]), ("grid_0", "grid_1", "grid_2", "orb")
    )
    return jax.shard_map(
        on_device,
        mesh=split,
        in_specs=(P("orb", GRID), P()),
        out_specs=(P(GRID_ORB, None), P(GRID_ORB), P()),
        check_vma=False,
    )
```

```python
import functools

import jax
import jax.numpy as jnp
from jax import lax
from jax.experimental import pallas as pl
from jax.experimental.pallas import tpu as pltpu
from jax.sharding import Mesh
from jax.sharding import PartitionSpec as P

ORB = 1800
GRID = ("grid_0", "grid_1", "grid_2")
GRID_ORB = ("grid_0", "grid_1", "grid_2", "orb")
MESH = pl.DeviceIdType.MESH
HIGHEST = lax.Precision.HIGHEST

STEPS = 3
PIV = 96
RANK = STEPS * PIV
HALF = PIV // 2
DEPTH = 450
WIDE = 512
ROWS = 8192
SHARE = 2048
PART = 1024
PIECE = 256
PIECES = PART // PIECE
BLOCK = 16
VALUES, FIELDS = 18, 11
WORDS = FIELDS * BLOCK
STRIPS = 4
FIELD = 19
SPARE = 32 - FIELD
REST = FIELD - SPARE
SCALE = float(2 ** (FIELD - 1) - 16)
TINY = 1e-30

FIRST = 768

CORE_A, X_A, Z_A, Y_A, X_O, Z_O, CORE_O, B, X_C, Z_C, CORE_B, FAR, NEAR, NORM, SUM = range(15)
LAST = SUM + PIECES - 1
PEAK_A = LAST + 2
SLOTS = LAST + 3


def nt(left, right, precision=None):
    return lax.dot_general(
        left, right, (((1,), (1,)), ((), ())), precision=precision,
        preferred_element_type=jnp.float32,
    )


def nn(left, right, precision=None):
    return lax.dot_general(
        left, right, (((1,), (0,)), ((), ())), precision=precision,
        preferred_element_type=jnp.float32,
    )


def inverse_factor(block):
    lanes = lax.broadcasted_iota(jnp.int32, (8, PIV), 1)
    subs = lax.broadcasted_iota(jnp.int32, (8, PIV), 0)
    groups = PIV // 8
    left = [block[8 * g : 8 * g + 8, :] for g in range(groups)]
    right = [jnp.where(lanes == subs + 8 * g, 1.0, 0.0) for g in range(groups)]

    def row(values, r):
        return jnp.broadcast_to(values[r : r + 1, :], (8, PIV))

    out = []
    for home in range(groups):
        column = {
            (g, j): jnp.broadcast_to(left[g][:, 8 * home + j : 8 * home + j + 1], (8, PIV))
            for g in range(home, groups)
            for j in range(8)
        }
        kept = right[home]
        for r in range(8):
            scale = lax.rsqrt(row(column[home, r], r))
            spread = [row(column[home, r], j) * scale for j in range(r + 1, 8)]
            row_left = row(left[home], r) * scale
            row_right = row(right[home], r) * scale
            kept = jnp.where(subs == r, row_right, kept)
            for g in range(home, groups):
                times = column[g, r] * scale
                if g == home:
                    times = jnp.where(subs > r, times, 0.0)
                left[g] = left[g] - times * row_left
                right[g] = right[g] - times * row_right
                for j in range(r + 1, 8):
                    column[g, j] = column[g, j] - times * spread[j - r - 1]
        out.append(kept)
    return jnp.concatenate(out, axis=0)


def kernel(
    orb_hbm, piv_hbm, factor_ref, diag_ref, peak_ref,
    pivots, orb, gathered, pv, a0, r0, r1, a2, r2, picked, far, sums_out, sums_in, words_out, words_in, own,
    norm_out, norm_in, own_squares, norm_own, pack, unpack, gram, low, inv, peak_buf, local_sem, send_sem, recv_sem,
):
    x = lax.axis_index("grid_0")
    z = lax.axis_index("grid_1")
    core = lax.axis_index("grid_2")
    me = lax.axis_index("orb")
    right, left, across = lax.rem(me + 1, 4), lax.rem(me + 3, 4), lax.rem(me + 2, 4)
    other = 1 - core

    barrier = pltpu.get_barrier_semaphore()
    for axis, count, index in (("orb", 4, me), ("grid_0", 4, x), ("grid_1", 4, z), ("grid_2", 2, core)):
        for d in range(1, count):
            there = {axis: lax.rem(index + d, count)}
            pl.semaphore_signal(barrier, inc=1, device_id=there, device_id_type=MESH)

    def owner_at(i):
        return lax.rem(me + 2 + i, 4)

    def load(part):
        return pltpu.make_async_copy(
            orb_hbm.at[:, pl.ds(pl.multiple_of(part * PART, PART), PART)], orb.at[part], local_sem.at[lax.div(part, 2)]
        )

    def loaded(owner):
        pair = orb.at[pl.ds(2 * owner, 2)]
        pltpu.make_async_copy(pair, pair, local_sem.at[owner]).wait()

    load_pivots = pltpu.make_async_copy(piv_hbm, pivots, local_sem.at[4])
    load_pivots.start()
    for i in range(4):
        load(2 * owner_at(i)).start()
        load(2 * owner_at(i) + 1).start()

    def remote(src, dst, slot, where):
        return pltpu.make_async_remote_copy(
            src_ref=src, dst_ref=dst, send_sem=send_sem.at[slot], recv_sem=recv_sem.at[slot],
            device_id=where, device_id_type=MESH,
        )

    def go(src, dst, slot, where):
        remote(src, dst, slot, where).start()

    unsent = []

    def arrived(slot, size):
        pltpu.make_async_copy(size, size, recv_sem.at[slot]).wait()
        unsent.append((slot, size))

    def sent():
        for slot, size in unsent:
            pltpu.make_async_copy(size, size, send_sem.at[slot]).wait()
        unsent.clear()

    base = ((x * 4 + z) * 2 + core) * ROWS
    gathered[...] = jnp.zeros_like(gathered)
    load_pivots.wait()
    square = (PIV, PIV)
    eye = lax.broadcasted_iota(jnp.int32, square, 0) == lax.broadcasted_iota(jnp.int32, square, 1)
    here = jnp.concatenate(
        [
            jnp.sum(
                jnp.where(eye, jnp.broadcast_to(pivots[s : s + 1].astype(jnp.float32), square), 0.0),
                axis=1, keepdims=True,
            )
            for s in range(STEPS)
        ],
        axis=0,
    ).astype(jnp.int32) - base

    def extract(i, carry):
        owner = owner_at(i)
        loaded(owner)
        for part in (2 * owner, 2 * owner + 1):
            spots = lax.broadcasted_iota(jnp.int32, (RANK, PART), 1) + part * PART
            chosen = jnp.where(spots == here, 1.0, 0.0).astype(jnp.bfloat16)
            gathered[:, 0:DEPTH] += nt(chosen, orb[part])
        return carry

    extract(0, 0)
    pl.semaphore_wait(barrier, 10)

    def far_copies(low, high):
        start = pl.multiple_of(across * SHARE, SHARE)
        span = slice(low, high)
        go(orb_hbm.at[:, pl.ds(start + low, high - low)], far.at[0, :, span], FAR, {"orb": left})
        go(orb_hbm.at[:, pl.ds(start + PART + low, high - low)], far.at[1, :, span], FAR, {"orb": right})

    far_copies(0, FIRST)
    lax.fori_loop(1, 4, extract, 0)
    for h in range(2):
        for lane in range(4):
            for s in range(STEPS):
                a0[h, lane, s] = gathered[
                    s * PIV + h * HALF : s * PIV + (h + 1) * HALF, lane * 128 : (lane + 1) * 128
                ].astype(jnp.bfloat16)

    go(a0.at[other], r0, CORE_A, {"grid_2": other})
    arrived(CORE_A, r0)
    r0[...] = (r0[...].astype(jnp.float32) + a0[core].astype(jnp.float32)).astype(jnp.bfloat16)
    for d in (1, 2, 3):
        there = lax.rem(x + d, 4)
        go(r0.at[there], r1.at[d - 1], X_A, {"grid_0": there})
    arrived(X_A, r1)
    total = r0[x].astype(jnp.float32)
    for d in range(3):
        total += r1[d].astype(jnp.float32)
    a2[0:STEPS] = total.astype(jnp.bfloat16)
    a2[STEPS] = jnp.zeros((HALF, 128), jnp.bfloat16)
    for d in (1, 2, 3):
        there = lax.rem(z + d, 4)
        go(a2.at[there], r2.at[d - 1], Z_A, {"grid_1": there})
    arrived(Z_A, r2)
    total = a2[z].astype(jnp.float32)
    for d in range(3):
        total += r2[d].astype(jnp.float32)
    pv[core, x, z, 0] = total.astype(jnp.bfloat16)
    mine = pv.at[core, x, z, 0]
    for d in (1, 2, 3):
        go(mine, pv.at[core, x, z, 4 - d], Y_A, {"orb": lax.rem(me + d, 4)})
    far_copies(FIRST, PART)

    for d in (1, 2, 3):
        go(mine, mine, X_O, {"grid_0": lax.rem(x + d, 4)})

    def squares(values):
        wide = values.astype(jnp.float32)
        return jnp.sum(wide * wide, axis=0, keepdims=True)

    def near_norms(t, carry):
        span = pl.ds(pl.multiple_of(t * PIECE, PIECE), PIECE)
        after = pl.ds(pl.multiple_of(PART + t * PIECE, PIECE), PIECE)
        for h, owned in enumerate((2 * left + 1, 2 * right)):
            norm_out[h, :, after] = squares(orb[owned, :, span])
        return carry

    lax.fori_loop(0, PIECES, near_norms, 0)
    arrived(X_O, r2)
    mine = pv.at[core, :, z, 0]
    for d in (1, 2, 3):
        go(mine, mine, Z_O, {"grid_1": lax.rem(z + d, 4)})
    arrived(Z_O, a0.at[0])
    mine = pv.at[core, :, 0:STEPS, 0]
    go(mine, mine, CORE_O, {"grid_2": other})
    arrived(CORE_O, pv.at[0, :, 0:STEPS, 0])

    def pick(y):
        for h in range(2):
            for lane in range(4):
                for s in range(STEPS):
                    picked[y, s * PIV + h * HALF : s * PIV + (h + 1) * HALF, lane * 128 : (lane + 1) * 128] = (
                        pv[h, lane, s, y]
                    )
        wide = picked[y].astype(jnp.float32)
        norm_own[y] = jnp.broadcast_to(jnp.sum(wide * wide, axis=1, keepdims=True), (RANK, PIECE))

    pick(0)
    pack[2] = lax.rsqrt(jnp.maximum(norm_own[0], TINY)) * SCALE

    def encode(product, scale, squared):
        whole = jnp.round(product * scale * lax.rsqrt(jnp.maximum(squared, TINY))).astype(jnp.int32)
        blocks = [whole[i * BLOCK : (i + 1) * BLOCK] for i in range(VALUES)]
        words = [block & ((1 << FIELD) - 1) for block in blocks[:FIELDS]]
        cut = VALUES - FIELDS
        for k, block in enumerate(blocks[FIELDS:]):
            words[k] = words[k] | (block << FIELD)
            top = (block >> SPARE) & ((1 << REST) - 1)
            words[cut + k // 2] = words[cut + k // 2] | (top << (FIELD + REST * (k % 2)))
        return jnp.concatenate(words, axis=0)

    def near_products(t, carry):
        span = pl.ds(pl.multiple_of(t * PIECE, PIECE), PIECE)
        after = pl.ds(pl.multiple_of(PART + t * PIECE, PIECE), PIECE)
        for h, (owned, where) in enumerate(((2 * left + 1, left), (2 * right, right))):
            product = nn(picked[0, :, 0:DEPTH], orb[owned, :, span])
            words_out[h, t] = encode(product, pack[2], norm_out[h, :, after])
            go(words_out.at[h, t], words_in.at[h, t], NEAR, {"orb": where})
        return carry

    lax.fori_loop(0, PIECES, near_products, 0)

    arrived(Y_A, r2)
    for d in (1, 2, 3):
        mine = pv.at[core, x, z, 1:2]
        go(mine, mine, B, {"grid_0": lax.rem(x + d, 4)})
        mine = pv.at[core, x, z, 2:4]
        go(mine, mine, B, {"grid_1": lax.rem(z + d, 4)})
    arrived(B, a0.at[0, 0:3])
    for d in (1, 2, 3):
        mine = pv.at[core, :, z, 1:2]
        go(mine, mine, Z_C, {"grid_1": lax.rem(z + d, 4)})
        mine = pv.at[core, x, 0:STEPS, 2:4]
        go(mine, mine, X_C, {"grid_0": lax.rem(x + d, 4)})

    arrived(FAR, far)

    def norms(t, carry):
        span = pl.ds(pl.multiple_of(t * PIECE, PIECE), PIECE)
        for h, owned in enumerate((2 * left, 2 * right + 1)):
            norm_out[h, :, span] = squares(orb[owned, :, span]) + squares(far[h, :, span])
        return carry

    lax.fori_loop(0, PIECES, norms, 0)
    go(norm_out.at[0], norm_in.at[0], NORM, {"orb": left})
    go(norm_out.at[1], norm_in.at[1], NORM, {"orb": right})
    arrived(Z_C, a0.at[0])
    arrived(X_C, pv.at[0, 0:3, 0:3, 0:2])
    mine = pv.at[core, :, 0:STEPS, 1:4]
    go(mine, mine, CORE_B, {"grid_2": other})
    arrived(CORE_B, pv.at[0, :, 0:STEPS, 1:4])
    for y in range(1, 4):
        pick(y)

    def size_of(squared):
        bounded = jnp.maximum(squared, TINY)
        return bounded * lax.rsqrt(bounded)

    for h, beside in enumerate((1, 3)):
        pack[h] = lax.rsqrt(jnp.maximum(norm_own[0] + norm_own[beside], TINY)) * SCALE
        unpack[h] = size_of(norm_own[beside] + norm_own[2]) * (1.0 / SCALE)
        unpack[2 + h] = size_of(norm_own[beside]) * (1.0 / SCALE)

    def decode(packed, scale, squared):
        words = [packed[i * BLOCK : (i + 1) * BLOCK] for i in range(FIELDS)]
        blocks = [(word << SPARE) >> SPARE for word in words]
        cut = VALUES - FIELDS
        for k in range(cut):
            top = (words[cut + k // 2] << (SPARE - REST * (k % 2 + 1))) >> (32 - REST)
            blocks.append((top << SPARE) | lax.shift_right_logical(words[k], FIELD))
        return jnp.concatenate(blocks, axis=0).astype(jnp.float32) * scale * size_of(squared)

    def send_sums(t, span, slot):
        for h, where in enumerate((left, right)):
            go(sums_out.at[h, t, :, span], sums_in.at[h, t, :, span], slot, {"orb": where})

    halves = (slice(0, 128), slice(128, 256))

    def middle(t, carry):
        span = pl.ds(pl.multiple_of(t * PIECE, PIECE), PIECE)
        for h, (own, source) in enumerate(((2 * left, 1), (2 * right + 1, 3))):
            a = orb[own, :, span]
            b = far[h, :, span]
            product = nn(picked[0, :, 0:DEPTH], a) + nn(picked[source, :, 0:DEPTH], b)
            sums_out[h, t] = encode(product, pack[h], norm_out[h, :, span])

        @pl.when(t < PIECES - 1)
        def _():
            send_sums(t, slice(0, PIECE), SUM + t)

        return carry

    lax.fori_loop(0, PIECES, middle, 0)
    for half in range(2):
        send_sums(PIECES - 1, halves[half], LAST + half)

    pairs = nt(picked[0], picked[0])
    for y in range(1, 4):
        pairs += nt(picked[y], picked[y])
    block = jnp.square(pairs * (1.0 / ORB))
    for i in range(STEPS):
        for j in range(i + 1):
            gram[3 * i + j] = block[i * PIV : (i + 1) * PIV, j * PIV : (j + 1) * PIV]

    def diagonal_inverse(i, carry):
        def update(k, carry):
            gram[4 * i] -= nt(low[3 * i + k], low[3 * i + k], HIGHEST)
            return carry

        lax.fori_loop(0, i, update, 0)
        inv[4 * i] = inverse_factor(gram[4 * i])

        def panel(j, carry):
            def update(k, carry):
                gram[3 * j + i] -= nt(low[3 * j + k], low[3 * i + k], HIGHEST)
                return carry

            lax.fori_loop(0, i, update, 0)
            low[3 * j + i] = nt(gram[3 * j + i], inv[4 * i], HIGHEST)
            return carry

        lax.fori_loop(i + 1, STEPS, panel, 0)
        return carry

    lax.fori_loop(0, STEPS, diagonal_inverse, 0)
    inv[3] = -nn(inv[4], nn(low[3], inv[0], HIGHEST), HIGHEST)
    inv[7] = -nn(inv[8], nn(low[7], inv[4], HIGHEST), HIGHEST)
    inv[6] = -nn(inv[8], nn(low[6], inv[0], HIGHEST) + nn(low[7], inv[3], HIGHEST), HIGHEST)

    arrived(NORM, norm_in)

    def own_and_coded(t, carry):
        span = pl.ds(pl.multiple_of(t * PIECE, PIECE), PIECE)
        after = pl.ds(pl.multiple_of(PART + t * PIECE, PIECE), PIECE)
        for h in range(2):
            a = orb[2 * me + h, :, span]
            squared = norm_in[1 - h, :, after]
            coded = decode(words_in[1 - h, t], unpack[3 - h], squared)
            own[h, t] = nn(picked[0, :, 0:DEPTH], a) + coded
            own_squares[h, :, span] = squares(a) + squared
        return carry

    arrived(NEAR, words_in)
    lax.fori_loop(0, PIECES, own_and_coded, 0)

    def finish(t, low, width, best):
        best = list(best)
        for h in range(2):
            start = t * PIECE + low
            span = pl.ds(pl.multiple_of(start, 128), width)
            out = pl.ds(pl.multiple_of(h * PART + start, 128), width)
            inside = slice(low, low + width)
            norm = norm_in[h, :, span]
            received = decode(sums_in[h, t, :, inside], unpack[h, :, 0:width], norm)
            columns = jnp.square((received + own[h, t, :, inside]) * (1.0 / ORB))
            rest = jnp.square((norm + own_squares[h, :, span]) * (1.0 / ORB))
            for i in range(STEPS):
                fresh = nn(inv[3 * i], columns[0:PIV], HIGHEST)
                for j in range(1, i + 1):
                    fresh += nn(inv[3 * i + j], columns[j * PIV : (j + 1) * PIV], HIGHEST)
                factor_ref[i * PIV : (i + 1) * PIV, out] = fresh
                rest -= jnp.sum(fresh * fresh, axis=0, keepdims=True)
                for at in range(0, width, 128):
                    best[i] = jnp.maximum(best[i], rest[:, at : at + 128])
            diag_ref[:, out] = rest
        return tuple(best)

    def whole_piece(t, best):
        size = sums_in.at[:, t]
        pltpu.make_async_copy(size, size, recv_sem.at[SUM + t]).wait()
        return finish(t, 0, PIECE, best)

    best = (jnp.full((1, 128), -jnp.inf, jnp.float32),) * STEPS
    best = lax.fori_loop(0, PIECES - 1, whole_piece, best)
    for half in range(2):
        arrived(LAST + half, sums_in.at[:, PIECES - 1, :, halves[half]])
        best = finish(PIECES - 1, half * 128, 128, best)
    lanes = lax.broadcasted_iota(jnp.int32, (1, 128), 1)
    peak = jnp.full((1, 128), -jnp.inf, jnp.float32)
    for i in range(STEPS):
        peak = jnp.where(lanes == i, jnp.max(best[i], axis=1, keepdims=True), peak)

    unsent.extend((SUM + t, sums_in.at[:, t]) for t in range(PIECES - 1))

    peak_buf[0] = peak
    shifts = [(dx, dz, dy, dc) for dx in range(4) for dz in range(4) for dy in range(4) for dc in range(2)]
    shifts.sort(key=lambda shift: -sum(min(step, 4 - step) for step in shift[:3]))
    for shift in shifts:
        if not any(shift):
            continue
        slot = ((shift[0] * 4 + shift[1]) * 4 + shift[2]) * 2 + shift[3]
        there = {
            "grid_0": lax.rem(x + shift[0], 4),
            "grid_1": lax.rem(z + shift[1], 4),
            "orb": lax.rem(me + shift[2], 4),
            "grid_2": lax.rem(core + shift[3], 2),
        }
        go(peak_buf.at[0], peak_buf.at[slot], PEAK_A, there)
    sent()
    arrived(PEAK_A, peak_buf.at[1:128])
    sent()
    peak_ref[...] = jnp.max(peak_buf[...], axis=0)


def hand_over(factor, diagonal, peaks, factor_out, diagonal_out, peaks_out, diagonal_flat, peaks_flat, sem):
    strip = RANK // STRIPS
    copies = []
    for i in range(STRIPS):
        rows = slice(i * strip, (i + 1) * strip)
        copies.append(pltpu.make_async_copy(factor.at[rows], factor_out.at[rows], sem.at[i]))
        copies[-1].start()
    diagonal_flat[...] = diagonal[...].reshape(SHARE)
    peaks_flat[...] = peaks[0, 0:STEPS]
    for src, dst in ((diagonal_flat, diagonal_out), (peaks_flat, peaks_out)):
        copies.append(pltpu.make_async_copy(src, dst, sem.at[len(copies)]))
        copies[-1].start()
    for copy in copies:
        copy.wait()


def on_device(orbitals, pivots):
    f32, bf16 = jnp.float32, jnp.bfloat16
    vmem = pl.BlockSpec(memory_space=pltpu.VMEM)
    factor, diagonal, peaks = pl.pallas_call(
        kernel,
        out_shape=(
            jax.ShapeDtypeStruct((RANK, SHARE), f32),
            jax.ShapeDtypeStruct((1, SHARE), f32),
            jax.ShapeDtypeStruct((1, 128), f32),
        ),
        in_specs=[pl.BlockSpec(memory_space=pltpu.HBM)] * 2,
        out_specs=(vmem, vmem, vmem),
        scratch_shapes=[
            pltpu.VMEM((STEPS, PIV), jnp.int32),
            pltpu.VMEM((ROWS // PART, DEPTH, PART), bf16),
            pltpu.VMEM((RANK, WIDE), f32),
            pltpu.VMEM((2, 4, 4, 4, HALF, 128), bf16),
            pltpu.VMEM((2, 4, STEPS, HALF, 128), bf16),
            pltpu.VMEM((4, STEPS, HALF, 128), bf16),
            pltpu.VMEM((3, STEPS, HALF, 128), bf16),
            pltpu.VMEM((4, HALF, 128), bf16),
            pltpu.VMEM((3, HALF, 128), bf16),
            pltpu.VMEM((4, RANK, WIDE), bf16),
            pltpu.VMEM((2, DEPTH, PART), bf16),
            pltpu.VMEM((2, PIECES, WORDS, PIECE), jnp.int32),
            pltpu.VMEM((2, PIECES, WORDS, PIECE), jnp.int32),
            pltpu.VMEM((2, PIECES, WORDS, PIECE), jnp.int32),
            pltpu.VMEM((2, PIECES, WORDS, PIECE), jnp.int32),
            pltpu.VMEM((2, PIECES, RANK, PIECE), f32),
            pltpu.VMEM((2, 1, 2 * PART), f32),
            pltpu.VMEM((2, 1, 2 * PART), f32),
            pltpu.VMEM((2, 1, PART), f32),
            pltpu.VMEM((4, RANK, PIECE), f32),
            pltpu.VMEM((3, RANK, PIECE), f32),
            pltpu.VMEM((4, RANK, PIECE), f32),
            pltpu.VMEM((9, PIV, PIV), f32),
            pltpu.VMEM((9, PIV, PIV), f32),
            pltpu.VMEM((9, PIV, PIV), f32),
            pltpu.VMEM((128, 1, 128), f32),
            pltpu.SemaphoreType.DMA((5,)),
            pltpu.SemaphoreType.DMA((SLOTS,)),
            pltpu.SemaphoreType.DMA((SLOTS,)),
        ],
        compiler_params=pltpu.CompilerParams(
            collective_id=0, has_side_effects=True, vmem_limit_bytes=50 * 1024 * 1024
        ),
    )(orbitals, pltpu.with_memory_space_constraint(pivots, pltpu.HBM))
    factor, diagonal, peaks = pl.pallas_call(
        hand_over,
        out_shape=(
            jax.ShapeDtypeStruct((RANK, SHARE), f32),
            jax.ShapeDtypeStruct((SHARE,), f32),
            jax.ShapeDtypeStruct((STEPS,), f32),
        ),
        in_specs=[vmem] * 3,
        out_specs=(pl.BlockSpec(memory_space=pltpu.HBM),) * 3,
        scratch_shapes=[pltpu.VMEM((SHARE,), f32), pltpu.VMEM((STEPS,), f32), pltpu.SemaphoreType.DMA((STRIPS + 2,))],
        compiler_params=pltpu.CompilerParams(vmem_limit_bytes=4 * 1024 * 1024),
    )(factor, diagonal, peaks)
    return factor.T, diagonal, peaks


def solution(mesh):
    split = Mesh(
        mesh.devices.reshape(4, 4, 2, mesh.shape["orb"]), ("grid_0", "grid_1", "grid_2", "orb")
    )
    return jax.shard_map(
        on_device,
        mesh=split,
        in_specs=(P("orb", GRID), P()),
        out_specs=(P(GRID_ORB, None), P(GRID_ORB), P()),
        check_vma=False,
    )
```

```python
import functools

import jax
import jax.numpy as jnp
from jax import lax
from jax.experimental import pallas as pl
from jax.experimental.pallas import tpu as pltpu
from jax.sharding import Mesh
from jax.sharding import PartitionSpec as P

ORB = 1800
GRID = ("grid_0", "grid_1", "grid_2")
GRID_ORB = ("grid_0", "grid_1", "grid_2", "orb")
MESH = pl.DeviceIdType.MESH
HIGHEST = lax.Precision.HIGHEST

STEPS = 3
PIV = 96
RANK = STEPS * PIV
HALF = PIV // 2
DEPTH = 450
WIDE = 512
ROWS = 8192
SHARE = 2048
PART = 1024
PIECE = 256
PIECES = PART // PIECE
BLOCK = 16
VALUES, FIELDS = 18, 11
WORDS = FIELDS * BLOCK
STRIPS = 4
FIELD = 19
SPARE = 32 - FIELD
REST = FIELD - SPARE
SCALE = float(2 ** (FIELD - 1) - 16)
TINY = 1e-30

FIRST = 768

CORE_A, X_A, Z_A, Y_A, X_O, Z_O, CORE_O, B, X_C, Z_C, CORE_B, FAR, NEAR, NORM, SUM = range(15)
LAST = SUM + PIECES - 1
PEAK_A = LAST + 2
SLOTS = LAST + 3


def nt(left, right, precision=None):
    return lax.dot_general(
        left, right, (((1,), (1,)), ((), ())), precision=precision,
        preferred_element_type=jnp.float32,
    )


def nn(left, right, precision=None):
    return lax.dot_general(
        left, right, (((1,), (0,)), ((), ())), precision=precision,
        preferred_element_type=jnp.float32,
    )


def inverse_factor(block):
    lanes = lax.broadcasted_iota(jnp.int32, (8, PIV), 1)
    subs = lax.broadcasted_iota(jnp.int32, (8, PIV), 0)
    groups = PIV // 8
    left = [block[8 * g : 8 * g + 8, :] for g in range(groups)]
    right = [jnp.where(lanes == subs + 8 * g, 1.0, 0.0) for g in range(groups)]

    def row(values, r):
        return jnp.broadcast_to(values[r : r + 1, :], (8, PIV))

    out = []
    for home in range(groups):
        column = {
            (g, j): jnp.broadcast_to(left[g][:, 8 * home + j : 8 * home + j + 1], (8, PIV))
            for g in range(home, groups)
            for j in range(8)
        }
        kept = right[home]
        for r in range(8):
            scale = lax.rsqrt(row(column[home, r], r))
            spread = [row(column[home, r], j) * scale for j in range(r + 1, 8)]
            row_left = row(left[home], r) * scale
            row_right = row(right[home], r) * scale
            kept = jnp.where(subs == r, row_right, kept)
            for g in range(home, groups):
                times = column[g, r] * scale
                if g == home:
                    times = jnp.where(subs > r, times, 0.0)
                left[g] = left[g] - times * row_left
                right[g] = right[g] - times * row_right
                for j in range(r + 1, 8):
                    column[g, j] = column[g, j] - times * spread[j - r - 1]
        out.append(kept)
    return jnp.concatenate(out, axis=0)


def kernel(
    orb_hbm, piv_hbm, factor_ref, diag_ref, peak_ref,
    pivots, orb, gathered, pv, a0, r0, r1, a2, r2, picked, far, sums_out, sums_in, words_out, words_in, own,
    norm_out, norm_in, own_squares, norm_own, pack, unpack, gram, low, inv, peak_buf, local_sem, send_sem, recv_sem,
):
    x = lax.axis_index("grid_0")
    z = lax.axis_index("grid_1")
    core = lax.axis_index("grid_2")
    me = lax.axis_index("orb")
    right, left, across = lax.rem(me + 1, 4), lax.rem(me + 3, 4), lax.rem(me + 2, 4)
    other = 1 - core

    barrier = pltpu.get_barrier_semaphore()
    for axis, count, index in (("orb", 4, me), ("grid_0", 4, x), ("grid_1", 4, z), ("grid_2", 2, core)):
        for d in range(1, count):
            there = {axis: lax.rem(index + d, count)}
            pl.semaphore_signal(barrier, inc=1, device_id=there, device_id_type=MESH)

    def owner_at(i):
        return lax.rem(me + 2 + i, 4)

    def load(part):
        return pltpu.make_async_copy(
            orb_hbm.at[:, pl.ds(pl.multiple_of(part * PART, PART), PART)], orb.at[part], local_sem.at[lax.div(part, 2)]
        )

    def loaded(owner):
        pair = orb.at[pl.ds(2 * owner, 2)]
        pltpu.make_async_copy(pair, pair, local_sem.at[owner]).wait()

    load_pivots = pltpu.make_async_copy(piv_hbm, pivots, local_sem.at[4])
    load_pivots.start()
    for i in range(4):
        load(2 * owner_at(i)).start()
        load(2 * owner_at(i) + 1).start()

    def remote(src, dst, slot, where):
        return pltpu.make_async_remote_copy(
            src_ref=src, dst_ref=dst, send_sem=send_sem.at[slot], recv_sem=recv_sem.at[slot],
            device_id=where, device_id_type=MESH,
        )

    def go(src, dst, slot, where):
        remote(src, dst, slot, where).start()

    unsent = []

    def arrived(slot, size):
        pltpu.make_async_copy(size, size, recv_sem.at[slot]).wait()
        unsent.append((slot, size))

    def sent():
        for slot, size in unsent:
            pltpu.make_async_copy(size, size, send_sem.at[slot]).wait()
        unsent.clear()

    pl.semaphore_wait(barrier, 10)

    def far_copies(low, high):
        start = pl.multiple_of(across * SHARE, SHARE)
        span = slice(low, high)
        go(orb_hbm.at[:, pl.ds(start + low, high - low)], far.at[0, :, span], FAR, {"orb": left})
        go(orb_hbm.at[:, pl.ds(start + PART + low, high - low)], far.at[1, :, span], FAR, {"orb": right})

    far_copies(0, FIRST)

    base = ((x * 4 + z) * 2 + core) * ROWS
    gathered[...] = jnp.zeros_like(gathered)
    load_pivots.wait()
    square = (PIV, PIV)
    eye = lax.broadcasted_iota(jnp.int32, square, 0) == lax.broadcasted_iota(jnp.int32, square, 1)
    here = jnp.concatenate(
        [
            jnp.sum(
                jnp.where(eye, jnp.broadcast_to(pivots[s : s + 1].astype(jnp.float32), square), 0.0),
                axis=1, keepdims=True,
            )
            for s in range(STEPS)
        ],
        axis=0,
    ).astype(jnp.int32) - base

    def extract(i, carry):
        owner = owner_at(i)
        loaded(owner)
        for part in (2 * owner, 2 * owner + 1):
            spots = lax.broadcasted_iota(jnp.int32, (RANK, PART), 1) + part * PART
            chosen = jnp.where(spots == here, 1.0, 0.0).astype(jnp.bfloat16)
            gathered[:, 0:DEPTH] += nt(chosen, orb[part])
        return carry

    lax.fori_loop(0, 4, extract, 0)
    for h in range(2):
        for lane in range(4):
            for s in range(STEPS):
                a0[h, lane, s] = gathered[
                    s * PIV + h * HALF : s * PIV + (h + 1) * HALF, lane * 128 : (lane + 1) * 128
                ].astype(jnp.bfloat16)

    go(a0.at[other], r0, CORE_A, {"grid_2": other})
    arrived(CORE_A, r0)
    r0[...] = (r0[...].astype(jnp.float32) + a0[core].astype(jnp.float32)).astype(jnp.bfloat16)
    for d in (1, 2, 3):
        there = lax.rem(x + d, 4)
        go(r0.at[there], r1.at[d - 1], X_A, {"grid_0": there})
    arrived(X_A, r1)
    total = r0[x].astype(jnp.float32)
    for d in range(3):
        total += r1[d].astype(jnp.float32)
    a2[0:STEPS] = total.astype(jnp.bfloat16)
    a2[STEPS] = jnp.zeros((HALF, 128), jnp.bfloat16)
    for d in (1, 2, 3):
        there = lax.rem(z + d, 4)
        go(a2.at[there], r2.at[d - 1], Z_A, {"grid_1": there})
    arrived(Z_A, r2)
    total = a2[z].astype(jnp.float32)
    for d in range(3):
        total += r2[d].astype(jnp.float32)
    pv[core, x, z, 0] = total.astype(jnp.bfloat16)
    mine = pv.at[core, x, z, 0]
    for d in (1, 2, 3):
        go(mine, pv.at[core, x, z, 4 - d], Y_A, {"orb": lax.rem(me + d, 4)})
    far_copies(FIRST, PART)

    for d in (1, 2, 3):
        go(mine, mine, X_O, {"grid_0": lax.rem(x + d, 4)})

    def squares(values):
        wide = values.astype(jnp.float32)
        return jnp.sum(wide * wide, axis=0, keepdims=True)

    def near_norms(t, carry):
        span = pl.ds(pl.multiple_of(t * PIECE, PIECE), PIECE)
        after = pl.ds(pl.multiple_of(PART + t * PIECE, PIECE), PIECE)
        for h, owned in enumerate((2 * left + 1, 2 * right)):
            norm_out[h, :, after] = squares(orb[owned, :, span])
        return carry

    lax.fori_loop(0, PIECES, near_norms, 0)
    arrived(X_O, r2)
    mine = pv.at[core, :, z, 0]
    for d in (1, 2, 3):
        go(mine, mine, Z_O, {"grid_1": lax.rem(z + d, 4)})
    arrived(Z_O, a0.at[0])
    mine = pv.at[core, :, 0:STEPS, 0]
    go(mine, mine, CORE_O, {"grid_2": other})
    arrived(CORE_O, pv.at[0, :, 0:STEPS, 0])

    arrived(Y_A, r2)
    for d in (1, 2, 3):
        mine = pv.at[core, x, z, 1:2]
        go(mine, mine, B, {"grid_0": lax.rem(x + d, 4)})
        mine = pv.at[core, x, z, 2:4]
        go(mine, mine, B, {"grid_1": lax.rem(z + d, 4)})

    def pick(y):
        for h in range(2):
            for lane in range(4):
                for s in range(STEPS):
                    picked[y, s * PIV + h * HALF : s * PIV + (h + 1) * HALF, lane * 128 : (lane + 1) * 128] = (
                        pv[h, lane, s, y]
                    )
        wide = picked[y].astype(jnp.float32)
        norm_own[y] = jnp.broadcast_to(jnp.sum(wide * wide, axis=1, keepdims=True), (RANK, PIECE))

    pick(0)
    pack[2] = lax.rsqrt(jnp.maximum(norm_own[0], TINY)) * SCALE

    def encode(product, scale, squared):
        whole = jnp.round(product * scale * lax.rsqrt(jnp.maximum(squared, TINY))).astype(jnp.int32)
        blocks = [whole[i * BLOCK : (i + 1) * BLOCK] for i in range(VALUES)]
        words = [block & ((1 << FIELD) - 1) for block in blocks[:FIELDS]]
        cut = VALUES - FIELDS
        for k, block in enumerate(blocks[FIELDS:]):
            words[k] = words[k] | (block << FIELD)
            top = (block >> SPARE) & ((1 << REST) - 1)
            words[cut + k // 2] = words[cut + k // 2] | (top << (FIELD + REST * (k % 2)))
        return jnp.concatenate(words, axis=0)

    def near_products(t, carry):
        span = pl.ds(pl.multiple_of(t * PIECE, PIECE), PIECE)
        after = pl.ds(pl.multiple_of(PART + t * PIECE, PIECE), PIECE)
        for h, (owned, where) in enumerate(((2 * left + 1, left), (2 * right, right))):
            product = nn(picked[0, :, 0:DEPTH], orb[owned, :, span])
            words_out[h, t] = encode(product, pack[2], norm_out[h, :, after])
            go(words_out.at[h, t], words_in.at[h, t], NEAR, {"orb": where})
        return carry

    lax.fori_loop(0, PIECES, near_products, 0)

    arrived(B, a0.at[0, 0:3])
    for d in (1, 2, 3):
        mine = pv.at[core, :, z, 1:2]
        go(mine, mine, Z_C, {"grid_1": lax.rem(z + d, 4)})
        mine = pv.at[core, x, 0:STEPS, 2:4]
        go(mine, mine, X_C, {"grid_0": lax.rem(x + d, 4)})

    arrived(FAR, far)

    def norms(t, carry):
        span = pl.ds(pl.multiple_of(t * PIECE, PIECE), PIECE)
        for h, owned in enumerate((2 * left, 2 * right + 1)):
            norm_out[h, :, span] = squares(orb[owned, :, span]) + squares(far[h, :, span])
        return carry

    lax.fori_loop(0, PIECES, norms, 0)
    go(norm_out.at[0], norm_in.at[0], NORM, {"orb": left})
    go(norm_out.at[1], norm_in.at[1], NORM, {"orb": right})
    arrived(Z_C, a0.at[0])
    arrived(X_C, pv.at[0, 0:3, 0:3, 0:2])
    mine = pv.at[core, :, 0:STEPS, 1:4]
    go(mine, mine, CORE_B, {"grid_2": other})
    arrived(CORE_B, pv.at[0, :, 0:STEPS, 1:4])
    for y in range(1, 4):
        pick(y)

    def size_of(squared):
        bounded = jnp.maximum(squared, TINY)
        return bounded * lax.rsqrt(bounded)

    for h, beside in enumerate((1, 3)):
        pack[h] = lax.rsqrt(jnp.maximum(norm_own[0] + norm_own[beside], TINY)) * SCALE
        unpack[h] = size_of(norm_own[beside] + norm_own[2]) * (1.0 / SCALE)
        unpack[2 + h] = size_of(norm_own[beside]) * (1.0 / SCALE)

    def decode(packed, scale, squared):
        words = [packed[i * BLOCK : (i + 1) * BLOCK] for i in range(FIELDS)]
        blocks = [(word << SPARE) >> SPARE for word in words]
        cut = VALUES - FIELDS
        for k in range(cut):
            top = (words[cut + k // 2] << (SPARE - REST * (k % 2 + 1))) >> (32 - REST)
            blocks.append((top << SPARE) | lax.shift_right_logical(words[k], FIELD))
        return jnp.concatenate(blocks, axis=0).astype(jnp.float32) * scale * size_of(squared)

    def send_sums(t, span, slot):
        for h, where in enumerate((left, right)):
            go(sums_out.at[h, t, :, span], sums_in.at[h, t, :, span], slot, {"orb": where})

    halves = (slice(0, 128), slice(128, 256))

    def middle(t, carry):
        span = pl.ds(pl.multiple_of(t * PIECE, PIECE), PIECE)
        for h, (own, source) in enumerate(((2 * left, 1), (2 * right + 1, 3))):
            a = orb[own, :, span]
            b = far[h, :, span]
            product = nn(picked[0, :, 0:DEPTH], a) + nn(picked[source, :, 0:DEPTH], b)
            sums_out[h, t] = encode(product, pack[h], norm_out[h, :, span])

        @pl.when(t < PIECES - 1)
        def _():
            send_sums(t, slice(0, PIECE), SUM + t)

        return carry

    lax.fori_loop(0, PIECES, middle, 0)
    for half in range(2):
        send_sums(PIECES - 1, halves[half], LAST + half)

    pairs = nt(picked[0], picked[0])
    for y in range(1, 4):
        pairs += nt(picked[y], picked[y])
    block = jnp.square(pairs * (1.0 / ORB))
    for i in range(STEPS):
        for j in range(i + 1):
            gram[3 * i + j] = block[i * PIV : (i + 1) * PIV, j * PIV : (j + 1) * PIV]

    def diagonal_inverse(i, carry):
        def update(k, carry):
            gram[4 * i] -= nt(low[3 * i + k], low[3 * i + k], HIGHEST)
            return carry

        lax.fori_loop(0, i, update, 0)
        inv[4 * i] = inverse_factor(gram[4 * i])

        def panel(j, carry):
            def update(k, carry):
                gram[3 * j + i] -= nt(low[3 * j + k], low[3 * i + k], HIGHEST)
                return carry

            lax.fori_loop(0, i, update, 0)
            low[3 * j + i] = nt(gram[3 * j + i], inv[4 * i], HIGHEST)
            return carry

        lax.fori_loop(i + 1, STEPS, panel, 0)
        return carry

    lax.fori_loop(0, STEPS, diagonal_inverse, 0)
    inv[3] = -nn(inv[4], nn(low[3], inv[0], HIGHEST), HIGHEST)
    inv[7] = -nn(inv[8], nn(low[7], inv[4], HIGHEST), HIGHEST)
    inv[6] = -nn(inv[8], nn(low[6], inv[0], HIGHEST) + nn(low[7], inv[3], HIGHEST), HIGHEST)

    arrived(NORM, norm_in)

    def own_and_coded(t, carry):
        span = pl.ds(pl.multiple_of(t * PIECE, PIECE), PIECE)
        after = pl.ds(pl.multiple_of(PART + t * PIECE, PIECE), PIECE)
        for h in range(2):
            a = orb[2 * me + h, :, span]
            squared = norm_in[1 - h, :, after]
            coded = decode(words_in[1 - h, t], unpack[3 - h], squared)
            own[h, t] = nn(picked[0, :, 0:DEPTH], a) + coded
            own_squares[h, :, span] = squares(a) + squared
        return carry

    arrived(NEAR, words_in)
    lax.fori_loop(0, PIECES, own_and_coded, 0)

    def finish(t, low, width, best):
        best = list(best)
        for h in range(2):
            start = t * PIECE + low
            span = pl.ds(pl.multiple_of(start, 128), width)
            out = pl.ds(pl.multiple_of(h * PART + start, 128), width)
            inside = slice(low, low + width)
            norm = norm_in[h, :, span]
            received = decode(sums_in[h, t, :, inside], unpack[h, :, 0:width], norm)
            columns = jnp.square((received + own[h, t, :, inside]) * (1.0 / ORB))
            rest = jnp.square((norm + own_squares[h, :, span]) * (1.0 / ORB))
            for i in range(STEPS):
                fresh = nn(inv[3 * i], columns[0:PIV], HIGHEST)
                for j in range(1, i + 1):
                    fresh += nn(inv[3 * i + j], columns[j * PIV : (j + 1) * PIV], HIGHEST)
                factor_ref[i * PIV : (i + 1) * PIV, out] = fresh
                rest -= jnp.sum(fresh * fresh, axis=0, keepdims=True)
                for at in range(0, width, 128):
                    best[i] = jnp.maximum(best[i], rest[:, at : at + 128])
            diag_ref[:, out] = rest
        return tuple(best)

    def whole_piece(t, best):
        size = sums_in.at[:, t]
        pltpu.make_async_copy(size, size, recv_sem.at[SUM + t]).wait()
        return finish(t, 0, PIECE, best)

    best = (jnp.full((1, 128), -jnp.inf, jnp.float32),) * STEPS
    best = lax.fori_loop(0, PIECES - 1, whole_piece, best)
    for half in range(2):
        arrived(LAST + half, sums_in.at[:, PIECES - 1, :, halves[half]])
        best = finish(PIECES - 1, half * 128, 128, best)
    lanes = lax.broadcasted_iota(jnp.int32, (1, 128), 1)
    peak = jnp.full((1, 128), -jnp.inf, jnp.float32)
    for i in range(STEPS):
        peak = jnp.where(lanes == i, jnp.max(best[i], axis=1, keepdims=True), peak)

    unsent.extend((SUM + t, sums_in.at[:, t]) for t in range(PIECES - 1))

    peak_buf[0] = peak
    shifts = [(dx, dz, dy, dc) for dx in range(4) for dz in range(4) for dy in range(4) for dc in range(2)]
    shifts.sort(key=lambda shift: -sum(min(step, 4 - step) for step in shift[:3]))
    for shift in shifts:
        if not any(shift):
            continue
        slot = ((shift[0] * 4 + shift[1]) * 4 + shift[2]) * 2 + shift[3]
        there = {
            "grid_0": lax.rem(x + shift[0], 4),
            "grid_1": lax.rem(z + shift[1], 4),
            "orb": lax.rem(me + shift[2], 4),
            "grid_2": lax.rem(core + shift[3], 2),
        }
        go(peak_buf.at[0], peak_buf.at[slot], PEAK_A, there)
    sent()
    arrived(PEAK_A, peak_buf.at[1:128])
    sent()
    peak_ref[...] = jnp.max(peak_buf[...], axis=0)


def hand_over(factor, diagonal, peaks, factor_out, diagonal_out, peaks_out, diagonal_flat, peaks_flat, sem):
    strip = RANK // STRIPS
    copies = []
    for i in range(STRIPS):
        rows = slice(i * strip, (i + 1) * strip)
        copies.append(pltpu.make_async_copy(factor.at[rows], factor_out.at[rows], sem.at[i]))
        copies[-1].start()
    diagonal_flat[...] = diagonal[...].reshape(SHARE)
    peaks_flat[...] = peaks[0, 0:STEPS]
    for src, dst in ((diagonal_flat, diagonal_out), (peaks_flat, peaks_out)):
        copies.append(pltpu.make_async_copy(src, dst, sem.at[len(copies)]))
        copies[-1].start()
    for copy in copies:
        copy.wait()


def on_device(orbitals, pivots):
    f32, bf16 = jnp.float32, jnp.bfloat16
    vmem = pl.BlockSpec(memory_space=pltpu.VMEM)
    factor, diagonal, peaks = pl.pallas_call(
        kernel,
        out_shape=(
            jax.ShapeDtypeStruct((RANK, SHARE), f32),
            jax.ShapeDtypeStruct((1, SHARE), f32),
            jax.ShapeDtypeStruct((1, 128), f32),
        ),
        in_specs=[pl.BlockSpec(memory_space=pltpu.HBM)] * 2,
        out_specs=(vmem, vmem, vmem),
        scratch_shapes=[
            pltpu.VMEM((STEPS, PIV), jnp.int32),
            pltpu.VMEM((ROWS // PART, DEPTH, PART), bf16),
            pltpu.VMEM((RANK, WIDE), f32),
            pltpu.VMEM((2, 4, 4, 4, HALF, 128), bf16),
            pltpu.VMEM((2, 4, STEPS, HALF, 128), bf16),
            pltpu.VMEM((4, STEPS, HALF, 128), bf16),
            pltpu.VMEM((3, STEPS, HALF, 128), bf16),
            pltpu.VMEM((4, HALF, 128), bf16),
            pltpu.VMEM((3, HALF, 128), bf16),
            pltpu.VMEM((4, RANK, WIDE), bf16),
            pltpu.VMEM((2, DEPTH, PART), bf16),
            pltpu.VMEM((2, PIECES, WORDS, PIECE), jnp.int32),
            pltpu.VMEM((2, PIECES, WORDS, PIECE), jnp.int32),
            pltpu.VMEM((2, PIECES, WORDS, PIECE), jnp.int32),
            pltpu.VMEM((2, PIECES, WORDS, PIECE), jnp.int32),
            pltpu.VMEM((2, PIECES, RANK, PIECE), f32),
            pltpu.VMEM((2, 1, 2 * PART), f32),
            pltpu.VMEM((2, 1, 2 * PART), f32),
            pltpu.VMEM((2, 1, PART), f32),
            pltpu.VMEM((4, RANK, PIECE), f32),
            pltpu.VMEM((3, RANK, PIECE), f32),
            pltpu.VMEM((4, RANK, PIECE), f32),
            pltpu.VMEM((9, PIV, PIV), f32),
            pltpu.VMEM((9, PIV, PIV), f32),
            pltpu.VMEM((9, PIV, PIV), f32),
            pltpu.VMEM((128, 1, 128), f32),
            pltpu.SemaphoreType.DMA((5,)),
            pltpu.SemaphoreType.DMA((SLOTS,)),
            pltpu.SemaphoreType.DMA((SLOTS,)),
        ],
        compiler_params=pltpu.CompilerParams(
            collective_id=0, has_side_effects=True, vmem_limit_bytes=50 * 1024 * 1024
        ),
    )(orbitals, pltpu.with_memory_space_constraint(pivots, pltpu.HBM))
    factor, diagonal, peaks = pl.pallas_call(
        hand_over,
        out_shape=(
            jax.ShapeDtypeStruct((RANK, SHARE), f32),
            jax.ShapeDtypeStruct((SHARE,), f32),
            jax.ShapeDtypeStruct((STEPS,), f32),
        ),
        in_specs=[vmem] * 3,
        out_specs=(pl.BlockSpec(memory_space=pltpu.HBM),) * 3,
        scratch_shapes=[pltpu.VMEM((SHARE,), f32), pltpu.VMEM((STEPS,), f32), pltpu.SemaphoreType.DMA((STRIPS + 2,))],
        compiler_params=pltpu.CompilerParams(vmem_limit_bytes=4 * 1024 * 1024),
    )(factor, diagonal, peaks)
    return factor.T, diagonal, peaks


def solution(mesh):
    split = Mesh(
        mesh.devices.reshape(4, 4, 2, mesh.shape["orb"]), ("grid_0", "grid_1", "grid_2", "orb")
    )
    return jax.shard_map(
        on_device,
        mesh=split,
        in_specs=(P("orb", GRID), P()),
        out_specs=(P(GRID_ORB, None), P(GRID_ORB), P()),
        check_vma=False,
    )
```

```python
import functools

import jax
import jax.numpy as jnp
from jax import lax
from jax.experimental import pallas as pl
from jax.experimental.pallas import tpu as pltpu
from jax.sharding import Mesh
from jax.sharding import PartitionSpec as P

ORB = 1800
GRID = ("grid_0", "grid_1", "grid_2")
GRID_ORB = ("grid_0", "grid_1", "grid_2", "orb")
MESH = pl.DeviceIdType.MESH
HIGHEST = lax.Precision.HIGHEST

STEPS = 3
PIV = 96
RANK = STEPS * PIV
HALF = PIV // 2
DEPTH = 450
WIDE = 512
ROWS = 8192
SHARE = 2048
PART = 1024
PIECE = 256
PIECES = PART // PIECE
BLOCK = 16
VALUES, FIELDS = 18, 11
WORDS = FIELDS * BLOCK
STRIPS = 4
FIELD = 19
SPARE = 32 - FIELD
REST = FIELD - SPARE
SCALE = float(2 ** (FIELD - 1) - 16)
TINY = 1e-30

FIRST = 768

CORE_A, X_A, Z_A, Y_A, X_O, Z_O, CORE_O, B, X_C, Z_C, CORE_B, FAR, NEAR, NORM, SUM = range(15)
LAST = SUM + PIECES - 1
PEAK_A = LAST + 2
SLOTS = LAST + 3


def nt(left, right, precision=None):
    return lax.dot_general(
        left, right, (((1,), (1,)), ((), ())), precision=precision,
        preferred_element_type=jnp.float32,
    )


def nn(left, right, precision=None):
    return lax.dot_general(
        left, right, (((1,), (0,)), ((), ())), precision=precision,
        preferred_element_type=jnp.float32,
    )


def inverse_factor(block):
    lanes = lax.broadcasted_iota(jnp.int32, (8, PIV), 1)
    subs = lax.broadcasted_iota(jnp.int32, (8, PIV), 0)
    groups = PIV // 8
    left = [block[8 * g : 8 * g + 8, :] for g in range(groups)]
    right = [jnp.where(lanes == subs + 8 * g, 1.0, 0.0) for g in range(groups)]

    def row(values, r):
        return jnp.broadcast_to(values[r : r + 1, :], (8, PIV))

    out = []
    for home in range(groups):
        column = {
            (g, j): jnp.broadcast_to(left[g][:, 8 * home + j : 8 * home + j + 1], (8, PIV))
            for g in range(home, groups)
            for j in range(8)
        }
        kept = right[home]
        for r in range(8):
            scale = lax.rsqrt(row(column[home, r], r))
            spread = [row(column[home, r], j) * scale for j in range(r + 1, 8)]
            row_left = row(left[home], r) * scale
            row_right = row(right[home], r) * scale
            kept = jnp.where(subs == r, row_right, kept)
            for g in range(home, groups):
                times = column[g, r] * scale
                if g == home:
                    times = jnp.where(subs > r, times, 0.0)
                left[g] = left[g] - times * row_left
                right[g] = right[g] - times * row_right
                for j in range(r + 1, 8):
                    column[g, j] = column[g, j] - times * spread[j - r - 1]
        out.append(kept)
    return jnp.concatenate(out, axis=0)


def kernel(
    orb_hbm, piv_hbm, factor_ref, diag_ref, peak_ref,
    pivots, orb, gathered, pv, a0, r0, r1, a2, r2, picked, far, sums_out, sums_in, words_out, words_in, own,
    norm_out, norm_in, own_squares, norm_own, pack, unpack, gram, low, inv, peak_buf, local_sem, send_sem, recv_sem,
):
    x = lax.axis_index("grid_0")
    z = lax.axis_index("grid_1")
    core = lax.axis_index("grid_2")
    me = lax.axis_index("orb")
    right, left, across = lax.rem(me + 1, 4), lax.rem(me + 3, 4), lax.rem(me + 2, 4)
    other = 1 - core

    barrier = pltpu.get_barrier_semaphore()
    for axis, count, index in (("orb", 4, me), ("grid_0", 4, x), ("grid_1", 4, z), ("grid_2", 2, core)):
        for d in range(1, count):
            there = {axis: lax.rem(index + d, count)}
            pl.semaphore_signal(barrier, inc=1, device_id=there, device_id_type=MESH)

    def owner_at(i):
        return lax.rem(me + 2 + i, 4)

    def load(part):
        return pltpu.make_async_copy(
            orb_hbm.at[:, pl.ds(pl.multiple_of(part * PART, PART), PART)], orb.at[part], local_sem.at[lax.div(part, 2)]
        )

    def loaded(owner):
        pair = orb.at[pl.ds(2 * owner, 2)]
        pltpu.make_async_copy(pair, pair, local_sem.at[owner]).wait()

    load_pivots = pltpu.make_async_copy(piv_hbm, pivots, local_sem.at[4])
    load_pivots.start()
    for i in range(4):
        load(2 * owner_at(i)).start()
        load(2 * owner_at(i) + 1).start()

    def remote(src, dst, slot, where):
        return pltpu.make_async_remote_copy(
            src_ref=src, dst_ref=dst, send_sem=send_sem.at[slot], recv_sem=recv_sem.at[slot],
            device_id=where, device_id_type=MESH,
        )

    def go(src, dst, slot, where):
        remote(src, dst, slot, where).start()

    unsent = []

    def arrived(slot, size):
        pltpu.make_async_copy(size, size, recv_sem.at[slot]).wait()
        unsent.append((slot, size))

    def sent():
        for slot, size in unsent:
            pltpu.make_async_copy(size, size, send_sem.at[slot]).wait()
        unsent.clear()

    pl.semaphore_wait(barrier, 10)

    def far_copies(low, high):
        start = pl.multiple_of(across * SHARE, SHARE)
        span = slice(low, high)
        go(orb_hbm.at[:, pl.ds(start + low, high - low)], far.at[0, :, span], FAR, {"orb": left})
        go(orb_hbm.at[:, pl.ds(start + PART + low, high - low)], far.at[1, :, span], FAR, {"orb": right})

    far_copies(0, FIRST)

    base = ((x * 4 + z) * 2 + core) * ROWS
    gathered[...] = jnp.zeros_like(gathered)
    load_pivots.wait()
    square = (PIV, PIV)
    eye = lax.broadcasted_iota(jnp.int32, square, 0) == lax.broadcasted_iota(jnp.int32, square, 1)
    here = jnp.concatenate(
        [
            jnp.sum(
                jnp.where(eye, jnp.broadcast_to(pivots[s : s + 1].astype(jnp.float32), square), 0.0),
                axis=1, keepdims=True,
            )
            for s in range(STEPS)
        ],
        axis=0,
    ).astype(jnp.int32) - base

    def extract(i, carry):
        owner = owner_at(i)
        loaded(owner)
        for part in (2 * owner, 2 * owner + 1):
            spots = lax.broadcasted_iota(jnp.int32, (RANK, PART), 1) + part * PART
            chosen = jnp.where(spots == here, 1.0, 0.0).astype(jnp.bfloat16)
            gathered[:, 0:DEPTH] += nt(chosen, orb[part])
        return carry

    lax.fori_loop(0, 4, extract, 0)
    for h in range(2):
        for lane in range(4):
            for s in range(STEPS):
                a0[h, lane, s] = gathered[
                    s * PIV + h * HALF : s * PIV + (h + 1) * HALF, lane * 128 : (lane + 1) * 128
                ].astype(jnp.bfloat16)

    go(a0.at[other], r0, CORE_A, {"grid_2": other})
    arrived(CORE_A, r0)
    r0[...] = (r0[...].astype(jnp.float32) + a0[core].astype(jnp.float32)).astype(jnp.bfloat16)
    for d in (1, 2, 3):
        there = lax.rem(x + d, 4)
        go(r0.at[there], r1.at[d - 1], X_A, {"grid_0": there})
    arrived(X_A, r1)
    total = r0[x].astype(jnp.float32)
    for d in range(3):
        total += r1[d].astype(jnp.float32)
    a2[0:STEPS] = total.astype(jnp.bfloat16)
    a2[STEPS] = jnp.zeros((HALF, 128), jnp.bfloat16)
    for d in (1, 2, 3):
        there = lax.rem(z + d, 4)
        go(a2.at[there], r2.at[d - 1], Z_A, {"grid_1": there})
    arrived(Z_A, r2)
    total = a2[z].astype(jnp.float32)
    for d in range(3):
        total += r2[d].astype(jnp.float32)
    pv[core, x, z, 0] = total.astype(jnp.bfloat16)
    mine = pv.at[core, x, z, 0]
    for d in (1, 2, 3):
        go(mine, pv.at[core, x, z, 4 - d], Y_A, {"orb": lax.rem(me + d, 4)})
    far_copies(FIRST, PART)

    for d in (1, 2, 3):
        go(mine, mine, X_O, {"grid_0": lax.rem(x + d, 4)})

    def squares(values):
        wide = values.astype(jnp.float32)
        return jnp.sum(wide * wide, axis=0, keepdims=True)

    def near_norms(t, carry):
        span = pl.ds(pl.multiple_of(t * PIECE, PIECE), PIECE)
        after = pl.ds(pl.multiple_of(PART + t * PIECE, PIECE), PIECE)
        for h, owned in enumerate((2 * left + 1, 2 * right)):
            norm_out[h, :, after] = squares(orb[owned, :, span])
        return carry

    lax.fori_loop(0, PIECES, near_norms, 0)
    arrived(X_O, r2)
    mine = pv.at[core, :, z, 0]
    for d in (1, 2, 3):
        go(mine, mine, Z_O, {"grid_1": lax.rem(z + d, 4)})
    arrived(Z_O, a0.at[0])
    mine = pv.at[core, :, 0:STEPS, 0]
    go(mine, mine, CORE_O, {"grid_2": other})
    arrived(CORE_O, pv.at[0, :, 0:STEPS, 0])

    arrived(Y_A, r2)
    for d in (1, 2, 3):
        mine = pv.at[core, x, z, 1:2]
        go(mine, mine, B, {"grid_0": lax.rem(x + d, 4)})
        mine = pv.at[core, x, z, 2:4]
        go(mine, mine, B, {"grid_1": lax.rem(z + d, 4)})

    def pick(y):
        for h in range(2):
            for lane in range(4):
                for s in range(STEPS):
                    picked[y, s * PIV + h * HALF : s * PIV + (h + 1) * HALF, lane * 128 : (lane + 1) * 128] = (
                        pv[h, lane, s, y]
                    )
        wide = picked[y].astype(jnp.float32)
        norm_own[y] = jnp.broadcast_to(jnp.sum(wide * wide, axis=1, keepdims=True), (RANK, PIECE))

    pick(0)
    pack[2] = lax.rsqrt(jnp.maximum(norm_own[0], TINY)) * SCALE

    def encode(product, scale, squared):
        whole = jnp.round(product * scale * lax.rsqrt(jnp.maximum(squared, TINY))).astype(jnp.int32)
        blocks = [whole[i * BLOCK : (i + 1) * BLOCK] for i in range(VALUES)]
        words = [block & ((1 << FIELD) - 1) for block in blocks[:FIELDS]]
        cut = VALUES - FIELDS
        for k, block in enumerate(blocks[FIELDS:]):
            words[k] = words[k] | (block << FIELD)
            top = (block >> SPARE) & ((1 << REST) - 1)
            words[cut + k // 2] = words[cut + k // 2] | (top << (FIELD + REST * (k % 2)))
        return jnp.concatenate(words, axis=0)

    def near_products(t, carry):
        span = pl.ds(pl.multiple_of(t * PIECE, PIECE), PIECE)
        after = pl.ds(pl.multiple_of(PART + t * PIECE, PIECE), PIECE)
        for h, (owned, where) in enumerate(((2 * left + 1, left), (2 * right, right))):
            product = nn(picked[0, :, 0:DEPTH], orb[owned, :, span])
            words_out[h, t] = encode(product, pack[2], norm_out[h, :, after])
            go(words_out.at[h, t], words_in.at[h, t], NEAR, {"orb": where})
        return carry

    lax.fori_loop(0, PIECES, near_products, 0)

    arrived(B, a0.at[0, 0:3])
    for d in (1, 2, 3):
        mine = pv.at[core, :, z, 1:2]
        go(mine, mine, Z_C, {"grid_1": lax.rem(z + d, 4)})
        mine = pv.at[core, x, 0:STEPS, 2:4]
        go(mine, mine, X_C, {"grid_0": lax.rem(x + d, 4)})

    arrived(FAR, far)

    def norms(t, carry):
        span = pl.ds(pl.multiple_of(t * PIECE, PIECE), PIECE)
        for h, owned in enumerate((2 * left, 2 * right + 1)):
            norm_out[h, :, span] = squares(orb[owned, :, span]) + squares(far[h, :, span])
        return carry

    lax.fori_loop(0, PIECES, norms, 0)
    go(norm_out.at[0], norm_in.at[0], NORM, {"orb": left})
    go(norm_out.at[1], norm_in.at[1], NORM, {"orb": right})
    arrived(Z_C, a0.at[0])
    arrived(X_C, pv.at[0, 0:3, 0:3, 0:2])
    mine = pv.at[core, :, 0:STEPS, 1:4]
    go(mine, mine, CORE_B, {"grid_2": other})
    arrived(CORE_B, pv.at[0, :, 0:STEPS, 1:4])
    for y in range(1, 4):
        pick(y)

    def size_of(squared):
        bounded = jnp.maximum(squared, TINY)
        return bounded * lax.rsqrt(bounded)

    for h, beside in enumerate((1, 3)):
        pack[h] = lax.rsqrt(jnp.maximum(norm_own[0] + norm_own[beside], TINY)) * SCALE
        unpack[h] = size_of(norm_own[beside] + norm_own[2]) * (1.0 / SCALE)
        unpack[2 + h] = size_of(norm_own[beside]) * (1.0 / SCALE)

    def decode(packed, scale, squared):
        words = [packed[i * BLOCK : (i + 1) * BLOCK] for i in range(FIELDS)]
        blocks = [(word << SPARE) >> SPARE for word in words]
        cut = VALUES - FIELDS
        for k in range(cut):
            top = (words[cut + k // 2] << (SPARE - REST * (k % 2 + 1))) >> (32 - REST)
            blocks.append((top << SPARE) | lax.shift_right_logical(words[k], FIELD))
        return jnp.concatenate(blocks, axis=0).astype(jnp.float32) * scale * size_of(squared)

    def send_sums(t, span, slot):
        for h, where in enumerate((left, right)):
            go(sums_out.at[h, t, :, span], sums_in.at[h, t, :, span], slot, {"orb": where})

    halves = (slice(0, 128), slice(128, 256))

    def middle(t, carry):
        span = pl.ds(pl.multiple_of(t * PIECE, PIECE), PIECE)
        for h, (own, source) in enumerate(((2 * left, 1), (2 * right + 1, 3))):
            a = orb[own, :, span]
            b = far[h, :, span]
            product = nn(picked[0, :, 0:DEPTH], a) + nn(picked[source, :, 0:DEPTH], b)
            sums_out[h, t] = encode(product, pack[h], norm_out[h, :, span])

        @pl.when(t < PIECES - 1)
        def _():
            send_sums(t, slice(0, PIECE), SUM + t)

        return carry

    lax.fori_loop(0, PIECES, middle, 0)
    for half in range(2):
        send_sums(PIECES - 1, halves[half], LAST + half)

    pairs = nt(picked[0], picked[0])
    for y in range(1, 4):
        pairs += nt(picked[y], picked[y])
    block = jnp.square(pairs * (1.0 / ORB))
    for i in range(STEPS):
        for j in range(i + 1):
            gram[3 * i + j] = block[i * PIV : (i + 1) * PIV, j * PIV : (j + 1) * PIV]

    def diagonal_inverse(i, carry):
        def update(k, carry):
            gram[4 * i] -= nt(low[3 * i + k], low[3 * i + k], HIGHEST)
            return carry

        lax.fori_loop(0, i, update, 0)
        inv[4 * i] = inverse_factor(gram[4 * i])

        def panel(j, carry):
            def update(k, carry):
                gram[3 * j + i] -= nt(low[3 * j + k], low[3 * i + k], HIGHEST)
                return carry

            lax.fori_loop(0, i, update, 0)
            low[3 * j + i] = nt(gram[3 * j + i], inv[4 * i], HIGHEST)
            return carry

        lax.fori_loop(i + 1, STEPS, panel, 0)
        return carry

    lax.fori_loop(0, STEPS, diagonal_inverse, 0)
    inv[3] = -nn(inv[4], nn(low[3], inv[0], HIGHEST), HIGHEST)
    inv[7] = -nn(inv[8], nn(low[7], inv[4], HIGHEST), HIGHEST)
    inv[6] = -nn(inv[8], nn(low[6], inv[0], HIGHEST) + nn(low[7], inv[3], HIGHEST), HIGHEST)

    arrived(NORM, norm_in)

    def own_and_coded(t, carry):
        span = pl.ds(pl.multiple_of(t * PIECE, PIECE), PIECE)
        after = pl.ds(pl.multiple_of(PART + t * PIECE, PIECE), PIECE)
        for h in range(2):
            a = orb[2 * me + h, :, span]
            squared = norm_in[1 - h, :, after]
            coded = decode(words_in[1 - h, t], unpack[3 - h], squared)
            own[h, t] = nn(picked[0, :, 0:DEPTH], a) + coded
            own_squares[h, :, span] = squares(a) + squared
        return carry

    arrived(NEAR, words_in)
    lax.fori_loop(0, PIECES, own_and_coded, 0)

    def finish(t, low, width, best):
        best = list(best)
        start = t * PIECE + low
        span = pl.ds(pl.multiple_of(start, 128), width)
        inside = slice(low, low + width)
        columns, rest = [], []
        for h in range(2):
            norm = norm_in[h, :, span]
            received = decode(sums_in[h, t, :, inside], unpack[h, :, 0:width], norm)
            columns.append(jnp.square((received + own[h, t, :, inside]) * (1.0 / ORB)))
            rest.append(jnp.square((norm + own_squares[h, :, span]) * (1.0 / ORB)))
        columns, rest = jnp.concatenate(columns, axis=1), jnp.concatenate(rest, axis=1)
        outs = [pl.ds(pl.multiple_of(h * PART + start, 128), width) for h in range(2)]
        for i in range(STEPS):
            fresh = nn(inv[3 * i], columns[0:PIV], HIGHEST)
            for j in range(1, i + 1):
                fresh += nn(inv[3 * i + j], columns[j * PIV : (j + 1) * PIV], HIGHEST)
            rest -= jnp.sum(fresh * fresh, axis=0, keepdims=True)
            for h in range(2):
                factor_ref[i * PIV : (i + 1) * PIV, outs[h]] = fresh[:, h * width : (h + 1) * width]
            for at in range(0, 2 * width, 128):
                best[i] = jnp.maximum(best[i], rest[:, at : at + 128])
        for h in range(2):
            diag_ref[:, outs[h]] = rest[:, h * width : (h + 1) * width]
        return tuple(best)

    def whole_piece(t, best):
        size = sums_in.at[:, t]
        pltpu.make_async_copy(size, size, recv_sem.at[SUM + t]).wait()
        return finish(t, 0, PIECE, best)

    best = (jnp.full((1, 128), -jnp.inf, jnp.float32),) * STEPS
    best = lax.fori_loop(0, PIECES - 1, whole_piece, best)
    for half in range(2):
        arrived(LAST + half, sums_in.at[:, PIECES - 1, :, halves[half]])
        best = finish(PIECES - 1, half * 128, 128, best)
    lanes = lax.broadcasted_iota(jnp.int32, (1, 128), 1)
    peak = jnp.full((1, 128), -jnp.inf, jnp.float32)
    for i in range(STEPS):
        peak = jnp.where(lanes == i, jnp.max(best[i], axis=1, keepdims=True), peak)

    unsent.extend((SUM + t, sums_in.at[:, t]) for t in range(PIECES - 1))

    peak_buf[0] = peak
    shifts = [(dx, dz, dy, dc) for dx in range(4) for dz in range(4) for dy in range(4) for dc in range(2)]
    shifts.sort(key=lambda shift: -sum(min(step, 4 - step) for step in shift[:3]))
    for shift in shifts:
        if not any(shift):
            continue
        slot = ((shift[0] * 4 + shift[1]) * 4 + shift[2]) * 2 + shift[3]
        there = {
            "grid_0": lax.rem(x + shift[0], 4),
            "grid_1": lax.rem(z + shift[1], 4),
            "orb": lax.rem(me + shift[2], 4),
            "grid_2": lax.rem(core + shift[3], 2),
        }
        go(peak_buf.at[0], peak_buf.at[slot], PEAK_A, there)
    sent()
    arrived(PEAK_A, peak_buf.at[1:128])
    sent()
    peak_ref[...] = jnp.max(peak_buf[...], axis=0)


def hand_over(factor, diagonal, peaks, factor_out, diagonal_out, peaks_out, diagonal_flat, peaks_flat, sem):
    strip = RANK // STRIPS
    copies = []
    for i in range(STRIPS):
        rows = slice(i * strip, (i + 1) * strip)
        copies.append(pltpu.make_async_copy(factor.at[rows], factor_out.at[rows], sem.at[i]))
        copies[-1].start()
    diagonal_flat[...] = diagonal[...].reshape(SHARE)
    peaks_flat[...] = peaks[0, 0:STEPS]
    for src, dst in ((diagonal_flat, diagonal_out), (peaks_flat, peaks_out)):
        copies.append(pltpu.make_async_copy(src, dst, sem.at[len(copies)]))
        copies[-1].start()
    for copy in copies:
        copy.wait()


def on_device(orbitals, pivots):
    f32, bf16 = jnp.float32, jnp.bfloat16
    vmem = pl.BlockSpec(memory_space=pltpu.VMEM)
    factor, diagonal, peaks = pl.pallas_call(
        kernel,
        out_shape=(
            jax.ShapeDtypeStruct((RANK, SHARE), f32),
            jax.ShapeDtypeStruct((1, SHARE), f32),
            jax.ShapeDtypeStruct((1, 128), f32),
        ),
        in_specs=[pl.BlockSpec(memory_space=pltpu.HBM)] * 2,
        out_specs=(vmem, vmem, vmem),
        scratch_shapes=[
            pltpu.VMEM((STEPS, PIV), jnp.int32),
            pltpu.VMEM((ROWS // PART, DEPTH, PART), bf16),
            pltpu.VMEM((RANK, WIDE), f32),
            pltpu.VMEM((2, 4, 4, 4, HALF, 128), bf16),
            pltpu.VMEM((2, 4, STEPS, HALF, 128), bf16),
            pltpu.VMEM((4, STEPS, HALF, 128), bf16),
            pltpu.VMEM((3, STEPS, HALF, 128), bf16),
            pltpu.VMEM((4, HALF, 128), bf16),
            pltpu.VMEM((3, HALF, 128), bf16),
            pltpu.VMEM((4, RANK, WIDE), bf16),
            pltpu.VMEM((2, DEPTH, PART), bf16),
            pltpu.VMEM((2, PIECES, WORDS, PIECE), jnp.int32),
            pltpu.VMEM((2, PIECES, WORDS, PIECE), jnp.int32),
            pltpu.VMEM((2, PIECES, WORDS, PIECE), jnp.int32),
            pltpu.VMEM((2, PIECES, WORDS, PIECE), jnp.int32),
            pltpu.VMEM((2, PIECES, RANK, PIECE), f32),
            pltpu.VMEM((2, 1, 2 * PART), f32),
            pltpu.VMEM((2, 1, 2 * PART), f32),
            pltpu.VMEM((2, 1, PART), f32),
            pltpu.VMEM((4, RANK, PIECE), f32),
            pltpu.VMEM((3, RANK, PIECE), f32),
            pltpu.VMEM((4, RANK, PIECE), f32),
            pltpu.VMEM((9, PIV, PIV), f32),
            pltpu.VMEM((9, PIV, PIV), f32),
            pltpu.VMEM((9, PIV, PIV), f32),
            pltpu.VMEM((128, 1, 128), f32),
            pltpu.SemaphoreType.DMA((5,)),
            pltpu.SemaphoreType.DMA((SLOTS,)),
            pltpu.SemaphoreType.DMA((SLOTS,)),
        ],
        compiler_params=pltpu.CompilerParams(
            collective_id=0, has_side_effects=True, vmem_limit_bytes=50 * 1024 * 1024
        ),
    )(orbitals, pltpu.with_memory_space_constraint(pivots, pltpu.HBM))
    factor, diagonal, peaks = pl.pallas_call(
        hand_over,
        out_shape=(
            jax.ShapeDtypeStruct((RANK, SHARE), f32),
            jax.ShapeDtypeStruct((SHARE,), f32),
            jax.ShapeDtypeStruct((STEPS,), f32),
        ),
        in_specs=[vmem] * 3,
        out_specs=(pl.BlockSpec(memory_space=pltpu.HBM),) * 3,
        scratch_shapes=[pltpu.VMEM((SHARE,), f32), pltpu.VMEM((STEPS,), f32), pltpu.SemaphoreType.DMA((STRIPS + 2,))],
        compiler_params=pltpu.CompilerParams(vmem_limit_bytes=4 * 1024 * 1024),
    )(factor, diagonal, peaks)
    return factor.T, diagonal, peaks


def solution(mesh):
    split = Mesh(
        mesh.devices.reshape(4, 4, 2, mesh.shape["orb"]), ("grid_0", "grid_1", "grid_2", "orb")
    )
    return jax.shard_map(
        on_device,
        mesh=split,
        in_specs=(P("orb", GRID), P()),
        out_specs=(P(GRID_ORB, None), P(GRID_ORB), P()),
        check_vma=False,
    )
```
